32 devices in a mesh: dp: 1 (over z), row: 4 (over y), col: 8 (over x, core).
Axes of the slice: x: 4, y: 4, z: 1, core: 2. Of those that a mesh axis runs over, the one named last changes fastest.
The devices are a block of a 4x4x8 slice.
Arguments:
- x: bfloat16 [16384, 1024], P(('dp', 'row', 'col'))
- route_idx: int32 [16384, 8], P(('dp', 'row', 'col'))
- gates: float32 [16384, 8], P(('dp', 'row', 'col'))
- w1: bfloat16 [64, 1024, 512], P(('row', 'col'))
- w3: bfloat16 [64, 1024, 512], P(('row', 'col'))
- w2: bfloat16 [64, 512, 1024], P(('row', 'col'))
- dy: bfloat16 [16384, 1024], P(('dp', 'row', 'col'))
Outputs:
- output 1: bfloat16 [16384, 1024], P(('dp', 'row', 'col'))
- output 2: bfloat16 [16384, 1024], P(('dp', 'row', 'col'))
- output 3: float32 [16384, 8], P(('dp', 'row', 'col'))
- output 4: float32 [64, 1024, 512], P(('dp', 'row', 'col'))
- output 5: float32 [64, 1024, 512], P(('dp', 'row', 'col'))
- output 6: float32 [64, 512, 1024], P(('dp', 'row', 'col'))
All inputs are finite; a program needn't handle non-finite values.
Results may differ from the reference program's by a relative error of at most 0.00111.
Values are sent between devices in bfloat16 or wider.
A program may use at most 768 MiB of HBM per device.

```python
import jax
import jax.numpy as jnp
from jax import lax

TOK = 512
NDEV = 32
D = 1024
FF = 512
EXPERTS = 64
TOP = 8

TG = NDEV * TOK
CAP = (4 * TOK * TOP + EXPERTS - 1) // EXPERTS
CG = NDEV * CAP
NH = max(1, min(TOP // 2, (8 * TOP) // NDEV))
HOT = 2 * EXPERTS // NDEV
NCOLD = EXPERTS - HOT


def setup_inputs(seed: int = 0, part: int = 0) -> dict:
    kw = jax.random.split(jax.random.key(seed), 3)
    kp = jax.random.split(jax.random.fold_in(jax.random.key(seed + 1), part), 8)
    w1 = (jax.random.normal(kw[0], (EXPERTS, D, FF), jnp.float32) * D ** -0.5).astype(jnp.bfloat16)
    w3 = (jax.random.normal(kw[1], (EXPERTS, D, FF), jnp.float32) * D ** -0.5).astype(jnp.bfloat16)
    w2 = (jax.random.normal(kw[2], (EXPERTS, FF, D), jnp.float32) * FF ** -0.5).astype(jnp.bfloat16)
    dmax = min(NH, HOT - NH, TOP - NH)
    sh = jax.random.randint(kp[2], (), 0, HOT)
    sc = jax.random.randint(kp[3], (), 0, NCOLD)
    dd = jax.random.randint(kp[0], (NDEV, TOK // 2), 0, dmax + 1)
    nh = jnp.stack([NH + dd, NH - dd], axis=-1).reshape(NDEV, TOK)
    nc = TOP - nh
    sth = jnp.cumsum(nh, axis=1) - nh
    stc = jnp.cumsum(nc, axis=1) - nc
    dev = jnp.arange(NDEV)[:, None, None]
    j = jnp.arange(TOP)[None, None, :]
    hot_ids = (sh + dev * (TOK * NH) + sth[:, :, None] + j) % HOT
    cold_ids = HOT + (sc + dev * (TOK * (TOP - NH)) + stc[:, :, None] + j - nh[:, :, None]) % NCOLD
    ids = jnp.where(j < nh[:, :, None], hot_ids, cold_ids).reshape(TG, TOP)
    ids = jax.random.permutation(kp[4], ids, axis=1, independent=True).astype(jnp.int32)
    gu = jax.random.uniform(kp[5], (TG, TOP), jnp.float32, 0.5, 1.5)
    gates = gu / jnp.sum(gu, axis=1, keepdims=True)
    x = jax.random.normal(kp[6], (TG, D), jnp.float32).astype(jnp.bfloat16)
    dy = jax.random.normal(kp[7], (TG, D), jnp.float32).astype(jnp.bfloat16)
    return {'x': x, 'route_idx': ids, 'gates': gates, 'w1': w1, 'w3': w3, 'w2': w2, 'dy': dy}


def reference(x, route_idx, gates, w1, w3, w2, dy):
    n = TG * TOP
    ef = route_idx.reshape(n)
    order = jnp.argsort(ef, stable=True).astype(jnp.int32)
    es = ef[order]
    first = jnp.searchsorted(es, es, side='left').astype(jnp.int32)
    rank = jnp.arange(n, dtype=jnp.int32) - first
    tab = jnp.full((EXPERTS, CG), n, jnp.int32).at[es, rank].set(order)
    gf = gates.reshape(n)

    def body(carry, inp):
        y_acc, dx_acc, dg = carry
        te, a1, a3, a2 = inp
        valid = te < n
        ai = jnp.minimum(te, n - 1)
        tk = ai // TOP
        xr = x[tk]
        xs = jnp.where(valid[:, None], xr, jnp.zeros_like(xr))
        u = jnp.dot(xs, a1, preferred_element_type=jnp.float32).astype(jnp.bfloat16).astype(jnp.float32)
        v = jnp.dot(xs, a3, preferred_element_type=jnp.float32).astype(jnp.bfloat16).astype(jnp.float32)
        sg = jax.nn.sigmoid(u)
        a = (u * sg * v).astype(jnp.bfloat16)
        o = jnp.dot(a, a2, preferred_element_type=jnp.float32).astype(jnp.bfloat16).astype(jnp.float32)
        g = jnp.where(valid, gf[ai], 0.0)
        y_acc = y_acc.at[tk].add(g[:, None] * o)
        dys = dy[tk].astype(jnp.float32)
        dg = dg.at[ai].add(jnp.where(valid, jnp.sum(dys * o, axis=1), 0.0))
        do = (g[:, None] * dys).astype(jnp.bfloat16)
        gw2 = jnp.dot(a.T, do, preferred_element_type=jnp.float32)
        da = jnp.dot(do, a2.T, preferred_element_type=jnp.float32)
        du = (da * v * sg * (1.0 + u * (1.0 - sg))).astype(jnp.bfloat16)
        dv = (da * u * sg).astype(jnp.bfloat16)
        gw1 = jnp.dot(xs.T, du, preferred_element_type=jnp.float32)
        gw3 = jnp.dot(xs.T, dv, preferred_element_type=jnp.float32)
        dxs = jnp.dot(du, a1.T, preferred_element_type=jnp.float32) + jnp.dot(dv, a3.T, preferred_element_type=jnp.float32)
        dx_acc = dx_acc.at[tk].add(dxs.astype(jnp.bfloat16).astype(jnp.float32))
        return (y_acc, dx_acc, dg), (gw1, gw3, gw2)

    init = (jnp.zeros((TG, D), jnp.float32), jnp.zeros((TG, D), jnp.float32), jnp.zeros((n,), jnp.float32))
    (y_acc, dx_acc, dg), (gw1, gw3, gw2) = lax.scan(body, init, (tab, w1, w3, w2))
    return (y_acc.astype(jnp.bfloat16), dx_acc.astype(jnp.bfloat16), dg.reshape(TG, TOP), gw1, gw3, gw2)
```

```python
import functools

import jax
import jax.numpy as jnp
from jax import lax
from jax.experimental import pallas as pl
from jax.experimental.pallas import tpu as pltpu
from jax.sharding import PartitionSpec as P

BF = jnp.bfloat16
F32 = jnp.float32


def mm(a, b, dims=((1,), (0,))):
    return lax.dot_general(a, b, (dims, ((), ())), preferred_element_type=F32)


def expert_kernel(cap, base_ref, meta_ref, x_ref, dy_ref, w1_ref, w3_ref, w2_ref, w1t_ref, w3t_ref, w2t_ref,
                  y_ref, dx_ref, dg_ref, gw1_ref, gw3_ref, gw2_ref,
                  xs_ref, do_ref, o_ref, dxs_ref, pt_ref, gc_ref, acc1, acc3, acc2, sem):
    step = pl.program_id(0)
    ns, top2, tok = meta_ref.shape
    top = top2 // 2
    el = w1_ref.shape[0]

    @pl.when(step == 0)
    def _():
        acc1[...] = jnp.zeros_like(acc1)
        acc3[...] = jnp.zeros_like(acc3)
        acc2[...] = jnp.zeros_like(acc2)

    tri = (lax.broadcasted_iota(jnp.int32, (tok, tok), 0) <= lax.broadcasted_iota(jnp.int32, (tok, tok), 1)).astype(BF)
    for s in range(ns):
        ids = meta_ref[s, :top, :]
        gts = meta_ref[s, top:, :]
        first = base_ref[0]
        masks, gws = [], []
        for e in range(el):
            hit = ids == (first + e).astype(F32)
            masks.append(jnp.sum(jnp.where(hit, 1.0, 0.0), axis=0, keepdims=True))
            gws.append(jnp.sum(jnp.where(hit, gts, 0.0), axis=0, keepdims=True))
        mask = jnp.concatenate(masks + [jnp.zeros((8 - el, tok), F32)], axis=0)
        cum = mm(mask.astype(BF), tri)
        pos = jnp.where(mask > 0.0, cum - 1.0, -1.0)
        gw = jnp.concatenate(gws + [jnp.zeros((8 - el, tok), F32)], axis=0)
        cols = jnp.concatenate([pos, gw], axis=0).T
        gc_ref[s] = cols
        rows = lax.broadcasted_iota(jnp.int32, (cap, tok), 0).astype(F32)
        lanes = lax.broadcasted_iota(jnp.int32, (tok, cap), 1).astype(F32)
        for e in range(el):
            hit = rows == pos[e:e + 1, :]
            p = jnp.where(hit, 1.0, 0.0).astype(BF)
            gs = jnp.sum(jnp.where(hit, gw[e:e + 1, :], 0.0), axis=1, keepdims=True)
            pt_ref[s, :, e * cap:(e + 1) * cap] = jnp.where(lanes == cols[:, e:e + 1], 1.0, 0.0).astype(BF)
            xs_ref[e, s * cap:(s + 1) * cap, :] = mm(p, x_ref[s * tok:(s + 1) * tok, :]).astype(BF)
            do_ref[e, s * cap:(s + 1) * cap, :] = (gs * mm(p, dy_ref[s * tok:(s + 1) * tok, :])).astype(BF)

    for e in range(el):
        xs = xs_ref[e]
        u = mm(xs, w1_ref[e]).astype(BF).astype(F32)
        v = mm(xs, w3_ref[e]).astype(BF).astype(F32)
        sg = jax.nn.sigmoid(u)
        a = (u * sg * v).astype(BF)
        o_ref[e] = mm(a, w2_ref[e]).astype(BF)
        do = do_ref[e]
        acc2[e] += mm(a, do, ((0,), (0,)))
        da = mm(do, w2t_ref[e])
        du = (da * v * sg * (1.0 + u * (1.0 - sg))).astype(BF)
        dv = (da * u * sg).astype(BF)
        acc1[e] += mm(xs, du, ((0,), (0,)))
        acc3[e] += mm(xs, dv, ((0,), (0,)))
        dxs = (mm(du, w1t_ref[e]) + mm(dv, w3t_ref[e])).astype(BF)
        for s in range(ns):
            dxs_ref[s, e * cap:(e + 1) * cap, :] = dxs[s * cap:(s + 1) * cap, :]

    for s in range(ns):
        tk = pl.ds(s * tok, tok)
        dx_ref[tk, :] = mm(pt_ref[s], dxs_ref[s])
        dyf = dy_ref[tk, :].astype(F32)
        yacc = None
        dgs = []
        for e in range(el):
            so = mm(pt_ref[s, :, e * cap:(e + 1) * cap], o_ref[e, s * cap:(s + 1) * cap, :])
            dgs.append(jnp.sum(dyf * so, axis=1, keepdims=True))
            term = gc_ref[s, :, 8 + e:9 + e] * so
            yacc = term if yacc is None else yacc + term
        y_ref[tk, :] = yacc
        dg = jnp.concatenate(dgs + [jnp.zeros((tok, 8 - el), F32)], axis=1)
        dg_ref[s] = dg.T

    @pl.when(step == pl.num_programs(0) - 1)
    def _():
        c1 = pltpu.make_async_copy(acc1, gw1_ref, sem.at[0])
        c3 = pltpu.make_async_copy(acc3, gw3_ref, sem.at[1])
        c2 = pltpu.make_async_copy(acc2, gw2_ref, sem.at[2])
        c1.start()
        c3.start()
        c2.start()
        c1.wait()
        c3.wait()
        c2.wait()


def expert_call(base, meta, x, dy, w1, w3, w2, tok, cap):
    nd = meta.shape[0]
    d = x.shape[1]
    el, _, f = w1.shape
    ns = 2
    any_spec = pl.BlockSpec(memory_space=pl.ANY)
    vm = pl.BlockSpec(memory_space=pltpu.VMEM)
    flops = 13 * 2 * nd * el * cap * d * f
    return pl.pallas_call(
        functools.partial(expert_kernel, cap),
        grid=(nd // ns,),
        in_specs=[
            pl.BlockSpec(memory_space=pltpu.SMEM),
            pl.BlockSpec((ns,) + meta.shape[1:], lambda i: (i, 0, 0)),
            pl.BlockSpec((ns * tok, d), lambda i: (i, 0)),
            pl.BlockSpec((ns * tok, d), lambda i: (i, 0)),
            vm, vm, vm, vm, vm, vm,
        ],
        out_specs=[
            pl.BlockSpec((ns * tok, d), lambda i: (i, 0)),
            pl.BlockSpec((ns * tok, d), lambda i: (i, 0)),
            pl.BlockSpec((ns, 8, tok), lambda i: (i, 0, 0)),
            any_spec, any_spec, any_spec,
        ],
        out_shape=[
            jax.ShapeDtypeStruct((nd * tok, d), F32),
            jax.ShapeDtypeStruct((nd * tok, d), F32),
            jax.ShapeDtypeStruct((nd, 8, tok), F32),
            jax.ShapeDtypeStruct((el, d, f), F32),
            jax.ShapeDtypeStruct((el, d, f), F32),
            jax.ShapeDtypeStruct((el, f, d), F32),
        ],
        scratch_shapes=[
            pltpu.VMEM((el, ns * cap, d), BF),
            pltpu.VMEM((el, ns * cap, d), BF),
            pltpu.VMEM((el, ns * cap, d), BF),
            pltpu.VMEM((ns, el * cap, d), BF),
            pltpu.VMEM((ns, tok, el * cap), BF),
            pltpu.VMEM((ns, tok, 16), F32),
            pltpu.VMEM((el, d, f), F32),
            pltpu.VMEM((el, d, f), F32),
            pltpu.VMEM((el, f, d), F32),
            pltpu.SemaphoreType.DMA((3,)),
        ],
        cost_estimate=pl.CostEstimate(flops=flops, bytes_accessed=nd * tok * d * 12, transcendentals=0),
        compiler_params=pltpu.CompilerParams(vmem_limit_bytes=63 * 1024 * 1024, dimension_semantics=("arbitrary",)),
    )(base, meta, x, dy, w1, w3, w2, jnp.swapaxes(w1, 1, 2), jnp.swapaxes(w3, 1, 2), jnp.swapaxes(w2, 1, 2))


def solution(mesh):
    nd = mesh.shape['row'] * mesh.shape['col']
    grp = ('row', 'col')
    tspec = P(('dp', 'row', 'col'), None)
    wspec = P(grp, None, None)
    gspec = P(('dp', 'row', 'col'), None, None)

    def local(x, ridx, gates, w1, w3, w2, dy):
        tok, d = x.shape
        top = ridx.shape[1]
        el = w1.shape[0]
        ne = el * nd
        cap = (4 * tok * top + ne - 1) // ne
        meta = jnp.concatenate([ridx.astype(F32).T, gates.T], axis=0)
        metas = lax.all_gather(meta, grp, axis=0, tiled=False)
        xg = lax.all_gather(x, grp, axis=0, tiled=True)
        dyg = lax.all_gather(dy, grp, axis=0, tiled=True)
        base = (lax.axis_index(grp) * el).astype(jnp.int32).reshape(1)
        yp, dxp, dg, gw1, gw3, gw2 = expert_call(base, metas, xg, dyg, w1, w3, w2, tok, cap)
        y = lax.psum_scatter(yp, grp, scatter_dimension=0, tiled=True).astype(BF)
        dx = lax.psum_scatter(dxp, grp, scatter_dimension=0, tiled=True).astype(BF)
        dgt = lax.all_to_all(dg[:, :el, :], grp, 0, 0, tiled=True).reshape(ne, tok)
        pick = ridx.T[:, None, :] == jnp.arange(ne, dtype=jnp.int32)[None, :, None]
        dgates = jnp.sum(jnp.where(pick, dgt[None], 0.0), axis=1).T
        return y, dx, dgates, gw1, gw3, gw2

    return jax.shard_map(local, mesh=mesh, in_specs=(tspec, tspec, tspec, wspec, wspec, wspec, tspec), out_specs=(tspec, tspec, tspec, gspec, gspec, gspec), check_vma=False)
```

```python
import functools

import jax
import jax.numpy as jnp
from jax import lax
from jax.experimental import pallas as pl
from jax.experimental.pallas import tpu as pltpu
from jax.sharding import PartitionSpec as P

BF = jnp.bfloat16
F32 = jnp.float32
MESH = pl.DeviceIdType.MESH


def mm(a, b, dims=((1,), (0,))):
    return lax.dot_general(a, b, (dims, ((), ())), preferred_element_type=F32)


def cycle_index(k, n, x, y):
    return n * ((1 - k) * y + k * x) + (x + y) % n


def cycle_chip(k, n, i):
    r = i // n
    o = (i % n - r + n) % n
    return k * r + (1 - k) * o, k * o + (1 - k) * r


def moe_kernel(n, cap, x_ref, dy_ref, meta_ref, w1_hbm, w3_hbm, w2_hbm,
               y_ref, dx_ref, dg_ref, gw1_ref, gw3_ref, gw2_ref, xb, db, mb, pown, psib, rin,
               w1_ref, w3_ref, w2_ref, acc1, acc3, acc2, xv, mv, dv_, xs_ref, do_ref, o_ref, dxs_ref, pt_ref, gc_ref, tri_ref,
               stage, pv, ov,
               ag_send, ag_recv, push_send, push_recv, part_recv, rs_send, rs_recv,
               ld_x, ld_m, ld_d, ld_w, st_loc, st_rem, ld_p, ld_r, out_sem):
    N = n * n
    H = N // 2
    row = lax.axis_index('row')
    col = lax.axis_index('col')
    cx = col // 2
    c = col % 2
    cy = row
    tok, d = x_ref.shape
    top = meta_ref.shape[0] // 2
    el = w1_ref.shape[0]
    half = tok // 2
    pos_k = (cycle_index(0, n, cx, cy), cycle_index(1, n, cx, cy))
    me = (1 - c) * pos_k[0] + c * pos_k[1]
    first = (cy * (2 * n) + 2 * cx + c) * el

    def device(i):
        px, py = cycle_chip(c, n, i)
        return {'row': py, 'col': 2 * px + c}

    nxt = device((me + 1) % N)
    prv = device((me + N - 1) % N)
    sib = {'row': row, 'col': 2 * cx + 1 - c}
    ring = (nxt, prv)

    def rcopy(src, dst, ss, rs, dev):
        return pltpu.make_async_remote_copy(src_ref=src, dst_ref=dst, send_sem=ss, recv_sem=rs, device_id=dev, device_id_type=MESH)

    barrier = pltpu.get_barrier_semaphore()
    for dev in (nxt, prv, sib):
        pl.semaphore_signal(barrier, inc=1, device_id=dev, device_id_type=MESH)
    pl.semaphore_wait(barrier, 3)

    own = (x_ref, meta_ref, dy_ref)
    bufs = (xb, mb, db)

    def ag_copy(q, kind, t, j, src=None):
        slot = bufs[kind].at[c, j]
        return rcopy(slot if src is None else src, slot, ag_send.at[q, t, kind], ag_recv.at[q, t, kind], ring[q])

    def push(kind, j, src=None):
        slot = bufs[kind].at[c, j]
        return rcopy(slot if src is None else src, slot, push_send.at[j, kind], push_recv.at[j, kind], sib)

    def push_arrival(kind, k, j):
        slot = bufs[kind].at[k, j]
        return rcopy(slot, slot, push_send.at[j, kind], push_recv.at[j, kind], sib)

    for kind in (0, 1, 2):
        ag_copy(0, kind, 0, me, own[kind]).start()
        ag_copy(1, kind, 0, me, own[kind]).start()
    for kind in (0, 1, 2):
        push(kind, me, own[kind]).start()

    weights = ((w1_hbm, w1_ref), (w3_hbm, w3_ref), (w2_hbm, w2_ref))
    for i, (src, dst) in enumerate(weights):
        pltpu.make_async_copy(src, dst, ld_w.at[i]).start()

    def unit_blocks(u):
        o = (u + 1) // 2
        ka = jnp.where(u == 0, 0, (u + 1) % 2)
        kb = jnp.where(u == N - 1, 1, (u + 1) % 2)
        ia = (1 - ka) * pos_k[0] + ka * pos_k[1]
        ib = (1 - kb) * pos_k[0] + kb * pos_k[1]
        return ((ka, (ia - o + N) % N), (kb, (ib + o) % N))

    def block_loads(u, b, k, j, local):
        slot = u % 2
        src = own if local else (xb.at[k, j], mb.at[k, j], db.at[k, j])
        return (pltpu.make_async_copy(src[0], xv.at[b], ld_x.at[b]),
                pltpu.make_async_copy(src[1], mv.at[b], ld_m.at[b]),
                pltpu.make_async_copy(src[2], dv_.at[slot, b], ld_d.at[b]))

    def start_loads(u):
        for b, (k, j) in enumerate(unit_blocks(u)):
            @pl.when(k != c)
            def _(k=k, j=j):
                for kind in (0, 1, 2):
                    push_arrival(kind, k, j).wait_recv()

            @pl.when(jnp.logical_and(u == 0, k == c))
            def _(b=b, k=k, j=j):
                for cp in block_loads(u, b, k, j, True):
                    cp.start()

            @pl.when(jnp.logical_or(u != 0, k != c))
            def _(b=b, k=k, j=j):
                for cp in block_loads(u, b, k, j, False):
                    cp.start()

    def wait_loads(u):
        for b, (k, j) in enumerate(unit_blocks(u)):
            for cp in block_loads(u, b, k, j, False):
                cp.wait()

    def ag_event(t):
        jf = (me - t + N) % N
        jb = (me + t) % N
        for kind, long_q in ((0, 0), (1, 0), (2, 1)):
            for q, j in ((0, jf), (1, jb)):
                reach = H if q == long_q else H - 1

                @pl.when(t <= reach)
                def _(kind=kind, q=q, j=j, reach=reach):
                    ag_copy(q, kind, t - 1, j).wait_recv()

                    @pl.when(t < reach)
                    def _():
                        ag_copy(q, kind, t, j).start()

                    push(kind, j).start()

    def rs_dest(q, s):
        return (me - 1 - s + 2 * N) % N if q == 0 else (me + 1 + s) % N

    def rows_of(h):
        return pl.ds(pl.multiple_of(h * half, half), half)

    def rs_loads(q, e):
        s, h = e // 2, e % 2
        dst = rs_dest(q, s)
        rows = rows_of(h)
        p0 = pltpu.make_async_copy(pown.at[dst, q, rows], pv.at[q, 0], ld_p.at[q, 0])
        p1 = pltpu.make_async_copy(psib.at[dst, q, rows], pv.at[q, 1], ld_p.at[q, 1])
        r = pltpu.make_async_copy(rin.at[q, jnp.maximum(s - 1, 0), rows], ov.at[q, e % 2], ld_r.at[q])
        return p0, p1, r

    def rs_copy(q, e):
        s, h = e // 2, e % 2
        return rcopy(ov.at[q, e % 2], rin.at[q, s, rows_of(h)], rs_send.at[q, e % 2], rs_recv.at[q, s, h], ring[q])

    def rs_start(q, e):
        s, h = e // 2, e % 2
        fresh = s <= H - 2
        if q == 0:
            fresh = jnp.logical_or(fresh, jnp.logical_or(s == H - 1, s == N - 1))

        @pl.when(jnp.logical_and(h == 0, fresh))
        def _():
            dst = rs_dest(q, s)
            rcopy(psib.at[dst], psib.at[dst], st_rem.at[0], part_recv.at[dst], sib).wait_recv()

        p0, p1, r = rs_loads(q, e)
        p0.start()
        p1.start()

        @pl.when(e >= 2)
        def _():
            rs_copy(q, e - 2).wait_send()
            rs_copy(q, e - 2).wait_recv()
            r.start()

    def rs_finish(q, e):
        p0, p1, r = rs_loads(q, e)
        p0.wait()
        p1.wait()
        step = min(64, half)

        @pl.when(e < 2)
        def _():
            def body(i, _):
                rr = pl.ds(pl.multiple_of(i * step, step), step)
                ov[q, e % 2, rr, :] = pv[q, 0, rr, :] + pv[q, 1, rr, :]
                return 0
            lax.fori_loop(0, half // step, body, 0)

        @pl.when(e >= 2)
        def _():
            r.wait()

            def body(i, _):
                rr = pl.ds(pl.multiple_of(i * step, step), step)
                ov[q, e % 2, rr, :] = ov[q, e % 2, rr, :] + (pv[q, 0, rr, :] + pv[q, 1, rr, :])
                return 0
            lax.fori_loop(0, half // step, body, 0)

        @pl.when(e < 2 * N - 2)
        def _():
            rs_copy(q, e).start()

    def stage_store(u, b, k, j):
        loc = pltpu.make_async_copy(stage.at[b], pown.at[j], st_loc.at[b])
        rem = rcopy(stage.at[b], psib.at[j], st_rem.at[b], part_recv.at[j], sib)
        return loc, rem

    def stage_start(u):
        for b, (k, j) in enumerate(unit_blocks(u)):
            loc, rem = stage_store(u, b, k, j)

            @pl.when(k == c)
            def _(loc=loc):
                loc.start()

            @pl.when(k != c)
            def _(rem=rem):
                rem.start()

    def stage_wait(u, local):
        for b, (k, j) in enumerate(unit_blocks(u)):
            loc, rem = stage_store(u, b, k, j)
            if local:
                @pl.when(k == c)
                def _(loc=loc):
                    loc.wait()
            else:
                @pl.when(k != c)
                def _(rem=rem):
                    rem.wait_send()

    start_loads(0)
    tri_ref[...] = (lax.broadcasted_iota(jnp.int32, (tok, tok), 0) <= lax.broadcasted_iota(jnp.int32, (tok, tok), 1)).astype(F32).astype(BF)
    for e in range(el):
        acc1[e] = jnp.zeros(acc1.shape[1:], F32)
        acc3[e] = jnp.zeros(acc3.shape[1:], F32)
        acc2[e] = jnp.zeros(acc2.shape[1:], F32)

    def gather_stage(u):
        rows = lax.broadcasted_iota(jnp.int32, (cap, tok), 0).astype(F32)
        lanes = lax.broadcasted_iota(jnp.int32, (tok, cap), 1).astype(F32)
        for b in range(2):
            ids = mv[b, :top, :]
            gts = mv[b, top:, :]
            masks, gws = [], []
            for e in range(el):
                hit = ids == (first + e).astype(F32)
                masks.append(jnp.sum(jnp.where(hit, 1.0, 0.0), axis=0, keepdims=True))
                gws.append(jnp.sum(jnp.where(hit, gts, 0.0), axis=0, keepdims=True))
            mask = jnp.concatenate(masks + [jnp.zeros((8 - el, tok), F32)], axis=0)
            cum = mm(mask.astype(BF), tri_ref[...])
            pos = jnp.where(mask > 0.0, cum - 1.0, -1.0)
            gw = jnp.concatenate(gws + [jnp.zeros((8 - el, tok), F32)], axis=0)
            cols = jnp.concatenate([pos, gw], axis=0).T
            gc_ref[b] = cols
            for e in range(el):
                hit = rows == pos[e:e + 1, :]
                p = jnp.where(hit, 1.0, 0.0).astype(BF)
                gs = jnp.sum(jnp.where(hit, gw[e:e + 1, :], 0.0), axis=1, keepdims=True)
                pt_ref[b, :, e * cap:(e + 1) * cap] = jnp.where(lanes == cols[:, e:e + 1], 1.0, 0.0).astype(BF)
                xs_ref[e, b * cap:(b + 1) * cap, :] = mm(p, xv[b]).astype(BF)
                do_ref[e, b * cap:(b + 1) * cap, :] = (gs * mm(p, dv_[u % 2, b])).astype(BF)

    def expert(e, tick):
        xs = xs_ref[e]
        uu = mm(xs, w1_ref[e]).astype(BF).astype(F32)
        vv = mm(xs, w3_ref[e]).astype(BF).astype(F32)
        sg = jax.nn.sigmoid(uu)
        a = (uu * sg * vv).astype(BF)
        o_ref[e] = mm(a, w2_ref[e]).astype(BF)
        do = do_ref[e]
        acc2[e] += mm(a, do, ((0,), (0,)))
        da = mm(do, w2_ref[e], ((1,), (1,)))
        du = (da * vv * sg * (1.0 + uu * (1.0 - sg))).astype(BF)
        dv = (da * uu * sg).astype(BF)
        tick()
        acc1[e] += mm(xs, du, ((0,), (0,)))
        acc3[e] += mm(xs, dv, ((0,), (0,)))
        dxs = (mm(du, w1_ref[e], ((1,), (1,))) + mm(dv, w3_ref[e], ((1,), (1,)))).astype(BF)
        for b in range(2):
            dxs_ref[b, e * cap:(e + 1) * cap, :] = dxs[b * cap:(b + 1) * cap, :]

    def scatter_stage(u):
        for b, (k, j) in enumerate(unit_blocks(u)):
            dyf = dv_[u % 2, b].astype(F32)
            yacc = None
            dgs = []
            for e in range(el):
                so = mm(pt_ref[b, :, e * cap:(e + 1) * cap], o_ref[e, b * cap:(b + 1) * cap, :])
                dgs.append(jnp.sum(dyf * so, axis=1, keepdims=True))
                term = gc_ref[b, :, 8 + e:9 + e] * so
                yacc = term if yacc is None else yacc + term
            stage[b, 0] = yacc
            stage[b, 1] = mm(pt_ref[b], dxs_ref[b])
            dg = jnp.concatenate(dgs + [jnp.zeros((tok, 8 - el), F32)], axis=1).T
            px, py = cycle_chip(k, n, j)
            dg_ref[py * (2 * n) + 2 * px + k] = dg

    def unit(u, carry):
        wait_loads(u)

        @pl.when(u >= 1)
        def _():
            stage_wait(u - 1, True)

        gather_stage(u)

        @pl.when(jnp.logical_and(u >= 1, u < N - 1))
        def _():
            start_loads(u + 1)

        @pl.when(u == 0)
        def _():
            for i, (src, dst) in enumerate(weights):
                pltpu.make_async_copy(src, dst, ld_w.at[i]).wait()

        live = u >= 3
        ev = u - 3

        def tick_a():
            @pl.when(live)
            def _():
                rs_start(0, ev)

        def tick_b():
            @pl.when(live)
            def _():
                rs_finish(0, ev)
                rs_start(1, ev)

        def tick_c():
            @pl.when(live)
            def _():
                rs_finish(1, ev)

        expert(0, tick_a)
        expert(1, tick_b)
        tick_c()

        @pl.when(u >= 1)
        def _():
            stage_wait(u - 1, False)

        scatter_stage(u)
        stage_start(u)

        @pl.when(jnp.logical_or(u == 0, jnp.logical_and(u % 2 == 1, u <= N - 3)))
        def _():
            ag_event(jnp.where(u == 0, 1, (u + 3) // 2))

        @pl.when(u == 0)
        def _():
            start_loads(1)

        return carry

    lax.fori_loop(0, N, unit, 0)
    stage_wait(N - 1, True)
    grads = ((acc1, gw1_ref), (acc3, gw3_ref), (acc2, gw2_ref))
    for i, (src, dst) in enumerate(grads):
        pltpu.make_async_copy(src, dst, ld_w.at[i]).start()

    def tail(e, carry):
        rs_start(0, e)
        rs_start(1, e)
        rs_finish(0, e)
        rs_finish(1, e)

        @pl.when(e >= 2 * N - 2)
        def _():
            rows = rows_of(e % 2)
            for q, out in ((0, y_ref), (1, dx_ref)):
                xs_ref[q, rows, :] = ov[q, e % 2].astype(BF)
                pltpu.make_async_copy(xs_ref.at[q, rows], out.at[rows], out_sem.at[q, e % 2]).start()
        return carry

    lax.fori_loop(N - 3, 2 * N, tail, 0)

    stage_wait(N - 1, False)
    for q, out in ((0, y_ref), (1, dx_ref)):
        for h in range(2):
            rows = pl.ds(h * half, half)
            pltpu.make_async_copy(xs_ref.at[q, rows], out.at[rows], out_sem.at[q, h]).wait()
    for i, (src, dst) in enumerate(grads):
        pltpu.make_async_copy(src, dst, ld_w.at[i]).wait()
    for kind, long_q in ((0, 0), (1, 0), (2, 1)):
        for q in range(2):
            reach = H if q == long_q else H - 1

            def drain(t, carry, kind=kind, q=q):
                ag_copy(q, kind, t, me).wait_send()
                return carry
            lax.fori_loop(0, reach, drain, 0)

        def drain_push(j, carry, kind=kind):
            push(kind, j).wait_send()
            return carry
        lax.fori_loop(0, N, drain_push, 0)


def moe_call(n, cap, meta, x, dy, w1, w3, w2):
    N = n * n
    tok, d = x.shape
    el, _, f = w1.shape
    half = tok // 2
    any_spec = pl.BlockSpec(memory_space=pl.ANY)
    vm = pl.BlockSpec(memory_space=pltpu.VMEM)
    flops = 13 * 2 * 2 * N * el * cap * d * f
    shape = jax.ShapeDtypeStruct
    dma = pltpu.SemaphoreType.DMA
    outs = pl.pallas_call(
        functools.partial(moe_kernel, n, cap),
        in_specs=[any_spec] * 6,
        out_specs=[any_spec, any_spec, vm] + [any_spec] * 9,
        out_shape=[
            shape((tok, d), BF),
            shape((tok, d), BF),
            shape((2 * N, 8, tok), F32),
            shape((el, d, f), F32),
            shape((el, d, f), F32),
            shape((el, f, d), F32),
            shape((2, N, tok, d), BF),
            shape((2, N, tok, d), BF),
            shape((2, N) + meta.shape, F32),
            shape((N, 2, tok, d), F32),
            shape((N, 2, tok, d), F32),
            shape((2, N - 1, tok, d), F32),
        ],
        scratch_shapes=[
            pltpu.VMEM((el, d, f), BF),
            pltpu.VMEM((el, d, f), BF),
            pltpu.VMEM((el, f, d), BF),
            pltpu.VMEM((el, d, f), F32),
            pltpu.VMEM((el, d, f), F32),
            pltpu.VMEM((el, f, d), F32),
            pltpu.VMEM((2, tok, d), BF),
            pltpu.VMEM((2,) + meta.shape, F32),
            pltpu.VMEM((2, 2, tok, d), BF),
            pltpu.VMEM((el, 2 * cap, d), BF),
            pltpu.VMEM((el, 2 * cap, d), BF),
            pltpu.VMEM((el, 2 * cap, d), BF),
            pltpu.VMEM((2, el * cap, d), BF),
            pltpu.VMEM((2, tok, el * cap), BF),
            pltpu.VMEM((2, tok, 16), F32),
            pltpu.VMEM((tok, tok), BF),
            pltpu.VMEM((2, 2, tok, d), F32),
            pltpu.VMEM((2, 2, half, d), F32),
            pltpu.VMEM((2, 2, half, d), F32),
            dma((2, N // 2, 3)),
            dma((2, N // 2, 3)),
            dma((N, 3)),
            dma((N, 3)),
            dma((N,)),
            dma((2, 2)),
            dma((2, N, 2)),
            dma((2,)),
            dma((2,)),
            dma((2,)),
            dma((3,)),
            dma((2,)),
            dma((2,)),
            dma((2, 2)),
            dma((2,)),
            dma((2, 2)),
        ],
        cost_estimate=pl.CostEstimate(flops=flops, bytes_accessed=2 * N * tok * d * 12, transcendentals=0),
        compiler_params=pltpu.CompilerParams(vmem_limit_bytes=63 * 1024 * 1024, collective_id=0, has_side_effects=True),
    )(x, dy, meta, w1, w3, w2)
    return outs[:6]


def solution(mesh):
    nd = mesh.shape['row'] * mesh.shape['col']
    n = mesh.shape['row']
    grp = ('row', 'col')
    tspec = P(('dp', 'row', 'col'), None)
    wspec = P(grp, None, None)
    gspec = P(('dp', 'row', 'col'), None, None)

    def local(x, ridx, gates, w1, w3, w2, dy):
        tok, d = x.shape
        top = ridx.shape[1]
        el = w1.shape[0]
        ne = el * nd
        cap = min(tok, (4 * tok * top + ne - 1) // ne)
        meta = jnp.concatenate([ridx.astype(F32).T, gates.T], axis=0)
        y, dx, dg, gw1, gw3, gw2 = moe_call(n, cap, meta, x, dy, w1, w3, w2)
        dgt = lax.all_to_all(dg[:, :el, :], grp, 0, 0, tiled=True).reshape(ne, tok)
        pick = ridx.T[:, None, :] == jnp.arange(ne, dtype=jnp.int32)[None, :, None]
        dgates = jnp.sum(jnp.where(pick, dgt[None], 0.0), axis=1).T
        return y, dx, dgates, gw1, gw3, gw2

    return jax.shard_map(local, mesh=mesh, in_specs=(tspec, tspec, tspec, wspec, wspec, wspec, tspec), out_specs=(tspec, tspec, tspec, gspec, gspec, gspec), check_vma=False)
```

```python
import functools

import jax
import jax.numpy as jnp
from jax import lax
from jax.experimental import pallas as pl
from jax.experimental.pallas import tpu as pltpu
from jax.sharding import PartitionSpec as P

BF = jnp.bfloat16
F32 = jnp.float32
MESH = pl.DeviceIdType.MESH


def mm(a, b, dims=((1,), (0,))):
    return lax.dot_general(a, b, (dims, ((), ())), preferred_element_type=F32)


def cycle_index(k, n, x, y):
    return n * ((1 - k) * y + k * x) + (x + y) % n


def cycle_chip(k, n, i):
    r = i // n
    o = (i % n - r + n) % n
    return k * r + (1 - k) * o, k * o + (1 - k) * r


def moe_kernel(n, cap, x_ref, dy_ref, meta_ref, w1_hbm, w3_hbm, w2_hbm,
               y_ref, dx_ref, dgates_ref, gw1_ref, gw3_ref, gw2_ref, xb, db, mb, pown, psib, rin,
               w1_ref, w3_ref, w2_ref, acc1, acc3, acc2, xv, mv, dv_, xs_ref, do_ref, o_ref, dxs_ref, pt_ref, gc_ref, tri_ref,
               stage, pv, ov, om, dg_out, dg_in,
               ag_send, ag_recv, push_send, push_recv, part_recv, rs_send, rs_recv, dg_send, dg_recv,
               ld_x, ld_m, ld_d, ld_w, st_loc, st_rem, ld_p, ld_r, out_sem, ld_o):
    N = n * n
    H = N // 2
    row = lax.axis_index('row')
    col = lax.axis_index('col')
    cx = col // 2
    c = col % 2
    cy = row
    tok, d = x_ref.shape
    top = meta_ref.shape[0] // 2
    el = w1_ref.shape[0]
    half = tok // 2
    pos_k = (cycle_index(0, n, cx, cy), cycle_index(1, n, cx, cy))
    me = (1 - c) * pos_k[0] + c * pos_k[1]
    rank = cy * (2 * n) + 2 * cx + c
    first = rank * el
    nd = 2 * N
    chunks = max(1, tok // 128)
    lane = tok // chunks
    ticks = 6
    rs_unit = max(N // 2, 4)
    rs_done = (ticks * (N - rs_unit)) // 4 if N > rs_unit else 0

    def device(i):
        px, py = cycle_chip(c, n, i)
        return {'row': py, 'col': 2 * px + c}

    nxt = device((me + 1) % N)
    prv = device((me + N - 1) % N)
    sib = {'row': row, 'col': 2 * cx + 1 - c}
    ring = (nxt, prv)

    def rcopy(src, dst, ss, rs, dev):
        return pltpu.make_async_remote_copy(src_ref=src, dst_ref=dst, send_sem=ss, recv_sem=rs, device_id=dev, device_id_type=MESH)

    def peer(p):
        return {'row': p // (2 * n), 'col': p % (2 * n)}

    barrier = pltpu.get_barrier_semaphore()

    def enter(p, carry):
        pl.semaphore_signal(barrier, inc=1, device_id=peer((rank + p) % nd), device_id_type=MESH)
        return carry

    lax.fori_loop(1, nd, enter, 0)
    pl.semaphore_wait(barrier, nd - 1)

    own = (x_ref, meta_ref, dy_ref)
    bufs = (xb, mb, db)

    def ag_copy(q, kind, t, j, src=None):
        slot = bufs[kind].at[c, j]
        return rcopy(slot if src is None else src, slot, ag_send.at[q, t, kind], ag_recv.at[q, t, kind], ring[q])

    def push(kind, j, src=None):
        slot = bufs[kind].at[c, j]
        return rcopy(slot if src is None else src, slot, push_send.at[j, kind], push_recv.at[j, kind], sib)

    def push_arrival(kind, k, j):
        slot = bufs[kind].at[k, j]
        return rcopy(slot, slot, push_send.at[j, kind], push_recv.at[j, kind], sib)

    for kind in (0, 1, 2):
        ag_copy(0, kind, 0, me, own[kind]).start()
        ag_copy(1, kind, 0, me, own[kind]).start()
    for kind in (0, 1, 2):
        push(kind, me, own[kind]).start()

    weights = ((w1_hbm, w1_ref), (w3_hbm, w3_ref), (w2_hbm, w2_ref))
    for i, (src, dst) in enumerate(weights):
        pltpu.make_async_copy(src, dst, ld_w.at[i]).start()
    own_meta = pltpu.make_async_copy(meta_ref, om, ld_o)
    own_meta.start()

    def unit_blocks(u):
        o = (u + 1) // 2
        ka = jnp.where(u == 0, 0, (u + 1) % 2)
        kb = jnp.where(u == N - 1, 1, (u + 1) % 2)
        ia = (1 - ka) * pos_k[0] + ka * pos_k[1]
        ib = (1 - kb) * pos_k[0] + kb * pos_k[1]
        return ((ka, (ia - o + N) % N), (kb, (ib + o) % N))

    def block_loads(u, b, k, j, local):
        slot = u % 2
        src = own if local else (xb.at[k, j], mb.at[k, j], db.at[k, j])
        return (pltpu.make_async_copy(src[0], xv.at[b], ld_x.at[b]),
                pltpu.make_async_copy(src[1], mv.at[b], ld_m.at[b]),
                pltpu.make_async_copy(src[2], dv_.at[slot, b], ld_d.at[b]))

    def start_loads(u):
        for b, (k, j) in enumerate(unit_blocks(u)):
            @pl.when(k != c)
            def _(k=k, j=j):
                for kind in (0, 1, 2):
                    push_arrival(kind, k, j).wait_recv()

            @pl.when(jnp.logical_and(u == 0, k == c))
            def _(b=b, k=k, j=j):
                for cp in block_loads(u, b, k, j, True):
                    cp.start()

            @pl.when(jnp.logical_or(u != 0, k != c))
            def _(b=b, k=k, j=j):
                for cp in block_loads(u, b, k, j, False):
                    cp.start()

    def wait_loads(u):
        for b, (k, j) in enumerate(unit_blocks(u)):
            for cp in block_loads(u, b, k, j, False):
                cp.wait()

    def ag_part(kinds, t):
        for kind in kinds:
            for q in range(2):
                j = (me - t + N) % N if q == 0 else (me + t) % N
                reach = H if (q == 1) == (kind == 2) else H - 1

                @pl.when(t <= reach)
                def _(kind=kind, q=q, j=j, reach=reach):
                    ag_copy(q, kind, t - 1, j).wait_recv()

                    @pl.when(t < reach)
                    def _():
                        ag_copy(q, kind, t, j).start()

                    push(kind, j).start()

    def rs_dest(q, s):
        return (me - 1 - s + 2 * N) % N if q == 0 else (me + 1 + s) % N

    def rows_of(h):
        return pl.ds(pl.multiple_of(h * half, half), half)

    def rs_loads(q, e):
        s, h = e // 2, e % 2
        dst = rs_dest(q, s)
        rows = rows_of(h)
        p0 = pltpu.make_async_copy(pown.at[dst, q, rows], pv.at[q, 0], ld_p.at[q, 0])
        p1 = pltpu.make_async_copy(psib.at[dst, q, rows], pv.at[q, 1], ld_p.at[q, 1])
        r = pltpu.make_async_copy(rin.at[q, jnp.maximum(s - 1, 0), rows], ov.at[q, e % 2], ld_r.at[q])
        return p0, p1, r

    def rs_copy(q, e):
        s, h = e // 2, e % 2
        return rcopy(ov.at[q, e % 2], rin.at[q, s, rows_of(h)], rs_send.at[q, e % 2], rs_recv.at[q, s, h], ring[q])

    def rs_start(q, e):
        s, h = e // 2, e % 2
        fresh = s <= H - 2
        if q == 0:
            fresh = jnp.logical_or(fresh, jnp.logical_or(s == H - 1, s == N - 1))

        @pl.when(jnp.logical_and(h == 0, fresh))
        def _():
            dst = rs_dest(q, s)
            rcopy(psib.at[dst], psib.at[dst], st_rem.at[0], part_recv.at[dst], sib).wait_recv()

        p0, p1, r = rs_loads(q, e)
        p0.start()
        p1.start()

        @pl.when(e >= 2)
        def _():
            rs_copy(q, e - 2).wait_send()
            rs_copy(q, e - 2).wait_recv()
            r.start()

    def rs_finish(q, e):
        p0, p1, r = rs_loads(q, e)
        p0.wait()
        p1.wait()
        step = min(64, half)

        @pl.when(e < 2)
        def _():
            def body(i, _):
                rr = pl.ds(pl.multiple_of(i * step, step), step)
                ov[q, e % 2, rr, :] = pv[q, 0, rr, :] + pv[q, 1, rr, :]
                return 0
            lax.fori_loop(0, half // step, body, 0)

        @pl.when(e >= 2)
        def _():
            r.wait()

            def body(i, _):
                rr = pl.ds(pl.multiple_of(i * step, step), step)
                ov[q, e % 2, rr, :] = ov[q, e % 2, rr, :] + (pv[q, 0, rr, :] + pv[q, 1, rr, :])
                return 0
            lax.fori_loop(0, half // step, body, 0)

        @pl.when(e < 2 * N - 2)
        def _():
            rs_copy(q, e).start()

    def stage_loc(b, j):
        return pltpu.make_async_copy(stage.at[b], pown.at[j], st_loc.at[b])

    def stage_rem(b, j):
        return rcopy(stage.at[b], psib.at[j], st_rem.at[b], part_recv.at[j], sib)

    def source_rank(k, j):
        px, py = cycle_chip(k, n, j)
        return py * (2 * n) + 2 * px + k

    def dg_copy(u, b, p):
        return rcopy(dg_out.at[p], dg_in.at[rank], dg_send.at[u, b], dg_recv, peer(p))

    def stage_start(u):
        for b, (k, j) in enumerate(unit_blocks(u)):
            @pl.when(k == c)
            def _(b=b, j=j):
                stage_loc(b, j).start()

            @pl.when(k != c)
            def _(b=b, j=j):
                stage_rem(b, j).start()

            p = source_rank(k, j)

            @pl.when(p != rank)
            def _(b=b, p=p):
                dg_copy(u, b, p).start()

    def stage_wait(u, local):
        for b, (k, j) in enumerate(unit_blocks(u)):
            if local:
                @pl.when(k == c)
                def _(b=b, j=j):
                    stage_loc(b, j).wait()
            else:
                @pl.when(k != c)
                def _(b=b, j=j):
                    stage_rem(b, j).wait_send()

    start_loads(0)
    tri_ref[...] = (lax.broadcasted_iota(jnp.int32, (tok, tok), 0) <= lax.broadcasted_iota(jnp.int32, (tok, tok), 1)).astype(F32).astype(BF)
    for e in range(el):
        acc1[e] = jnp.zeros(acc1.shape[1:], F32)
        acc3[e] = jnp.zeros(acc3.shape[1:], F32)
        acc2[e] = jnp.zeros(acc2.shape[1:], F32)

    def gather_stage(u):
        rows = lax.broadcasted_iota(jnp.int32, (cap, tok), 0).astype(F32)
        lanes = lax.broadcasted_iota(jnp.int32, (tok, cap), 1).astype(F32)
        for b in range(2):
            ids = mv[b, :top, :]
            gts = mv[b, top:, :]
            masks, gws = [], []
            for e in range(el):
                hit = ids == (first + e).astype(F32)
                masks.append(jnp.sum(jnp.where(hit, 1.0, 0.0), axis=0, keepdims=True))
                gws.append(jnp.sum(jnp.where(hit, gts, 0.0), axis=0, keepdims=True))
            mask = jnp.concatenate(masks + [jnp.zeros((8 - el, tok), F32)], axis=0)
            cum = mm(mask.astype(BF), tri_ref[...])
            pos = jnp.where(mask > 0.0, cum - 1.0, -1.0)
            gw = jnp.concatenate(gws + [jnp.zeros((8 - el, tok), F32)], axis=0)
            cols = jnp.concatenate([pos, gw], axis=0).T
            gc_ref[b] = cols
            for e in range(el):
                hit = rows == pos[e:e + 1, :]
                p = jnp.where(hit, 1.0, 0.0).astype(BF)
                gs = jnp.sum(jnp.where(hit, gw[e:e + 1, :], 0.0), axis=1, keepdims=True)
                pt_ref[b, :, e * cap:(e + 1) * cap] = jnp.where(lanes == cols[:, e:e + 1], 1.0, 0.0).astype(BF)
                xs_ref[e, b * cap:(b + 1) * cap, :] = mm(p, xv[b]).astype(BF)
                do_ref[e, b * cap:(b + 1) * cap, :] = (gs * mm(p, dv_[u % 2, b])).astype(BF)

    def expert(e, tick):
        xs = xs_ref[e]
        uu = mm(xs, w1_ref[e]).astype(BF).astype(F32)
        vv = mm(xs, w3_ref[e]).astype(BF).astype(F32)
        sg = jax.nn.sigmoid(uu)
        a = (uu * sg * vv).astype(BF)
        o_ref[e] = mm(a, w2_ref[e]).astype(BF)
        do = do_ref[e]
        acc2[e] += mm(a, do, ((0,), (0,)))
        da = mm(do, w2_ref[e], ((1,), (1,)))
        du = (da * vv * sg * (1.0 + uu * (1.0 - sg))).astype(BF)
        dv = (da * uu * sg).astype(BF)
        tick()
        acc1[e] += mm(xs, du, ((0,), (0,)))
        acc3[e] += mm(xs, dv, ((0,), (0,)))
        dxs = (mm(du, w1_ref[e], ((1,), (1,))) + mm(dv, w3_ref[e], ((1,), (1,)))).astype(BF)
        for b in range(2):
            dxs_ref[b, e * cap:(e + 1) * cap, :] = dxs[b * cap:(b + 1) * cap, :]

    def scatter_stage(u):
        for b, (k, j) in enumerate(unit_blocks(u)):
            dyf = dv_[u % 2, b].astype(F32)
            yacc = None
            dgs = []
            for e in range(el):
                so = mm(pt_ref[b, :, e * cap:(e + 1) * cap], o_ref[e, b * cap:(b + 1) * cap, :])
                dgs.append(jnp.sum(dyf * so, axis=1, keepdims=True))
                term = gc_ref[b, :, 8 + e:9 + e] * so
                yacc = term if yacc is None else yacc + term
            stage[b, 0] = yacc
            stage[b, 1] = mm(pt_ref[b], dxs_ref[b])
            dg = jnp.concatenate(dgs + [jnp.zeros((tok, 8 - el), F32)], axis=1).T
            pieces = [dg[e:e + 1, i * lane:(i + 1) * lane] for e in range(el) for i in range(chunks)]
            if len(pieces) < 8:
                pieces.append(jnp.zeros((8 - len(pieces), lane), F32))
            dg = jnp.concatenate(pieces, axis=0)
            p = source_rank(k, j)
            dg_out[p] = dg

            @pl.when(p == rank)
            def _(dg=dg):
                dg_in[rank] = dg

    def unit(u, carry):
        live = u >= rs_unit

        def tick(i):
            tau = ticks * u + i
            if i % 2 == 0:
                ahead = tau - 8
                t = ahead // 8 + 2

                @pl.when(jnp.logical_and(jnp.logical_and(ahead >= 0, t <= H), ahead % 8 == 0))
                def _():
                    ag_part((0, 1), t)

                @pl.when(jnp.logical_and(jnp.logical_and(ahead >= 0, t <= H), ahead % 8 == 4))
                def _():
                    ag_part((2,), t)

            ev = (tau - ticks * rs_unit) // 4
            turn = (u % 2 == 0) if i in (0, 1, 4, 5) else (u % 2 == 1)
            turn = jnp.logical_and(live, turn)
            if i % 2 == 0:
                @pl.when(turn)
                def _():
                    rs_start(0, ev)
                    rs_start(1, ev)
            else:
                @pl.when(turn)
                def _():
                    rs_finish(0, ev)
                    rs_finish(1, ev)

        wait_loads(u)

        @pl.when(u >= 1)
        def _():
            stage_wait(u - 1, True)

        gather_stage(u)

        @pl.when(u == 0)
        def _():
            for i, (src, dst) in enumerate(weights):
                pltpu.make_async_copy(src, dst, ld_w.at[i]).wait()

        tick(0)
        expert(0, lambda: tick(1))
        tick(2)
        expert(1, lambda: tick(3))
        tick(4)

        @pl.when(jnp.logical_and(u >= 1, u < N - 1))
        def _():
            start_loads(u + 1)

        @pl.when(u >= 1)
        def _():
            stage_wait(u - 1, False)

        scatter_stage(u)
        stage_start(u)
        tick(5)

        @pl.when(u == 0)
        def _():
            ag_part((0, 1, 2), 1)
            start_loads(1)

        return carry

    lax.fori_loop(0, N, unit, 0)
    stage_wait(N - 1, True)
    grads = ((acc1, gw1_ref), (acc3, gw3_ref), (acc2, gw2_ref))
    for i, (src, dst) in enumerate(grads):
        pltpu.make_async_copy(src, dst, ld_w.at[i]).start()

    def tail(e, carry):
        rs_start(0, e)
        rs_start(1, e)
        rs_finish(0, e)
        rs_finish(1, e)

        @pl.when(e >= 2 * N - 2)
        def _():
            rows = rows_of(e % 2)
            for q, out in ((0, y_ref), (1, dx_ref)):
                xs_ref[q, rows, :] = ov[q, e % 2].astype(BF)
                pltpu.make_async_copy(xs_ref.at[q, rows], out.at[rows], out_sem.at[q, e % 2]).start()
        return carry

    lax.fori_loop(rs_done, 2 * N, tail, 0)

    own_meta.wait()
    rcopy(dg_in.at[pl.ds(0, nd - 1)], dg_in.at[pl.ds(0, nd - 1)], dg_send.at[0, 0], dg_recv, sib).wait_recv()
    for i in range(chunks):
        lanes = slice(i * lane, (i + 1) * lane)
        ids = om[:top, lanes]

        def pick(p, total, ids=ids, i=i):
            for e in range(el):
                row = e * chunks + i
                total = total + jnp.where(ids == (p * el + e).astype(F32), dg_in[p, row:row + 1, :], 0.0)
            return total

        dgates_ref[:, lanes] = lax.fori_loop(0, nd, pick, jnp.zeros((top, lane), F32))

    def drain_dg(u, carry):
        for b, (k, j) in enumerate(unit_blocks(u)):
            p = source_rank(k, j)

            @pl.when(p != rank)
            def _(b=b, p=p):
                dg_copy(u, b, p).wait_send()
        return carry

    lax.fori_loop(0, N, drain_dg, 0)

    stage_wait(N - 1, False)
    for q, out in ((0, y_ref), (1, dx_ref)):
        for h in range(2):
            rows = pl.ds(h * half, half)
            pltpu.make_async_copy(xs_ref.at[q, rows], out.at[rows], out_sem.at[q, h]).wait()
    for i, (src, dst) in enumerate(grads):
        pltpu.make_async_copy(src, dst, ld_w.at[i]).wait()
    for kind, long_q in ((0, 0), (1, 0), (2, 1)):
        for q in range(2):
            reach = H if q == long_q else H - 1

            def drain(t, carry, kind=kind, q=q):
                ag_copy(q, kind, t, me).wait_send()
                return carry
            lax.fori_loop(0, reach, drain, 0)

        def drain_push(j, carry, kind=kind):
            push(kind, j).wait_send()
            return carry
        lax.fori_loop(0, N, drain_push, 0)


def moe_call(n, cap, meta, x, dy, w1, w3, w2):
    N = n * n
    tok, d = x.shape
    el, _, f = w1.shape
    half = tok // 2
    any_spec = pl.BlockSpec(memory_space=pl.ANY)
    vm = pl.BlockSpec(memory_space=pltpu.VMEM)
    flops = 13 * 2 * 2 * N * el * cap * d * f
    shape = jax.ShapeDtypeStruct
    dma = pltpu.SemaphoreType.DMA
    outs = pl.pallas_call(
        functools.partial(moe_kernel, n, cap),
        in_specs=[any_spec] * 6,
        out_specs=[any_spec, any_spec, vm] + [any_spec] * 9,
        out_shape=[
            shape((tok, d), BF),
            shape((tok, d), BF),
            shape((meta.shape[0] // 2, tok), F32),
            shape((el, d, f), F32),
            shape((el, d, f), F32),
            shape((el, f, d), F32),
            shape((2, N, tok, d), BF),
            shape((2, N, tok, d), BF),
            shape((2, N) + meta.shape, F32),
            shape((N, 2, tok, d), F32),
            shape((N, 2, tok, d), F32),
            shape((2, N - 1, tok, d), F32),
        ],
        scratch_shapes=[
            pltpu.VMEM((el, d, f), BF),
            pltpu.VMEM((el, d, f), BF),
            pltpu.VMEM((el, f, d), BF),
            pltpu.VMEM((el, d, f), F32),
            pltpu.VMEM((el, d, f), F32),
            pltpu.VMEM((el, f, d), F32),
            pltpu.VMEM((2, tok, d), BF),
            pltpu.VMEM((2,) + meta.shape, F32),
            pltpu.VMEM((2, 2, tok, d), BF),
            pltpu.VMEM((el, 2 * cap, d), BF),
            pltpu.VMEM((el, 2 * cap, d), BF),
            pltpu.VMEM((el, 2 * cap, d), BF),
            pltpu.VMEM((2, el * cap, d), BF),
            pltpu.VMEM((2, tok, el * cap), BF),
            pltpu.VMEM((2, tok, 16), F32),
            pltpu.VMEM((tok, tok), BF),
            pltpu.VMEM((2, 2, tok, d), F32),
            pltpu.VMEM((2, 2, half, d), F32),
            pltpu.VMEM((2, 2, half, d), F32),
            pltpu.VMEM(meta.shape, F32),
            pltpu.VMEM((2 * N, 8, tok // max(1, tok // 128)), F32),
            pltpu.VMEM((2 * N, 8, tok // max(1, tok // 128)), F32),
            dma((2, N // 2, 3)),
            dma((2, N // 2, 3)),
            dma((N, 3)),
            dma((N, 3)),
            dma((N,)),
            dma((2, 2)),
            dma((2, N, 2)),
            dma((N, 2)),
            dma(()),
            dma((2,)),
            dma((2,)),
            dma((2,)),
            dma((3,)),
            dma((2,)),
            dma((2,)),
            dma((2, 2)),
            dma((2,)),
            dma((2, 2)),
            dma(()),
        ],
        cost_estimate=pl.CostEstimate(flops=flops, bytes_accessed=2 * N * tok * d * 12, transcendentals=0),
        compiler_params=pltpu.CompilerParams(vmem_limit_bytes=63 * 1024 * 1024, collective_id=0, has_side_effects=True),
    )(x, dy, meta, w1, w3, w2)
    return outs[:6]


def solution(mesh):
    nd = mesh.shape['row'] * mesh.shape['col']
    n = mesh.shape['row']
    grp = ('row', 'col')
    tspec = P(('dp', 'row', 'col'), None)
    wspec = P(grp, None, None)
    gspec = P(('dp', 'row', 'col'), None, None)

    def local(x, ridx, gates, w1, w3, w2, dy):
        tok, d = x.shape
        top = ridx.shape[1]
        el = w1.shape[0]
        ne = el * nd
        cap = min(tok, (4 * tok * top + ne - 1) // ne)
        meta = jnp.concatenate([ridx.astype(F32).T, gates.T], axis=0)
        y, dx, dgt, gw1, gw3, gw2 = moe_call(n, cap, meta, x, dy, w1, w3, w2)
        dgates = dgt.T
        return y, dx, dgates, gw1, gw3, gw2

    return jax.shard_map(local, mesh=mesh, in_specs=(tspec, tspec, tspec, wspec, wspec, wspec, tspec), out_specs=(tspec, tspec, tspec, gspec, gspec, gspec), check_vma=False)
```

```python
import functools

import jax
import jax.numpy as jnp
from jax import lax
from jax.experimental import pallas as pl
from jax.experimental.pallas import tpu as pltpu
from jax.sharding import PartitionSpec as P

BF = jnp.bfloat16
F32 = jnp.float32
MESH = pl.DeviceIdType.MESH


def mm(a, b, dims=((1,), (0,))):
    return lax.dot_general(a, b, (dims, ((), ())), preferred_element_type=F32)


def cycle_index(k, n, x, y):
    return n * ((1 - k) * y + k * x) + (x + y) % n


def cycle_chip(k, n, i):
    r = i // n
    o = (i % n - r + n) % n
    return k * r + (1 - k) * o, k * o + (1 - k) * r


def moe_kernel(n, cap, x_ref, dy_ref, meta_ref, w1_hbm, w3_hbm, w2_hbm,
               y_ref, dx_ref, dgates_ref, gw1_ref, gw3_ref, gw2_ref, xb, db, mb, pown, psib, rin,
               w1_ref, w3_ref, w2_ref, acc1, acc3, acc2, xv, mv, dv_, xs_ref, do_ref, o_ref, dxs_ref, du_ref, dw_ref, pt_ref, gc_ref, tri_ref,
               stage, pv, ov, om, dg_out, dg_in,
               ag_send, ag_recv, push_send, push_recv, part_recv, rs_send, rs_recv, dg_send, dg_recv,
               ld_x, ld_m, ld_d, ld_w, st_loc, st_rem, ld_p, ld_r, out_sem, ld_o):
    N = n * n
    H = N // 2
    row = lax.axis_index('row')
    col = lax.axis_index('col')
    cx = col // 2
    c = col % 2
    cy = row
    tok, d = x_ref.shape
    top = meta_ref.shape[0] // 2
    el = w1_ref.shape[0]
    half = tok // 2
    pos_k = (cycle_index(0, n, cx, cy), cycle_index(1, n, cx, cy))
    me = (1 - c) * pos_k[0] + c * pos_k[1]
    rank = cy * (2 * n) + 2 * cx + c
    first = rank * el
    nd = 2 * N
    chunks = max(1, tok // 128)
    lane = tok // chunks
    ticks = 3
    rs_unit = max(N // 2, 4)
    rs_done = (ticks * (N - rs_unit)) // 2 if N > rs_unit else 0

    def device(i):
        px, py = cycle_chip(c, n, i)
        return {'row': py, 'col': 2 * px + c}

    nxt = device((me + 1) % N)
    prv = device((me + N - 1) % N)
    sib = {'row': row, 'col': 2 * cx + 1 - c}
    ring = (nxt, prv)

    def rcopy(src, dst, ss, rs, dev):
        return pltpu.make_async_remote_copy(src_ref=src, dst_ref=dst, send_sem=ss, recv_sem=rs, device_id=dev, device_id_type=MESH)

    def peer(p):
        return {'row': p // (2 * n), 'col': p % (2 * n)}

    barrier = pltpu.get_barrier_semaphore()

    def enter(p, carry):
        pl.semaphore_signal(barrier, inc=1, device_id=peer((rank + p) % nd), device_id_type=MESH)
        return carry

    lax.fori_loop(1, nd, enter, 0)
    pl.semaphore_wait(barrier, nd - 1)

    own = (x_ref, meta_ref, dy_ref)
    bufs = (xb, mb, db)

    def ag_copy(q, kind, t, j, src=None):
        slot = bufs[kind].at[c, j]
        return rcopy(slot if src is None else src, slot, ag_send.at[q, t, kind], ag_recv.at[q, t, kind], ring[q])

    def push(kind, j, src=None):
        slot = bufs[kind].at[c, j]
        return rcopy(slot if src is None else src, slot, push_send.at[j, kind], push_recv.at[j, kind], sib)

    def push_arrival(kind, k, j):
        slot = bufs[kind].at[k, j]
        return rcopy(slot, slot, push_send.at[j, kind], push_recv.at[j, kind], sib)

    for kind in (0, 1, 2):
        ag_copy(0, kind, 0, me, own[kind]).start()
        ag_copy(1, kind, 0, me, own[kind]).start()
    for kind in (0, 1, 2):
        push(kind, me, own[kind]).start()

    weights = ((w1_hbm, w1_ref), (w3_hbm, w3_ref), (w2_hbm, w2_ref))
    for i, (src, dst) in enumerate(weights):
        pltpu.make_async_copy(src, dst, ld_w.at[i]).start()
    own_meta = pltpu.make_async_copy(meta_ref, om, ld_o)
    own_meta.start()

    def unit_blocks(u):
        o = (u + 1) // 2
        ka = jnp.where(u == 0, 0, (u + 1) % 2)
        kb = jnp.where(u == N - 1, 1, (u + 1) % 2)
        ia = (1 - ka) * pos_k[0] + ka * pos_k[1]
        ib = (1 - kb) * pos_k[0] + kb * pos_k[1]
        return ((ka, (ia - o + N) % N), (kb, (ib + o) % N))

    def block_loads(u, b, k, j, local):
        slot = u % 2
        src = own if local else (xb.at[k, j], mb.at[k, j], db.at[k, j])
        return (pltpu.make_async_copy(src[0], xv.at[b], ld_x.at[b]),
                pltpu.make_async_copy(src[1], mv.at[b], ld_m.at[b]),
                pltpu.make_async_copy(src[2], dv_.at[slot, b], ld_d.at[b]))

    def start_loads(u):
        for b, (k, j) in enumerate(unit_blocks(u)):
            @pl.when(k != c)
            def _(k=k, j=j):
                for kind in (0, 1, 2):
                    push_arrival(kind, k, j).wait_recv()

            @pl.when(jnp.logical_and(u == 0, k == c))
            def _(b=b, k=k, j=j):
                for cp in block_loads(u, b, k, j, True):
                    cp.start()

            @pl.when(jnp.logical_or(u != 0, k != c))
            def _(b=b, k=k, j=j):
                for cp in block_loads(u, b, k, j, False):
                    cp.start()

    def wait_loads(u):
        for b, (k, j) in enumerate(unit_blocks(u)):
            for cp in block_loads(u, b, k, j, False):
                cp.wait()

    def ag_part(kinds, t):
        for kind in kinds:
            for q in range(2):
                j = (me - t + N) % N if q == 0 else (me + t) % N
                reach = H if (q == 1) == (kind == 2) else H - 1

                @pl.when(t <= reach)
                def _(kind=kind, q=q, j=j, reach=reach):
                    ag_copy(q, kind, t - 1, j).wait_recv()

                    @pl.when(t < reach)
                    def _():
                        ag_copy(q, kind, t, j).start()

                    push(kind, j).start()

    def rs_dest(q, s):
        return (me - 1 - s + 2 * N) % N if q == 0 else (me + 1 + s) % N

    def rows_of(h):
        return pl.ds(pl.multiple_of(h * half, half), half)

    def rs_loads(q, e):
        s, h = e // 2, e % 2
        dst = rs_dest(q, s)
        rows = rows_of(h)
        p0 = pltpu.make_async_copy(pown.at[dst, q, rows], pv.at[q, 0], ld_p.at[q, 0])
        p1 = pltpu.make_async_copy(psib.at[dst, q, rows], pv.at[q, 1], ld_p.at[q, 1])
        r = pltpu.make_async_copy(rin.at[q, jnp.maximum(s - 1, 0), rows], ov.at[q, e % 2], ld_r.at[q])
        return p0, p1, r

    def rs_copy(q, e):
        s, h = e // 2, e % 2
        return rcopy(ov.at[q, e % 2], rin.at[q, s, rows_of(h)], rs_send.at[q, e % 2], rs_recv.at[q, s, h], ring[q])

    def rs_start(q, e):
        s, h = e // 2, e % 2
        fresh = s <= H - 2
        if q == 0:
            fresh = jnp.logical_or(fresh, jnp.logical_or(s == H - 1, s == N - 1))

        @pl.when(jnp.logical_and(h == 0, fresh))
        def _():
            dst = rs_dest(q, s)
            rcopy(psib.at[dst], psib.at[dst], st_rem.at[0], part_recv.at[dst], sib).wait_recv()

        p0, p1, r = rs_loads(q, e)
        p0.start()
        p1.start()

        @pl.when(e >= 2)
        def _():
            rs_copy(q, e - 2).wait_send()
            rs_copy(q, e - 2).wait_recv()
            r.start()

    def rs_finish(q, e):
        p0, p1, r = rs_loads(q, e)
        p0.wait()
        p1.wait()
        step = min(64, half)

        @pl.when(e < 2)
        def _():
            def body(i, _):
                rr = pl.ds(pl.multiple_of(i * step, step), step)
                ov[q, e % 2, rr, :] = pv[q, 0, rr, :] + pv[q, 1, rr, :]
                return 0
            lax.fori_loop(0, half // step, body, 0)

        @pl.when(e >= 2)
        def _():
            r.wait()

            def body(i, _):
                rr = pl.ds(pl.multiple_of(i * step, step), step)
                ov[q, e % 2, rr, :] = ov[q, e % 2, rr, :] + (pv[q, 0, rr, :] + pv[q, 1, rr, :])
                return 0
            lax.fori_loop(0, half // step, body, 0)

        @pl.when(e < 2 * N - 2)
        def _():
            rs_copy(q, e).start()

    def stage_loc(b, j):
        return pltpu.make_async_copy(stage.at[b], pown.at[j], st_loc.at[b])

    def stage_rem(b, j):
        return rcopy(stage.at[b], psib.at[j], st_rem.at[b], part_recv.at[j], sib)

    def source_rank(k, j):
        px, py = cycle_chip(k, n, j)
        return py * (2 * n) + 2 * px + k

    def dg_copy(u, b, p):
        return rcopy(dg_out.at[p], dg_in.at[rank], dg_send.at[u, b], dg_recv, peer(p))

    def stage_start(u):
        for b, (k, j) in enumerate(unit_blocks(u)):
            @pl.when(k == c)
            def _(b=b, j=j):
                stage_loc(b, j).start()

            @pl.when(k != c)
            def _(b=b, j=j):
                stage_rem(b, j).start()

            p = source_rank(k, j)

            @pl.when(p != rank)
            def _(b=b, p=p):
                dg_copy(u, b, p).start()

    def stage_wait(u, local):
        for b, (k, j) in enumerate(unit_blocks(u)):
            if local:
                @pl.when(k == c)
                def _(b=b, j=j):
                    stage_loc(b, j).wait()
            else:
                @pl.when(k != c)
                def _(b=b, j=j):
                    stage_rem(b, j).wait_send()

    start_loads(0)
    tri_ref[...] = (lax.broadcasted_iota(jnp.int32, (tok, tok), 0) <= lax.broadcasted_iota(jnp.int32, (tok, tok), 1)).astype(F32).astype(BF)
    for e in range(el):
        acc1[e] = jnp.zeros(acc1.shape[1:], F32)
        acc3[e] = jnp.zeros(acc3.shape[1:], F32)
        acc2[e] = jnp.zeros(acc2.shape[1:], F32)

    def gather_stage(u):
        rows = lax.broadcasted_iota(jnp.int32, (cap, tok), 0).astype(F32)
        lanes = lax.broadcasted_iota(jnp.int32, (tok, cap), 1).astype(F32)
        for b in range(2):
            ids = mv[b, :top, :]
            gts = mv[b, top:, :]
            masks, gws = [], []
            for e in range(el):
                hit = ids == (first + e).astype(F32)
                masks.append(jnp.sum(jnp.where(hit, 1.0, 0.0), axis=0, keepdims=True))
                gws.append(jnp.sum(jnp.where(hit, gts, 0.0), axis=0, keepdims=True))
            mask = jnp.concatenate(masks + [jnp.zeros((8 - el, tok), F32)], axis=0)
            cum = mm(mask.astype(BF), tri_ref[...])
            pos = jnp.where(mask > 0.0, cum - 1.0, -1.0)
            gw = jnp.concatenate(gws + [jnp.zeros((8 - el, tok), F32)], axis=0)
            cols = jnp.concatenate([pos, gw], axis=0).T
            gc_ref[b] = cols
            picks = []
            scales = []
            for e in range(el):
                hit = rows == pos[e:e + 1, :]
                picks.append(jnp.where(hit, 1.0, 0.0).astype(BF))
                scales.append(jnp.sum(jnp.where(hit, gw[e:e + 1, :], 0.0), axis=1, keepdims=True))
                pt_ref[b, :, e * cap:(e + 1) * cap] = jnp.where(lanes == cols[:, e:e + 1], 1.0, 0.0).astype(BF)
            p = jnp.concatenate(picks, axis=0)
            xr = mm(p, xv[b]).astype(BF)
            dr = (jnp.concatenate(scales, axis=0) * mm(p, dv_[u % 2, b])).astype(BF)
            for e in range(el):
                xs_ref[e, b * cap:(b + 1) * cap, :] = xr[e * cap:(e + 1) * cap]
                do_ref[e, b * cap:(b + 1) * cap, :] = dr[e * cap:(e + 1) * cap]

    def expert_a(e):
        xs = xs_ref[e]
        uu = mm(xs, w1_ref[e]).astype(BF).astype(F32)
        vv = mm(xs, w3_ref[e]).astype(BF).astype(F32)
        sg = jax.nn.sigmoid(uu)
        a = (uu * sg * vv).astype(BF)
        o_ref[e] = mm(a, w2_ref[e]).astype(BF)
        do = do_ref[e]
        da = mm(do, w2_ref[e], ((1,), (1,)))
        du_ref[e] = (da * vv * sg * (1.0 + uu * (1.0 - sg))).astype(BF)
        dw_ref[e] = (da * uu * sg).astype(BF)
        acc2[e] += mm(a, do, ((0,), (0,)))

    def expert_b(e):
        xs = xs_ref[e]
        du = du_ref[e]
        dw = dw_ref[e]
        dxs = (mm(du, w1_ref[e], ((1,), (1,))) + mm(dw, w3_ref[e], ((1,), (1,)))).astype(BF)
        for b in range(2):
            dxs_ref[b, e * cap:(e + 1) * cap, :] = dxs[b * cap:(b + 1) * cap, :]
        acc1[e] += mm(xs, du, ((0,), (0,)))
        acc3[e] += mm(xs, dw, ((0,), (0,)))

    def scatter_stage(u):
        for b, (k, j) in enumerate(unit_blocks(u)):
            dyf = dv_[u % 2, b].astype(F32)
            yacc = None
            dgs = []
            for e in range(el):
                so = mm(pt_ref[b, :, e * cap:(e + 1) * cap], o_ref[e, b * cap:(b + 1) * cap, :])
                dgs.append(jnp.sum(dyf * so, axis=1, keepdims=True))
                term = gc_ref[b, :, 8 + e:9 + e] * so
                yacc = term if yacc is None else yacc + term
            stage[b, 0] = yacc
            stage[b, 1] = mm(pt_ref[b], dxs_ref[b])
            dg = jnp.concatenate(dgs + [jnp.zeros((tok, 8 - el), F32)], axis=1).T
            pieces = [dg[e:e + 1, i * lane:(i + 1) * lane] for e in range(el) for i in range(chunks)]
            if len(pieces) < 8:
                pieces.append(jnp.zeros((8 - len(pieces), lane), F32))
            dg = jnp.concatenate(pieces, axis=0)
            p = source_rank(k, j)
            dg_out[p] = dg

            @pl.when(p == rank)
            def _(dg=dg):
                dg_in[rank] = dg

    def unit(u, carry):
        live = u >= rs_unit

        def tick(i):
            tau = ticks * u + i
            ahead = tau - 4
            t = ahead // 4 + 2
            due = jnp.logical_and(ahead >= 0, t <= H)

            @pl.when(jnp.logical_and(due, ahead % 4 == 0))
            def _():
                ag_part((0, 1), t)

            @pl.when(jnp.logical_and(due, ahead % 4 == 2))
            def _():
                ag_part((2,), t)

            turn = tau - ticks * rs_unit

            @pl.when(jnp.logical_and(live, turn % 2 == 0))
            def _():
                rs_start(0, turn // 2)
                rs_start(1, turn // 2)

            @pl.when(jnp.logical_and(live, turn % 2 == 1))
            def _():
                rs_finish(0, turn // 2)
                rs_finish(1, turn // 2)

        wait_loads(u)

        @pl.when(u == 0)
        def _():
            for i, (src, dst) in enumerate(weights):
                pltpu.make_async_copy(src, dst, ld_w.at[i]).wait()

        gather_stage(u)
        expert_a(0)
        tick(0)
        expert_a(1)
        expert_b(0)
        tick(1)

        @pl.when(u >= 1)
        def _():
            stage_wait(u - 1, True)
            stage_wait(u - 1, False)

            @pl.when(u < N - 1)
            def _():
                start_loads(u + 1)

        expert_b(1)
        scatter_stage(u)
        stage_start(u)
        tick(2)

        @pl.when(u == 0)
        def _():
            ag_part((0, 1, 2), 1)
            start_loads(1)

        return carry

    lax.fori_loop(0, N, unit, 0)
    stage_wait(N - 1, True)
    grads = ((acc1, gw1_ref), (acc3, gw3_ref), (acc2, gw2_ref))
    for i, (src, dst) in enumerate(grads):
        pltpu.make_async_copy(src, dst, ld_w.at[i]).start()

    def tail(e, carry):
        rs_start(0, e)
        rs_start(1, e)
        rs_finish(0, e)
        rs_finish(1, e)

        @pl.when(e >= 2 * N - 2)
        def _():
            rows = rows_of(e % 2)
            for q, out in ((0, y_ref), (1, dx_ref)):
                xs_ref[q, rows, :] = ov[q, e % 2].astype(BF)
                pltpu.make_async_copy(xs_ref.at[q, rows], out.at[rows], out_sem.at[q, e % 2]).start()
        return carry

    lax.fori_loop(rs_done, 2 * N, tail, 0)

    own_meta.wait()
    rcopy(dg_in.at[pl.ds(0, nd - 1)], dg_in.at[pl.ds(0, nd - 1)], dg_send.at[0, 0], dg_recv, sib).wait_recv()
    for i in range(chunks):
        lanes = slice(i * lane, (i + 1) * lane)
        ids = om[:top, lanes]

        def pick(p, total, ids=ids, i=i):
            for e in range(el):
                row = e * chunks + i
                total = total + jnp.where(ids == (p * el + e).astype(F32), dg_in[p, row:row + 1, :], 0.0)
            return total

        dgates_ref[:, lanes] = lax.fori_loop(0, nd, pick, jnp.zeros((top, lane), F32))

    def drain_dg(u, carry):
        for b, (k, j) in enumerate(unit_blocks(u)):
            p = source_rank(k, j)

            @pl.when(p != rank)
            def _(b=b, p=p):
                dg_copy(u, b, p).wait_send()
        return carry

    lax.fori_loop(0, N, drain_dg, 0)

    stage_wait(N - 1, False)
    for q, out in ((0, y_ref), (1, dx_ref)):
        for h in range(2):
            rows = pl.ds(h * half, half)
            pltpu.make_async_copy(xs_ref.at[q, rows], out.at[rows], out_sem.at[q, h]).wait()
    for i, (src, dst) in enumerate(grads):
        pltpu.make_async_copy(src, dst, ld_w.at[i]).wait()
    for kind, long_q in ((0, 0), (1, 0), (2, 1)):
        for q in range(2):
            reach = H if q == long_q else H - 1

            def drain(t, carry, kind=kind, q=q):
                ag_copy(q, kind, t, me).wait_send()
                return carry
            lax.fori_loop(0, reach, drain, 0)

        def drain_push(j, carry, kind=kind):
            push(kind, j).wait_send()
            return carry
        lax.fori_loop(0, N, drain_push, 0)


def moe_call(n, cap, meta, x, dy, w1, w3, w2):
    N = n * n
    tok, d = x.shape
    el, _, f = w1.shape
    half = tok // 2
    any_spec = pl.BlockSpec(memory_space=pl.ANY)
    vm = pl.BlockSpec(memory_space=pltpu.VMEM)
    flops = 13 * 2 * 2 * N * el * cap * d * f
    shape = jax.ShapeDtypeStruct
    dma = pltpu.SemaphoreType.DMA
    outs = pl.pallas_call(
        functools.partial(moe_kernel, n, cap),
        in_specs=[any_spec] * 6,
        out_specs=[any_spec, any_spec, vm] + [any_spec] * 9,
        out_shape=[
            shape((tok, d), BF),
            shape((tok, d), BF),
            shape((meta.shape[0] // 2, tok), F32),
            shape((el, d, f), F32),
            shape((el, d, f), F32),
            shape((el, f, d), F32),
            shape((2, N, tok, d), BF),
            shape((2, N, tok, d), BF),
            shape((2, N) + meta.shape, F32),
            shape((N, 2, tok, d), F32),
            shape((N, 2, tok, d), F32),
            shape((2, N - 1, tok, d), F32),
        ],
        scratch_shapes=[
            pltpu.VMEM((el, d, f), BF),
            pltpu.VMEM((el, d, f), BF),
            pltpu.VMEM((el, f, d), BF),
            pltpu.VMEM((el, d, f), F32),
            pltpu.VMEM((el, d, f), F32),
            pltpu.VMEM((el, f, d), F32),
            pltpu.VMEM((2, tok, d), BF),
            pltpu.VMEM((2,) + meta.shape, F32),
            pltpu.VMEM((2, 2, tok, d), BF),
            pltpu.VMEM((el, 2 * cap, d), BF),
            pltpu.VMEM((el, 2 * cap, d), BF),
            pltpu.VMEM((el, 2 * cap, d), BF),
            pltpu.VMEM((2, el * cap, d), BF),
            pltpu.VMEM((el, 2 * cap, f), BF),
            pltpu.VMEM((el, 2 * cap, f), BF),
            pltpu.VMEM((2, tok, el * cap), BF),
            pltpu.VMEM((2, tok, 16), F32),
            pltpu.VMEM((tok, tok), BF),
            pltpu.VMEM((2, 2, tok, d), F32),
            pltpu.VMEM((2, 2, half, d), F32),
            pltpu.VMEM((2, 2, half, d), F32),
            pltpu.VMEM(meta.shape, F32),
            pltpu.VMEM((2 * N, 8, tok // max(1, tok // 128)), F32),
            pltpu.VMEM((2 * N, 8, tok // max(1, tok // 128)), F32),
            dma((2, N // 2, 3)),
            dma((2, N // 2, 3)),
            dma((N, 3)),
            dma((N, 3)),
            dma((N,)),
            dma((2, 2)),
            dma((2, N, 2)),
            dma((N, 2)),
            dma(()),
            dma((2,)),
            dma((2,)),
            dma((2,)),
            dma((3,)),
            dma((2,)),
            dma((2,)),
            dma((2, 2)),
            dma((2,)),
            dma((2, 2)),
            dma(()),
        ],
        cost_estimate=pl.CostEstimate(flops=flops, bytes_accessed=2 * N * tok * d * 12, transcendentals=0),
        compiler_params=pltpu.CompilerParams(vmem_limit_bytes=63 * 1024 * 1024, collective_id=0, has_side_effects=True),
    )(x, dy, meta, w1, w3, w2)
    return outs[:6]


def solution(mesh):
    nd = mesh.shape['row'] * mesh.shape['col']
    n = mesh.shape['row']
    grp = ('row', 'col')
    tspec = P(('dp', 'row', 'col'), None)
    wspec = P(grp, None, None)
    gspec = P(('dp', 'row', 'col'), None, None)

    def local(x, ridx, gates, w1, w3, w2, dy):
        tok, d = x.shape
        top = ridx.shape[1]
        el = w1.shape[0]
        ne = el * nd
        cap = min(tok, (4 * tok * top + ne - 1) // ne)
        meta = jnp.concatenate([ridx.astype(F32).T, gates.T], axis=0)
        y, dx, dgt, gw1, gw3, gw2 = moe_call(n, cap, meta, x, dy, w1, w3, w2)
        dgates = dgt.T
        return y, dx, dgates, gw1, gw3, gw2

    return jax.shard_map(local, mesh=mesh, in_specs=(tspec, tspec, tspec, wspec, wspec, wspec, tspec), out_specs=(tspec, tspec, tspec, gspec, gspec, gspec), check_vma=False)
```

```python
import functools

import jax
import jax.numpy as jnp
from jax import lax
from jax.experimental import pallas as pl
from jax.experimental.pallas import tpu as pltpu
from jax.sharding import PartitionSpec as P

BF = jnp.bfloat16
F32 = jnp.float32
MESH = pl.DeviceIdType.MESH


def mm(a, b, dims=((1,), (0,))):
    return lax.dot_general(a, b, (dims, ((), ())), preferred_element_type=F32)


def cycle_index(k, n, x, y):
    return n * ((1 - k) * y + k * x) + (x + y) % n


def cycle_chip(k, n, i):
    r = i // n
    o = (i % n - r + n) % n
    return k * r + (1 - k) * o, k * o + (1 - k) * r


def moe_kernel(n, cap, x_ref, dy_ref, ids_ref, gates_ref, w1_hbm, w3_hbm, w2_hbm,
               y_ref, dx_ref, dgates_ref, gw1_ref, gw3_ref, gw2_ref, xb, db, mb, pown, psib, rin,
               w1_ref, w3_ref, w2_ref, acc1, acc3, acc2, xv, mv, dv_, xs_ref, do_ref, o_ref, dxs_ref, du_ref, dw_ref, pt_ref, gc_ref, tri_ref,
               stage, pv, ov, om, oi, dg_out, dg_in,
               ag_send, ag_recv, push_send, push_recv, part_recv, rs_send, rs_recv, dg_send, dg_recv,
               ld_x, ld_m, ld_d, ld_w, st_loc, st_rem, ld_p, ld_r, out_sem, ld_o):
    N = n * n
    H = N // 2
    row = lax.axis_index('row')
    col = lax.axis_index('col')
    cx = col // 2
    c = col % 2
    cy = row
    tok, d = x_ref.shape
    top = ids_ref.shape[0]
    el = w1_ref.shape[0]
    half = tok // 2
    pos_k = (cycle_index(0, n, cx, cy), cycle_index(1, n, cx, cy))
    me = (1 - c) * pos_k[0] + c * pos_k[1]
    rank = cy * (2 * n) + 2 * cx + c
    first = rank * el
    nd = 2 * N
    chunks = max(1, tok // 128)
    lane = tok // chunks
    ticks = 3
    rs_unit = max(N // 2, 4)
    rs_done = (ticks * (N - rs_unit)) // 2 if N > rs_unit else 0

    def device(i):
        px, py = cycle_chip(c, n, i)
        return {'row': py, 'col': 2 * px + c}

    nxt = device((me + 1) % N)
    prv = device((me + N - 1) % N)
    sib = {'row': row, 'col': 2 * cx + 1 - c}
    ring = (nxt, prv)

    def rcopy(src, dst, ss, rs, dev):
        return pltpu.make_async_remote_copy(src_ref=src, dst_ref=dst, send_sem=ss, recv_sem=rs, device_id=dev, device_id_type=MESH)

    def peer(p):
        return {'row': p // (2 * n), 'col': p % (2 * n)}

    barrier = pltpu.get_barrier_semaphore()
    for dr in range(n):
        for dc in range(2 * n):
            if dr or dc:
                dev = {'row': (row + dr) % n, 'col': (col + dc) % (2 * n)}
                pl.semaphore_signal(barrier, inc=1, device_id=dev, device_id_type=MESH)
    small = (pltpu.make_async_copy(ids_ref, oi, ld_o.at[0]), pltpu.make_async_copy(gates_ref, om.at[pl.ds(top, top)], ld_o.at[1]))
    for cp in small:
        cp.start()
    pl.semaphore_wait(barrier, nd - 1)

    own = (x_ref, om, dy_ref)
    bufs = (xb, mb, db)

    def ag_copy(q, kind, t, j, src=None):
        slot = bufs[kind].at[c, j]
        return rcopy(slot if src is None else src, slot, ag_send.at[q, t, kind], ag_recv.at[q, t, kind], ring[q])

    def push(kind, j, src=None):
        slot = bufs[kind].at[c, j]
        return rcopy(slot if src is None else src, slot, push_send.at[j, kind], push_recv.at[j, kind], sib)

    def push_arrival(kind, k, j):
        slot = bufs[kind].at[k, j]
        return rcopy(slot, slot, push_send.at[j, kind], push_recv.at[j, kind], sib)

    for kind in (0, 1, 2):
        if kind == 1:
            for cp in small:
                cp.wait()
            om[:top, :] = oi[...].astype(F32)
        ag_copy(0, kind, 0, me, own[kind]).start()
        ag_copy(1, kind, 0, me, own[kind]).start()
        push(kind, me, own[kind]).start()

    weights = ((w1_hbm, w1_ref), (w3_hbm, w3_ref), (w2_hbm, w2_ref))
    for i, (src, dst) in enumerate(weights):
        pltpu.make_async_copy(src, dst, ld_w.at[i]).start()

    def unit_blocks(u):
        o = (u + 1) // 2
        ka = jnp.where(u == 0, 0, (u + 1) % 2)
        kb = jnp.where(u == N - 1, 1, (u + 1) % 2)
        ia = (1 - ka) * pos_k[0] + ka * pos_k[1]
        ib = (1 - kb) * pos_k[0] + kb * pos_k[1]
        return ((ka, (ia - o + N) % N), (kb, (ib + o) % N))

    def block_loads(u, b, k, j, local):
        slot = u % 2
        cps = [pltpu.make_async_copy(x_ref if local else xb.at[k, j], xv.at[b], ld_x.at[b]),
               pltpu.make_async_copy(dy_ref if local else db.at[k, j], dv_.at[slot, b], ld_d.at[b])]
        if not local:
            cps.append(pltpu.make_async_copy(mb.at[k, j], mv.at[b], ld_m.at[b]))
        return cps

    def start_loads(u):
        for b, (k, j) in enumerate(unit_blocks(u)):
            @pl.when(k != c)
            def _(k=k, j=j):
                for kind in (0, 1, 2):
                    push_arrival(kind, k, j).wait_recv()

            @pl.when(jnp.logical_and(u == 0, k == c))
            def _(b=b, k=k, j=j):
                for cp in block_loads(u, b, k, j, True):
                    cp.start()
                mv[b] = om[...]

            @pl.when(jnp.logical_or(u != 0, k != c))
            def _(b=b, k=k, j=j):
                for cp in block_loads(u, b, k, j, False):
                    cp.start()

    def wait_loads(u):
        for b, (k, j) in enumerate(unit_blocks(u)):
            for cp in block_loads(u, b, k, j, True):
                cp.wait()

            @pl.when(jnp.logical_or(u != 0, k != c))
            def _(b=b, k=k, j=j):
                pltpu.make_async_copy(mb.at[k, j], mv.at[b], ld_m.at[b]).wait()

    def ag_part(kinds, t):
        for kind in kinds:
            for q in range(2):
                j = (me - t + N) % N if q == 0 else (me + t) % N
                reach = H if (q == 1) == (kind == 2) else H - 1

                @pl.when(t <= reach)
                def _(kind=kind, q=q, j=j, reach=reach):
                    ag_copy(q, kind, t - 1, j).wait_recv()

                    @pl.when(t < reach)
                    def _():
                        ag_copy(q, kind, t, j).start()

                    push(kind, j).start()

    def rs_dest(q, s):
        return (me - 1 - s + 2 * N) % N if q == 0 else (me + 1 + s) % N

    def rows_of(h):
        return pl.ds(pl.multiple_of(h * half, half), half)

    def rs_loads(q, e):
        s, h = e // 2, e % 2
        dst = rs_dest(q, s)
        rows = rows_of(h)
        p0 = pltpu.make_async_copy(pown.at[dst, q, rows], pv.at[q, 0], ld_p.at[q, 0])
        p1 = pltpu.make_async_copy(psib.at[dst, q, rows], pv.at[q, 1], ld_p.at[q, 1])
        r = pltpu.make_async_copy(rin.at[q, jnp.maximum(s - 1, 0), rows], ov.at[q, e % 2], ld_r.at[q])
        return p0, p1, r

    def rs_copy(q, e):
        s, h = e // 2, e % 2
        return rcopy(ov.at[q, e % 2], rin.at[q, s, rows_of(h)], rs_send.at[q, e % 2], rs_recv.at[q, s, h], ring[q])

    def rs_start(q, e):
        s, h = e // 2, e % 2
        fresh = s <= H - 2
        if q == 0:
            fresh = jnp.logical_or(fresh, jnp.logical_or(s == H - 1, s == N - 1))

        @pl.when(jnp.logical_and(h == 0, fresh))
        def _():
            dst = rs_dest(q, s)
            rcopy(psib.at[dst], psib.at[dst], st_rem.at[0], part_recv.at[dst], sib).wait_recv()

        p0, p1, r = rs_loads(q, e)
        p0.start()
        p1.start()

        @pl.when(e >= 2)
        def _():
            rs_copy(q, e - 2).wait_send()
            rs_copy(q, e - 2).wait_recv()
            r.start()

    def rs_finish(q, e):
        p0, p1, r = rs_loads(q, e)
        p0.wait()
        p1.wait()
        step = min(64, half)

        @pl.when(e < 2)
        def _():
            def body(i, _):
                rr = pl.ds(pl.multiple_of(i * step, step), step)
                ov[q, e % 2, rr, :] = pv[q, 0, rr, :] + pv[q, 1, rr, :]
                return 0
            lax.fori_loop(0, half // step, body, 0)

        @pl.when(e >= 2)
        def _():
            r.wait()

            def body(i, _):
                rr = pl.ds(pl.multiple_of(i * step, step), step)
                ov[q, e % 2, rr, :] = ov[q, e % 2, rr, :] + (pv[q, 0, rr, :] + pv[q, 1, rr, :])
                return 0
            lax.fori_loop(0, half // step, body, 0)

        @pl.when(e < 2 * N - 2)
        def _():
            rs_copy(q, e).start()

    def stage_loc(b, j):
        return pltpu.make_async_copy(stage.at[b], pown.at[j], st_loc.at[b])

    def stage_rem(b, j):
        return rcopy(stage.at[b], psib.at[j], st_rem.at[b], part_recv.at[j], sib)

    def source_rank(k, j):
        px, py = cycle_chip(k, n, j)
        return py * (2 * n) + 2 * px + k

    def dg_copy(u, b, p):
        return rcopy(dg_out.at[p], dg_in.at[rank], dg_send.at[u, b], dg_recv, peer(p))

    def stage_start(u):
        for b, (k, j) in enumerate(unit_blocks(u)):
            @pl.when(k == c)
            def _(b=b, j=j):
                stage_loc(b, j).start()

            @pl.when(k != c)
            def _(b=b, j=j):
                stage_rem(b, j).start()

            p = source_rank(k, j)

            @pl.when(p != rank)
            def _(b=b, p=p):
                dg_copy(u, b, p).start()

    def stage_wait(u, local):
        for b, (k, j) in enumerate(unit_blocks(u)):
            if local:
                @pl.when(k == c)
                def _(b=b, j=j):
                    stage_loc(b, j).wait()
            else:
                @pl.when(k != c)
                def _(b=b, j=j):
                    stage_rem(b, j).wait_send()

    start_loads(0)
    tri_ref[...] = (lax.broadcasted_iota(jnp.int32, (tok, tok), 0) <= lax.broadcasted_iota(jnp.int32, (tok, tok), 1)).astype(F32).astype(BF)
    for e in range(el):
        acc1[e] = jnp.zeros(acc1.shape[1:], F32)
        acc3[e] = jnp.zeros(acc3.shape[1:], F32)
        acc2[e] = jnp.zeros(acc2.shape[1:], F32)

    def gather_stage(u):
        rows = lax.broadcasted_iota(jnp.int32, (cap, tok), 0).astype(F32)
        lanes = lax.broadcasted_iota(jnp.int32, (tok, cap), 1).astype(F32)
        for b in range(2):
            ids = mv[b, :top, :]
            gts = mv[b, top:, :]
            masks, gws = [], []
            for e in range(el):
                hit = ids == (first + e).astype(F32)
                masks.append(jnp.sum(jnp.where(hit, 1.0, 0.0), axis=0, keepdims=True))
                gws.append(jnp.sum(jnp.where(hit, gts, 0.0), axis=0, keepdims=True))
            mask = jnp.concatenate(masks + [jnp.zeros((8 - el, tok), F32)], axis=0)
            cum = mm(mask.astype(BF), tri_ref[...])
            pos = jnp.where(mask > 0.0, cum - 1.0, -1.0)
            gw = jnp.concatenate(gws + [jnp.zeros((8 - el, tok), F32)], axis=0)
            cols = jnp.concatenate([pos, gw], axis=0).T
            gc_ref[b] = cols
            picks = []
            scales = []
            for e in range(el):
                hit = rows == pos[e:e + 1, :]
                picks.append(jnp.where(hit, 1.0, 0.0).astype(BF))
                scales.append(jnp.sum(jnp.where(hit, gw[e:e + 1, :], 0.0), axis=1, keepdims=True))
                pt_ref[b, :, e * cap:(e + 1) * cap] = jnp.where(lanes == cols[:, e:e + 1], 1.0, 0.0).astype(BF)
            p = jnp.concatenate(picks, axis=0)
            xr = mm(p, xv[b]).astype(BF)
            dr = (jnp.concatenate(scales, axis=0) * mm(p, dv_[u % 2, b])).astype(BF)
            for e in range(el):
                xs_ref[e, b * cap:(b + 1) * cap, :] = xr[e * cap:(e + 1) * cap]
                do_ref[e, b * cap:(b + 1) * cap, :] = dr[e * cap:(e + 1) * cap]

    def expert_a(e):
        xs = xs_ref[e]
        uu = mm(xs, w1_ref[e]).astype(BF).astype(F32)
        vv = mm(xs, w3_ref[e]).astype(BF).astype(F32)
        sg = jax.nn.sigmoid(uu)
        a = (uu * sg * vv).astype(BF)
        o_ref[e] = mm(a, w2_ref[e]).astype(BF)
        do = do_ref[e]
        da = mm(do, w2_ref[e], ((1,), (1,)))
        du_ref[e] = (da * vv * sg * (1.0 + uu * (1.0 - sg))).astype(BF)
        dw_ref[e] = (da * uu * sg).astype(BF)
        acc2[e] += mm(a, do, ((0,), (0,)))

    def expert_b(e):
        xs = xs_ref[e]
        du = du_ref[e]
        dw = dw_ref[e]
        dxs = (mm(du, w1_ref[e], ((1,), (1,))) + mm(dw, w3_ref[e], ((1,), (1,)))).astype(BF)
        for b in range(2):
            dxs_ref[b, e * cap:(e + 1) * cap, :] = dxs[b * cap:(b + 1) * cap, :]
        acc1[e] += mm(xs, du, ((0,), (0,)))
        acc3[e] += mm(xs, dw, ((0,), (0,)))

    def scatter_stage(u):
        for b, (k, j) in enumerate(unit_blocks(u)):
            dyf = dv_[u % 2, b].astype(F32)
            yacc = None
            dgs = []
            for e in range(el):
                so = mm(pt_ref[b, :, e * cap:(e + 1) * cap], o_ref[e, b * cap:(b + 1) * cap, :])
                dgs.append(jnp.sum(dyf * so, axis=1, keepdims=True))
                term = gc_ref[b, :, 8 + e:9 + e] * so
                yacc = term if yacc is None else yacc + term
            stage[b, 0] = yacc
            stage[b, 1] = mm(pt_ref[b], dxs_ref[b])
            dg = jnp.concatenate(dgs + [jnp.zeros((tok, 8 - el), F32)], axis=1).T
            pieces = [dg[e:e + 1, i * lane:(i + 1) * lane] for e in range(el) for i in range(chunks)]
            if len(pieces) < 8:
                pieces.append(jnp.zeros((8 - len(pieces), lane), F32))
            dg = jnp.concatenate(pieces, axis=0)
            p = source_rank(k, j)
            dg_out[p] = dg

            @pl.when(p == rank)
            def _(dg=dg):
                dg_in[rank] = dg

    def unit(u, carry):
        live = u >= rs_unit

        def tick(i):
            tau = ticks * u + i
            ahead = tau - 4
            t = ahead // 4 + 2
            due = jnp.logical_and(ahead >= 0, t <= H)

            @pl.when(jnp.logical_and(due, ahead % 4 == 0))
            def _():
                ag_part((0, 1), t)

            @pl.when(jnp.logical_and(due, ahead % 4 == 2))
            def _():
                ag_part((2,), t)

            turn = tau - ticks * rs_unit

            @pl.when(jnp.logical_and(live, turn % 2 == 0))
            def _():
                rs_start(0, turn // 2)
                rs_start(1, turn // 2)

            @pl.when(jnp.logical_and(live, turn % 2 == 1))
            def _():
                rs_finish(0, turn // 2)
                rs_finish(1, turn // 2)

        wait_loads(u)

        @pl.when(u == 0)
        def _():
            for i, (src, dst) in enumerate(weights):
                pltpu.make_async_copy(src, dst, ld_w.at[i]).wait()

        gather_stage(u)
        expert_a(0)
        tick(0)
        expert_a(1)
        expert_b(0)
        tick(1)

        @pl.when(u >= 1)
        def _():
            stage_wait(u - 1, True)
            stage_wait(u - 1, False)

            @pl.when(u < N - 1)
            def _():
                start_loads(u + 1)

        expert_b(1)
        scatter_stage(u)
        stage_start(u)
        tick(2)

        @pl.when(u == 0)
        def _():
            ag_part((0, 1, 2), 1)
            start_loads(1)

        return carry

    lax.fori_loop(0, N, unit, 0)
    stage_wait(N - 1, True)
    grads = ((acc1, gw1_ref), (acc3, gw3_ref), (acc2, gw2_ref))
    for i, (src, dst) in enumerate(grads):
        pltpu.make_async_copy(src, dst, ld_w.at[i]).start()

    def drain_sends():
        for kind in (0, 1, 2):
            for q in range(2):
                def drain(t, carry, kind=kind, q=q):
                    ag_copy(q, kind, t, me).wait_send()
                    return carry
                lax.fori_loop(0, H if (q == 1) == (kind == 2) else H - 1, drain, 0)

            def drain_push(j, carry, kind=kind):
                push(kind, j).wait_send()
                return carry
            lax.fori_loop(0, N, drain_push, 0)

        def drain_dg(u, carry):
            for b in range(2):
                @pl.when(jnp.logical_or(u > 0, c != b))
                def _(b=b):
                    dg_copy(u, b, rank).wait_send()
            return carry
        lax.fori_loop(0, N, drain_dg, 0)
        stage_wait(N - 1, False)

    def finish_dgates():
        rcopy(dg_in.at[pl.ds(0, nd - 1)], dg_in.at[pl.ds(0, nd - 1)], dg_send.at[0, 0], dg_recv, sib).wait_recv()
        for i in range(chunks):
            lanes = slice(i * lane, (i + 1) * lane)
            ids = om[:top, lanes]

            def pick(p, total, ids=ids, i=i):
                for e in range(el):
                    r = e * chunks + i
                    total = total + jnp.where(ids == (p * el + e).astype(F32), dg_in[p, r:r + 1, :], 0.0)
                return total

            dgates_ref[:, lanes] = lax.fori_loop(0, nd, pick, jnp.zeros((top, lane), F32))

    def tail(e, carry):
        rs_start(0, e)
        rs_start(1, e)
        rs_finish(0, e)
        rs_finish(1, e)

        @pl.when(e == rs_done + 1)
        def _():
            drain_sends()

        @pl.when(e == 2 * N - 6)
        def _():
            finish_dgates()

        @pl.when(e >= 2 * N - 2)
        def _():
            rows = rows_of(e % 2)
            for q, out in ((0, y_ref), (1, dx_ref)):
                xs_ref[q, rows, :] = ov[q, e % 2].astype(BF)
                pltpu.make_async_copy(xs_ref.at[q, rows], out.at[rows], out_sem.at[q, e % 2]).start()
        return carry

    lax.fori_loop(rs_done, 2 * N, tail, 0)

    for i, (src, dst) in enumerate(grads):
        pltpu.make_async_copy(src, dst, ld_w.at[i]).wait()
    for q, out in ((0, y_ref), (1, dx_ref)):
        for h in range(2):
            rows = pl.ds(h * half, half)
            pltpu.make_async_copy(xs_ref.at[q, rows], out.at[rows], out_sem.at[q, h]).wait()


def move_kernel(*refs):
    k = len(refs) // 3
    srcs, dsts, bufs, sems = refs[:k], refs[k:2 * k], refs[2 * k:3 * k], refs[3 * k]
    parts = []
    for i in range(k):
        rows = srcs[i].shape[0]
        step = rows if rows < 1024 else rows // 2
        for a in range(0, rows, step):
            parts.append((i, pl.ds(a, step)))
    for t, (i, r) in enumerate(parts):
        pltpu.make_async_copy(srcs[i].at[r], bufs[i].at[r], sems.at[0, t]).start()
    for t, (i, r) in enumerate(parts):
        pltpu.make_async_copy(srcs[i].at[r], bufs[i].at[r], sems.at[0, t]).wait()
        pltpu.make_async_copy(bufs[i].at[r], dsts[i].at[r], sems.at[1, t]).start()
    for t, (i, r) in enumerate(parts):
        pltpu.make_async_copy(bufs[i].at[r], dsts[i].at[r], sems.at[1, t]).wait()


def move_call(arrays):
    any_spec = pl.BlockSpec(memory_space=pl.ANY)
    flat = [a.reshape(-1, a.shape[-1]) for a in arrays]
    outs = pl.pallas_call(
        move_kernel,
        in_specs=[any_spec] * len(flat),
        out_specs=[any_spec] * len(flat),
        out_shape=[jax.ShapeDtypeStruct(a.shape, a.dtype) for a in flat],
        scratch_shapes=[pltpu.VMEM(a.shape, a.dtype) for a in flat] + [pltpu.SemaphoreType.DMA((2, 2 * len(flat)))],
        cost_estimate=pl.CostEstimate(flops=1, bytes_accessed=sum(2 * a.size * a.dtype.itemsize for a in flat), transcendentals=0),
        compiler_params=pltpu.CompilerParams(vmem_limit_bytes=60 * 1024 * 1024),
    )(*flat)
    return [o.reshape(a.shape) for o, a in zip(outs, arrays)]


def moe_call(n, cap, ids, gates, x, dy, w1, w3, w2):
    N = n * n
    tok, d = x.shape
    el, _, f = w1.shape
    half = tok // 2
    meta = (2 * ids.shape[0], tok)
    any_spec = pl.BlockSpec(memory_space=pl.ANY)
    vm = pl.BlockSpec(memory_space=pltpu.VMEM)
    flops = 13 * 2 * 2 * N * el * cap * d * f
    shape = jax.ShapeDtypeStruct
    dma = pltpu.SemaphoreType.DMA
    outs = pl.pallas_call(
        functools.partial(moe_kernel, n, cap),
        in_specs=[any_spec] * 7,
        out_specs=[any_spec, any_spec, vm] + [any_spec] * 9,
        out_shape=[
            shape((tok, d), BF),
            shape((tok, d), BF),
            shape(ids.shape, F32),
            shape((el, d, f), F32),
            shape((el, d, f), F32),
            shape((el, f, d), F32),
            shape((2, N, tok, d), BF),
            shape((2, N, tok, d), BF),
            shape((2, N) + meta, F32),
            shape((N, 2, tok, d), F32),
            shape((N, 2, tok, d), F32),
            shape((2, N - 1, tok, d), F32),
        ],
        scratch_shapes=[
            pltpu.VMEM((el, d, f), BF),
            pltpu.VMEM((el, d, f), BF),
            pltpu.VMEM((el, f, d), BF),
            pltpu.VMEM((el, d, f), F32),
            pltpu.VMEM((el, d, f), F32),
            pltpu.VMEM((el, f, d), F32),
            pltpu.VMEM((2, tok, d), BF),
            pltpu.VMEM((2,) + meta, F32),
            pltpu.VMEM((2, 2, tok, d), BF),
            pltpu.VMEM((el, 2 * cap, d), BF),
            pltpu.VMEM((el, 2 * cap, d), BF),
            pltpu.VMEM((el, 2 * cap, d), BF),
            pltpu.VMEM((2, el * cap, d), BF),
            pltpu.VMEM((el, 2 * cap, f), BF),
            pltpu.VMEM((el, 2 * cap, f), BF),
            pltpu.VMEM((2, tok, el * cap), BF),
            pltpu.VMEM((2, tok, 16), F32),
            pltpu.VMEM((tok, tok), BF),
            pltpu.VMEM((2, 2, tok, d), F32),
            pltpu.VMEM((2, 2, half, d), F32),
            pltpu.VMEM((2, 2, half, d), F32),
            pltpu.VMEM(meta, F32),
            pltpu.VMEM(ids.shape, jnp.int32),
            pltpu.VMEM((2 * N, 8, tok // max(1, tok // 128)), F32),
            pltpu.VMEM((2 * N, 8, tok // max(1, tok // 128)), F32),
            dma((2, N // 2, 3)),
            dma((2, N // 2, 3)),
            dma((N, 3)),
            dma((N, 3)),
            dma((N,)),
            dma((2, 2)),
            dma((2, N, 2)),
            dma((N, 2)),
            dma(()),
            dma((2,)),
            dma((2,)),
            dma((2,)),
            dma((3,)),
            dma((2,)),
            dma((2,)),
            dma((2, 2)),
            dma((2,)),
            dma((2, 2)),
            dma((2,)),
        ],
        cost_estimate=pl.CostEstimate(flops=flops, bytes_accessed=2 * N * tok * d * 12, transcendentals=0),
        compiler_params=pltpu.CompilerParams(vmem_limit_bytes=63 * 1024 * 1024, collective_id=0, has_side_effects=True),
    )(x, dy, ids, gates, w1, w3, w2)
    return outs[:6]


def solution(mesh):
    nd = mesh.shape['row'] * mesh.shape['col']
    n = mesh.shape['row']
    grp = ('row', 'col')
    tspec = P(('dp', 'row', 'col'), None)
    wspec = P(grp, None, None)
    gspec = P(('dp', 'row', 'col'), None, None)

    def local(x, ridx, gates, w1, w3, w2, dy):
        tok, d = x.shape
        top = ridx.shape[1]
        el = w1.shape[0]
        ne = el * nd
        cap = min(tok, (4 * tok * top + ne - 1) // ne)
        y, dx, dgt, gw1, gw3, gw2 = move_call(moe_call(n, cap, ridx.T, gates.T, x, dy, w1, w3, w2))
        dgates = dgt.T
        return y, dx, dgates, gw1, gw3, gw2

    return jax.shard_map(local, mesh=mesh, in_specs=(tspec, tspec, tspec, wspec, wspec, wspec, tspec), out_specs=(tspec, tspec, tspec, gspec, gspec, gspec), check_vma=False)
```

```python
import functools

import jax
import jax.numpy as jnp
from jax import lax
from jax.experimental import pallas as pl
from jax.experimental.pallas import tpu as pltpu
from jax.sharding import PartitionSpec as P

BF = jnp.bfloat16
F32 = jnp.float32
MESH = pl.DeviceIdType.MESH


def mm(a, b, dims=((1,), (0,))):
    return lax.dot_general(a, b, (dims, ((), ())), preferred_element_type=F32)


def cycle_index(k, n, x, y):
    return n * ((1 - k) * y + k * x) + (x + y) % n


def cycle_chip(k, n, i):
    r = i // n
    o = (i % n - r + n) % n
    return k * r + (1 - k) * o, k * o + (1 - k) * r


def moe_kernel(n, cap, x_ref, dy_ref, ids_ref, gates_ref, w1_hbm, w3_hbm, w2_hbm,
               y_ref, dx_ref, dgates_ref, gw1_ref, gw3_ref, gw2_ref, xb, db, mb, pown, psib, rin,
               w1_ref, w3_ref, w2_ref, acc1, acc3, acc2, xv, mv, dv_, xs_ref, do_ref, o_ref, dxs_ref, du_ref, dw_ref, pt_ref, gc_ref, tri_ref,
               stage, pv, ov, om, oi, dg_out, dg_in,
               ag_send, ag_recv, push_send, push_recv, part_recv, rs_send, rs_recv, dg_send, dg_recv,
               ld_x, ld_m, ld_d, ld_w, st_loc, st_rem, ld_p, ld_r, out_sem, ld_o):
    N = n * n
    H = N // 2
    row = lax.axis_index('row')
    col = lax.axis_index('col')
    cx = col // 2
    c = col % 2
    cy = row
    tok, d = x_ref.shape
    top = ids_ref.shape[0]
    el = w1_ref.shape[0]
    parts = ov.shape[1]
    part = tok // parts
    pos_k = (cycle_index(0, n, cx, cy), cycle_index(1, n, cx, cy))
    me = (1 - c) * pos_k[0] + c * pos_k[1]
    rank = cy * (2 * n) + 2 * cx + c
    first = rank * el
    nd = 2 * N
    chunks = max(1, tok // 128)
    lane = tok // chunks
    ticks = 3
    rs_unit = max(N // 2, 4)
    rs_first = ticks * rs_unit - 1
    rs_done = ticks * N - rs_first

    def device(i):
        px, py = cycle_chip(c, n, i)
        return {'row': py, 'col': 2 * px + c}

    nxt = device((me + 1) % N)
    prv = device((me + N - 1) % N)
    sib = {'row': row, 'col': 2 * cx + 1 - c}
    ring = (nxt, prv)

    def rcopy(src, dst, ss, rs, dev):
        return pltpu.make_async_remote_copy(src_ref=src, dst_ref=dst, send_sem=ss, recv_sem=rs, device_id=dev, device_id_type=MESH)

    def peer(p):
        return {'row': p // (2 * n), 'col': p % (2 * n)}

    barrier = pltpu.get_barrier_semaphore()
    for dr in range(n):
        for dc in range(2 * n):
            if dr or dc:
                dev = {'row': (row + dr) % n, 'col': (col + dc) % (2 * n)}
                pl.semaphore_signal(barrier, inc=1, device_id=dev, device_id_type=MESH)
    small = (pltpu.make_async_copy(ids_ref, oi, ld_o.at[0]), pltpu.make_async_copy(gates_ref, om.at[pl.ds(top, top)], ld_o.at[1]))
    for cp in small:
        cp.start()
    pl.semaphore_wait(barrier, nd - 1)

    own = (x_ref, om, dy_ref)
    bufs = (xb, mb, db)

    def ag_copy(q, kind, t, j, src=None):
        slot = bufs[kind].at[c, j]
        return rcopy(slot if src is None else src, slot, ag_send.at[q, t, kind], ag_recv.at[q, t, kind], ring[q])

    def push(kind, j, src=None):
        slot = bufs[kind].at[c, j]
        return rcopy(slot if src is None else src, slot, push_send.at[j, kind], push_recv.at[j, kind], sib)

    def push_arrival(kind, k, j):
        slot = bufs[kind].at[k, j]
        return rcopy(slot, slot, push_send.at[j, kind], push_recv.at[j, kind], sib)

    for kind in (0, 1, 2):
        if kind == 1:
            for cp in small:
                cp.wait()
            om[:top, :] = oi[...].astype(F32)
        ag_copy(0, kind, 0, me, own[kind]).start()
        ag_copy(1, kind, 0, me, own[kind]).start()
        push(kind, me, own[kind]).start()

    weights = ((w1_hbm, w1_ref), (w3_hbm, w3_ref), (w2_hbm, w2_ref))
    for i, (src, dst) in enumerate(weights):
        pltpu.make_async_copy(src, dst, ld_w.at[i]).start()

    def unit_blocks(u):
        o = (u + 1) // 2
        ka = jnp.where(u == 0, 0, (u + 1) % 2)
        kb = jnp.where(u == N - 1, 1, (u + 1) % 2)
        ia = (1 - ka) * pos_k[0] + ka * pos_k[1]
        ib = (1 - kb) * pos_k[0] + kb * pos_k[1]
        return ((ka, (ia - o + N) % N), (kb, (ib + o) % N))

    def block_loads(u, b, k, j, local):
        slot = u % 2
        cps = [pltpu.make_async_copy(x_ref if local else xb.at[k, j], xv.at[b], ld_x.at[b]),
               pltpu.make_async_copy(dy_ref if local else db.at[k, j], dv_.at[slot, b], ld_d.at[b])]
        if not local:
            cps.append(pltpu.make_async_copy(mb.at[k, j], mv.at[b], ld_m.at[b]))
        return cps

    def start_loads(u):
        for b, (k, j) in enumerate(unit_blocks(u)):
            @pl.when(k != c)
            def _(k=k, j=j):
                for kind in (0, 1, 2):
                    push_arrival(kind, k, j).wait_recv()

            @pl.when(jnp.logical_and(u == 0, k == c))
            def _(b=b, k=k, j=j):
                for cp in block_loads(u, b, k, j, True):
                    cp.start()
                mv[b] = om[...]

            @pl.when(jnp.logical_or(u != 0, k != c))
            def _(b=b, k=k, j=j):
                for cp in block_loads(u, b, k, j, False):
                    cp.start()

    def wait_loads(u):
        for b, (k, j) in enumerate(unit_blocks(u)):
            for cp in block_loads(u, b, k, j, True):
                cp.wait()

            @pl.when(jnp.logical_or(u != 0, k != c))
            def _(b=b, k=k, j=j):
                pltpu.make_async_copy(mb.at[k, j], mv.at[b], ld_m.at[b]).wait()

    def ag_part(kinds, t):
        for kind in kinds:
            for q in range(2):
                j = (me - t + N) % N if q == 0 else (me + t) % N
                reach = H if (q == 1) == (kind == 2) else H - 1

                @pl.when(t <= reach)
                def _(kind=kind, q=q, j=j, reach=reach):
                    ag_copy(q, kind, t - 1, j).wait_recv()

                    @pl.when(t < reach)
                    def _():
                        ag_copy(q, kind, t, j).start()

                    push(kind, j).start()

    def rs_dest(q, s):
        return (me - 1 - s + 2 * N) % N if q == 0 else (me + 1 + s) % N

    def rows_of(h):
        return pl.ds(pl.multiple_of(h * part, part), part)

    def rs_loads(q, e):
        s, h = e // parts, e % parts
        dst = rs_dest(q, s)
        rows = rows_of(h)
        p0 = pltpu.make_async_copy(pown.at[dst, q, rows], pv.at[q, 0], ld_p.at[q, 0])
        p1 = pltpu.make_async_copy(psib.at[dst, q, rows], pv.at[q, 1], ld_p.at[q, 1])
        r = pltpu.make_async_copy(rin.at[q, jnp.maximum(s - 1, 0), rows], ov.at[q, h], ld_r.at[q])
        return p0, p1, r

    def rs_copy(q, e):
        s, h = e // parts, e % parts
        return rcopy(ov.at[q, h], rin.at[q, s, rows_of(h)], rs_send.at[q, h], rs_recv.at[q, s, h], ring[q])

    def rs_start(q, e):
        s, h = e // parts, e % parts
        fresh = s <= H - 2
        if q == 0:
            fresh = jnp.logical_or(fresh, jnp.logical_or(s == H - 1, s == N - 1))

        @pl.when(jnp.logical_and(h == 0, fresh))
        def _():
            dst = rs_dest(q, s)
            rcopy(psib.at[dst], psib.at[dst], st_rem.at[0], part_recv.at[dst], sib).wait_recv()

        p0, p1, r = rs_loads(q, e)
        p0.start()
        p1.start()

        @pl.when(e >= parts)
        def _():
            rs_copy(q, e - parts).wait_send()
            rs_copy(q, e - parts).wait_recv()
            r.start()

    def rs_finish(q, e):
        h = e % parts
        p0, p1, r = rs_loads(q, e)
        p0.wait()
        p1.wait()
        step = min(64, part)

        def add(first):
            def body(i, carry):
                rr = pl.ds(pl.multiple_of(i * step, step), step)
                total = pv[q, 0, rr, :] + pv[q, 1, rr, :]
                ov[q, h, rr, :] = total if first else ov[q, h, rr, :] + total
                return carry
            lax.fori_loop(0, part // step, body, 0)

        @pl.when(e < parts)
        def _():
            add(True)

        @pl.when(e >= parts)
        def _():
            r.wait()
            add(False)

        @pl.when(e < parts * (N - 1))
        def _():
            rs_copy(q, e).start()

    def stage_loc(b, j):
        return pltpu.make_async_copy(stage.at[b], pown.at[j], st_loc.at[b])

    def stage_rem(b, j):
        return rcopy(stage.at[b], psib.at[j], st_rem.at[b], part_recv.at[j], sib)

    def source_rank(k, j):
        px, py = cycle_chip(k, n, j)
        return py * (2 * n) + 2 * px + k

    def dg_copy(u, b, p):
        return rcopy(dg_out.at[p], dg_in.at[rank], dg_send.at[u, b], dg_recv, peer(p))

    def stage_start(u):
        for b, (k, j) in enumerate(unit_blocks(u)):
            @pl.when(k == c)
            def _(b=b, j=j):
                stage_loc(b, j).start()

            @pl.when(k != c)
            def _(b=b, j=j):
                stage_rem(b, j).start()

            p = source_rank(k, j)

            @pl.when(p != rank)
            def _(b=b, p=p):
                dg_copy(u, b, p).start()

    def stage_wait(u, local):
        for b, (k, j) in enumerate(unit_blocks(u)):
            if local:
                @pl.when(k == c)
                def _(b=b, j=j):
                    stage_loc(b, j).wait()
            else:
                @pl.when(k != c)
                def _(b=b, j=j):
                    stage_rem(b, j).wait_send()

    start_loads(0)
    tri_ref[...] = (lax.broadcasted_iota(jnp.int32, (tok, tok), 0) <= lax.broadcasted_iota(jnp.int32, (tok, tok), 1)).astype(F32).astype(BF)
    for e in range(el):
        acc1[e] = jnp.zeros(acc1.shape[1:], F32)
        acc3[e] = jnp.zeros(acc3.shape[1:], F32)
        acc2[e] = jnp.zeros(acc2.shape[1:], F32)

    def gather_stage(u):
        rows = lax.broadcasted_iota(jnp.int32, (cap, tok), 0).astype(F32)
        lanes = lax.broadcasted_iota(jnp.int32, (tok, cap), 1).astype(F32)
        for b in range(2):
            ids = mv[b, :top, :]
            gts = mv[b, top:, :]
            masks, gws = [], []
            for e in range(el):
                hit = ids == (first + e).astype(F32)
                masks.append(jnp.sum(jnp.where(hit, 1.0, 0.0), axis=0, keepdims=True))
                gws.append(jnp.sum(jnp.where(hit, gts, 0.0), axis=0, keepdims=True))
            mask = jnp.concatenate(masks + [jnp.zeros((8 - el, tok), F32)], axis=0)
            cum = mm(mask.astype(BF), tri_ref[...])
            pos = jnp.where(mask > 0.0, cum - 1.0, -1.0)
            gw = jnp.concatenate(gws + [jnp.zeros((8 - el, tok), F32)], axis=0)
            cols = jnp.concatenate([pos, gw], axis=0).T
            gc_ref[b] = cols
            picks = []
            scales = []
            for e in range(el):
                hit = rows == pos[e:e + 1, :]
                picks.append(jnp.where(hit, 1.0, 0.0).astype(BF))
                scales.append(jnp.sum(jnp.where(hit, gw[e:e + 1, :], 0.0), axis=1, keepdims=True))
                pt_ref[b, :, e * cap:(e + 1) * cap] = jnp.where(lanes == cols[:, e:e + 1], 1.0, 0.0).astype(BF)
            p = jnp.concatenate(picks, axis=0)
            xr = mm(p, xv[b]).astype(BF)
            dr = (jnp.concatenate(scales, axis=0) * mm(p, dv_[u % 2, b])).astype(BF)
            for e in range(el):
                xs_ref[e, b * cap:(b + 1) * cap, :] = xr[e * cap:(e + 1) * cap]
                do_ref[e, b * cap:(b + 1) * cap, :] = dr[e * cap:(e + 1) * cap]

    def expert_a(e):
        xs = xs_ref[e]
        uu = mm(xs, w1_ref[e]).astype(BF).astype(F32)
        vv = mm(xs, w3_ref[e]).astype(BF).astype(F32)
        sg = jax.nn.sigmoid(uu)
        a = (uu * sg * vv).astype(BF)
        o_ref[e] = mm(a, w2_ref[e]).astype(BF)
        do = do_ref[e]
        da = mm(do, w2_ref[e], ((1,), (1,)))
        du_ref[e] = (da * vv * sg * (1.0 + uu * (1.0 - sg))).astype(BF)
        dw_ref[e] = (da * uu * sg).astype(BF)
        acc2[e] += mm(a, do, ((0,), (0,)))

    def expert_b(e):
        xs = xs_ref[e]
        du = du_ref[e]
        dw = dw_ref[e]
        dxs = (mm(du, w1_ref[e], ((1,), (1,))) + mm(dw, w3_ref[e], ((1,), (1,)))).astype(BF)
        for b in range(2):
            dxs_ref[b, e * cap:(e + 1) * cap, :] = dxs[b * cap:(b + 1) * cap, :]
        acc1[e] += mm(xs, du, ((0,), (0,)))
        acc3[e] += mm(xs, dw, ((0,), (0,)))

    def scatter_stage(u):
        for b, (k, j) in enumerate(unit_blocks(u)):
            dyf = dv_[u % 2, b].astype(F32)
            yacc = None
            dgs = []
            for e in range(el):
                so = mm(pt_ref[b, :, e * cap:(e + 1) * cap], o_ref[e, b * cap:(b + 1) * cap, :])
                dgs.append(jnp.sum(dyf * so, axis=1, keepdims=True))
                term = gc_ref[b, :, 8 + e:9 + e] * so
                yacc = term if yacc is None else yacc + term
            stage[b, 0] = yacc
            stage[b, 1] = mm(pt_ref[b], dxs_ref[b])
            dg = jnp.concatenate(dgs + [jnp.zeros((tok, 8 - el), F32)], axis=1).T
            pieces = [dg[e:e + 1, i * lane:(i + 1) * lane] for e in range(el) for i in range(chunks)]
            if len(pieces) < 8:
                pieces.append(jnp.zeros((8 - len(pieces), lane), F32))
            dg = jnp.concatenate(pieces, axis=0)
            p = source_rank(k, j)
            dg_out[p] = dg

            @pl.when(p == rank)
            def _(dg=dg):
                dg_in[rank] = dg

    def unit(u, carry):
        def tick(i):
            tau = ticks * u + i
            ahead = tau - 4
            t = ahead // 4 + 2
            due = jnp.logical_and(ahead >= 0, t <= H)

            @pl.when(jnp.logical_and(due, ahead % 4 == 0))
            def _():
                ag_part((0, 1), t)

            @pl.when(jnp.logical_and(due, ahead % 4 == 2))
            def _():
                ag_part((2,), t)

            ev = tau - rs_first

            @pl.when(ev >= 1)
            def _():
                rs_finish(0, ev - 1)
                rs_finish(1, ev - 1)

            @pl.when(ev >= 0)
            def _():
                rs_start(0, ev)
                rs_start(1, ev)

        wait_loads(u)

        @pl.when(u == 0)
        def _():
            for i, (src, dst) in enumerate(weights):
                pltpu.make_async_copy(src, dst, ld_w.at[i]).wait()

        gather_stage(u)
        expert_a(0)
        tick(0)
        expert_a(1)
        expert_b(0)
        tick(1)

        @pl.when(u >= 1)
        def _():
            stage_wait(u - 1, True)
            stage_wait(u - 1, False)

            @pl.when(u < N - 1)
            def _():
                start_loads(u + 1)

        expert_b(1)
        scatter_stage(u)
        stage_start(u)
        tick(2)

        @pl.when(u == 0)
        def _():
            ag_part((0, 1, 2), 1)
            start_loads(1)

        return carry

    lax.fori_loop(0, N, unit, 0)
    stage_wait(N - 1, True)
    grads = ((acc1, gw1_ref), (acc3, gw3_ref), (acc2, gw2_ref))
    for i, (src, dst) in enumerate(grads):
        pltpu.make_async_copy(src, dst, ld_w.at[i]).start()

    def drain_sends():
        for kind in (0, 1, 2):
            for q in range(2):
                def drain(t, carry, kind=kind, q=q):
                    ag_copy(q, kind, t, me).wait_send()
                    return carry
                lax.fori_loop(0, H if (q == 1) == (kind == 2) else H - 1, drain, 0)

            def drain_push(j, carry, kind=kind):
                push(kind, j).wait_send()
                return carry
            lax.fori_loop(0, N, drain_push, 0)

        def drain_dg(u, carry):
            for b in range(2):
                @pl.when(jnp.logical_or(u > 0, c != b))
                def _(b=b):
                    dg_copy(u, b, rank).wait_send()
            return carry
        lax.fori_loop(0, N, drain_dg, 0)
        stage_wait(N - 1, False)

    def finish_dgates():
        rcopy(dg_in.at[pl.ds(0, nd - 1)], dg_in.at[pl.ds(0, nd - 1)], dg_send.at[0, 0], dg_recv, sib).wait_recv()
        for i in range(chunks):
            lanes = slice(i * lane, (i + 1) * lane)
            ids = om[:top, lanes]

            def pick(p, total, ids=ids, i=i):
                for e in range(el):
                    r = e * chunks + i
                    total = total + jnp.where(ids == (p * el + e).astype(F32), dg_in[p, r:r + 1, :], 0.0)
                return total

            dgates_ref[:, lanes] = lax.fori_loop(0, nd, pick, jnp.zeros((top, lane), F32))

    def tail(e, carry):
        rs_start(0, e)
        rs_start(1, e)
        rs_finish(0, e)
        rs_finish(1, e)

        @pl.when(e == rs_done + 2)
        def _():
            drain_sends()

        @pl.when(e == parts * (N - 2))
        def _():
            finish_dgates()

        @pl.when(e >= parts * (N - 1))
        def _():
            rows = rows_of(e % parts)
            for q, out in ((0, y_ref), (1, dx_ref)):
                xs_ref[q, rows, :] = ov[q, e % parts].astype(BF)
                pltpu.make_async_copy(xs_ref.at[q, rows], out.at[rows], out_sem.at[q, e % parts]).start()
        return carry

    rs_finish(0, rs_done - 1)
    rs_finish(1, rs_done - 1)
    lax.fori_loop(rs_done, parts * N, tail, 0)

    for i, (src, dst) in enumerate(grads):
        pltpu.make_async_copy(src, dst, ld_w.at[i]).wait()
    for q, out in ((0, y_ref), (1, dx_ref)):
        for h in range(parts):
            rows = pl.ds(h * part, part)
            pltpu.make_async_copy(xs_ref.at[q, rows], out.at[rows], out_sem.at[q, h]).wait()


def move_kernel(*refs):
    k = len(refs) // 3
    srcs, dsts, bufs, sems = refs[:k], refs[k:2 * k], refs[2 * k:3 * k], refs[3 * k]
    parts = []
    for i in range(k):
        rows = srcs[i].shape[0]
        step = rows if rows < 1024 else rows // 2
        for a in range(0, rows, step):
            parts.append((i, pl.ds(a, step)))
    for t, (i, r) in enumerate(parts):
        pltpu.make_async_copy(srcs[i].at[r], bufs[i].at[r], sems.at[0, t]).start()
    for t, (i, r) in enumerate(parts):
        pltpu.make_async_copy(srcs[i].at[r], bufs[i].at[r], sems.at[0, t]).wait()
        pltpu.make_async_copy(bufs[i].at[r], dsts[i].at[r], sems.at[1, t]).start()
    for t, (i, r) in enumerate(parts):
        pltpu.make_async_copy(bufs[i].at[r], dsts[i].at[r], sems.at[1, t]).wait()


def move_call(arrays):
    any_spec = pl.BlockSpec(memory_space=pl.ANY)
    flat = [a.reshape(-1, a.shape[-1]) for a in arrays]
    outs = pl.pallas_call(
        move_kernel,
        in_specs=[any_spec] * len(flat),
        out_specs=[any_spec] * len(flat),
        out_shape=[jax.ShapeDtypeStruct(a.shape, a.dtype) for a in flat],
        scratch_shapes=[pltpu.VMEM(a.shape, a.dtype) for a in flat] + [pltpu.SemaphoreType.DMA((2, 2 * len(flat)))],
        cost_estimate=pl.CostEstimate(flops=1, bytes_accessed=sum(2 * a.size * a.dtype.itemsize for a in flat), transcendentals=0),
        compiler_params=pltpu.CompilerParams(vmem_limit_bytes=60 * 1024 * 1024),
    )(*flat)
    return [o.reshape(a.shape) for o, a in zip(outs, arrays)]


def moe_call(n, cap, ids, gates, x, dy, w1, w3, w2):
    N = n * n
    tok, d = x.shape
    el, _, f = w1.shape
    parts = 4
    part = tok // parts
    meta = (2 * ids.shape[0], tok)
    any_spec = pl.BlockSpec(memory_space=pl.ANY)
    vm = pl.BlockSpec(memory_space=pltpu.VMEM)
    flops = 13 * 2 * 2 * N * el * cap * d * f
    shape = jax.ShapeDtypeStruct
    dma = pltpu.SemaphoreType.DMA
    outs = pl.pallas_call(
        functools.partial(moe_kernel, n, cap),
        in_specs=[any_spec] * 7,
        out_specs=[any_spec, any_spec, vm] + [any_spec] * 9,
        out_shape=[
            shape((tok, d), BF),
            shape((tok, d), BF),
            shape(ids.shape, F32),
            shape((el, d, f), F32),
            shape((el, d, f), F32),
            shape((el, f, d), F32),
            shape((2, N, tok, d), BF),
            shape((2, N, tok, d), BF),
            shape((2, N) + meta, F32),
            shape((N, 2, tok, d), F32),
            shape((N, 2, tok, d), F32),
            shape((2, N - 1, tok, d), F32),
        ],
        scratch_shapes=[
            pltpu.VMEM((el, d, f), BF),
            pltpu.VMEM((el, d, f), BF),
            pltpu.VMEM((el, f, d), BF),
            pltpu.VMEM((el, d, f), F32),
            pltpu.VMEM((el, d, f), F32),
            pltpu.VMEM((el, f, d), F32),
            pltpu.VMEM((2, tok, d), BF),
            pltpu.VMEM((2,) + meta, F32),
            pltpu.VMEM((2, 2, tok, d), BF),
            pltpu.VMEM((el, 2 * cap, d), BF),
            pltpu.VMEM((el, 2 * cap, d), BF),
            pltpu.VMEM((el, 2 * cap, d), BF),
            pltpu.VMEM((2, el * cap, d), BF),
            pltpu.VMEM((el, 2 * cap, f), BF),
            pltpu.VMEM((el, 2 * cap, f), BF),
            pltpu.VMEM((2, tok, el * cap), BF),
            pltpu.VMEM((2, tok, 16), F32),
            pltpu.VMEM((tok, tok), BF),
            pltpu.VMEM((2, 2, tok, d), F32),
            pltpu.VMEM((2, 2, part, d), F32),
            pltpu.VMEM((2, parts, part, d), F32),
            pltpu.VMEM(meta, F32),
            pltpu.VMEM(ids.shape, jnp.int32),
            pltpu.VMEM((2 * N, 8, tok // max(1, tok // 128)), F32),
            pltpu.VMEM((2 * N, 8, tok // max(1, tok // 128)), F32),
            dma((2, N // 2, 3)),
            dma((2, N // 2, 3)),
            dma((N, 3)),
            dma((N, 3)),
            dma((N,)),
            dma((2, parts)),
            dma((2, N, parts)),
            dma((N, 2)),
            dma(()),
            dma((2,)),
            dma((2,)),
            dma((2,)),
            dma((3,)),
            dma((2,)),
            dma((2,)),
            dma((2, 2)),
            dma((2,)),
            dma((2, parts)),
            dma((2,)),
        ],
        cost_estimate=pl.CostEstimate(flops=flops, bytes_accessed=2 * N * tok * d * 12, transcendentals=0),
        compiler_params=pltpu.CompilerParams(vmem_limit_bytes=63 * 1024 * 1024, collective_id=0, has_side_effects=True),
    )(x, dy, ids, gates, w1, w3, w2)
    return outs[:6]


def solution(mesh):
    nd = mesh.shape['row'] * mesh.shape['col']
    n = mesh.shape['row']
    grp = ('row', 'col')
    tspec = P(('dp', 'row', 'col'), None)
    wspec = P(grp, None, None)
    gspec = P(('dp', 'row', 'col'), None, None)

    def local(x, ridx, gates, w1, w3, w2, dy):
        tok, d = x.shape
        top = ridx.shape[1]
        el = w1.shape[0]
        ne = el * nd
        cap = min(tok, (4 * tok * top + ne - 1) // ne)
        y, dx, dgt, gw1, gw3, gw2 = move_call(moe_call(n, cap, ridx.T, gates.T, x, dy, w1, w3, w2))
        dgates = dgt.T
        return y, dx, dgates, gw1, gw3, gw2

    return jax.shard_map(local, mesh=mesh, in_specs=(tspec, tspec, tspec, wspec, wspec, wspec, tspec), out_specs=(tspec, tspec, tspec, gspec, gspec, gspec), check_vma=False)
```

```python
import functools

import jax
import jax.numpy as jnp
from jax import lax
from jax.experimental import pallas as pl
from jax.experimental.pallas import tpu as pltpu
from jax.sharding import PartitionSpec as P

BF = jnp.bfloat16
F32 = jnp.float32
MESH = pl.DeviceIdType.MESH


def mm(a, b, dims=((1,), (0,))):
    return lax.dot_general(a, b, (dims, ((), ())), preferred_element_type=F32)


def cycle_index(k, n, x, y):
    return n * ((1 - k) * y + k * x) + (x + y) % n


def cycle_chip(k, n, i):
    r = i // n
    o = (i % n - r + n) % n
    return k * r + (1 - k) * o, k * o + (1 - k) * r


def moe_kernel(n, cap, x_ref, dy_ref, ids_ref, gates_ref, w1_hbm, w3_hbm, w2_hbm,
               y_ref, dx_ref, dgates_ref, acc1, acc3, acc2, xb, db, mb, pown, psib, rin,
               w1_ref, w3_ref, w2_ref, xv, mv, dv_, xs_ref, do_ref, o_ref, dxs_ref, du_ref, dw_ref, pt_ref, gc_ref, tri_ref,
               stage, pv, ov, om, oi, dg_out, dg_in,
               ag_send, ag_recv, push_send, push_recv, part_recv, rs_send, rs_recv, dg_send, dg_recv,
               ld_x, ld_m, ld_d, ld_w, st_loc, st_rem, ld_p, ld_r, ld_o):
    N = n * n
    H = N // 2
    row = lax.axis_index('row')
    col = lax.axis_index('col')
    cx = col // 2
    c = col % 2
    cy = row
    tok, d = x_ref.shape
    top = ids_ref.shape[0]
    el = w1_ref.shape[0]
    parts = ov.shape[1]
    part = tok // parts
    pos_k = (cycle_index(0, n, cx, cy), cycle_index(1, n, cx, cy))
    me = (1 - c) * pos_k[0] + c * pos_k[1]
    rank = cy * (2 * n) + 2 * cx + c
    first = rank * el
    nd = 2 * N
    chunks = max(1, tok // 128)
    lane = tok // chunks
    ticks = 3
    rs_unit = max(N // 2, 4)
    rs_first = ticks * rs_unit - 1
    rs_done = ticks * N - rs_first

    def device(i):
        px, py = cycle_chip(c, n, i)
        return {'row': py, 'col': 2 * px + c}

    nxt = device((me + 1) % N)
    prv = device((me + N - 1) % N)
    sib = {'row': row, 'col': 2 * cx + 1 - c}
    ring = (nxt, prv)

    def rcopy(src, dst, ss, rs, dev):
        return pltpu.make_async_remote_copy(src_ref=src, dst_ref=dst, send_sem=ss, recv_sem=rs, device_id=dev, device_id_type=MESH)

    def peer(p):
        return {'row': p // (2 * n), 'col': p % (2 * n)}

    barrier = pltpu.get_barrier_semaphore()
    for dr in range(n):
        for dc in range(2 * n):
            if dr or dc:
                dev = {'row': (row + dr) % n, 'col': (col + dc) % (2 * n)}
                pl.semaphore_signal(barrier, inc=1, device_id=dev, device_id_type=MESH)
    small = (pltpu.make_async_copy(ids_ref, oi, ld_o.at[0]), pltpu.make_async_copy(gates_ref, om.at[pl.ds(top, top)], ld_o.at[1]))
    for cp in small:
        cp.start()
    pl.semaphore_wait(barrier, nd - 1)

    own = (x_ref, om, dy_ref)
    bufs = (xb, mb, db)

    def ag_copy(q, kind, t, j, src=None):
        slot = bufs[kind].at[c, j]
        return rcopy(slot if src is None else src, slot, ag_send.at[q, t, kind], ag_recv.at[q, t, kind], ring[q])

    def push(kind, j, src=None):
        slot = bufs[kind].at[c, j]
        return rcopy(slot if src is None else src, slot, push_send.at[j, kind], push_recv.at[j, kind], sib)

    def push_arrival(kind, k, j):
        slot = bufs[kind].at[k, j]
        return rcopy(slot, slot, push_send.at[j, kind], push_recv.at[j, kind], sib)

    for kind in (0, 1, 2):
        if kind == 1:
            for cp in small:
                cp.wait()
            om[:top, :] = oi[...].astype(F32)
        ag_copy(0, kind, 0, me, own[kind]).start()
        ag_copy(1, kind, 0, me, own[kind]).start()
        push(kind, me, own[kind]).start()

    weights = ((w1_hbm, w1_ref), (w3_hbm, w3_ref), (w2_hbm, w2_ref))
    for i, (src, dst) in enumerate(weights):
        pltpu.make_async_copy(src, dst, ld_w.at[i]).start()

    def unit_blocks(u):
        o = (u + 1) // 2
        ka = jnp.where(u == 0, 0, (u + 1) % 2)
        kb = jnp.where(u == N - 1, 1, (u + 1) % 2)
        ia = (1 - ka) * pos_k[0] + ka * pos_k[1]
        ib = (1 - kb) * pos_k[0] + kb * pos_k[1]
        return ((ka, (ia - o + N) % N), (kb, (ib + o) % N))

    def block_loads(u, b, k, j, local):
        slot = u % 2
        cps = [pltpu.make_async_copy(x_ref if local else xb.at[k, j], xv.at[b], ld_x.at[b]),
               pltpu.make_async_copy(dy_ref if local else db.at[k, j], dv_.at[slot, b], ld_d.at[b])]
        if not local:
            cps.append(pltpu.make_async_copy(mb.at[k, j], mv.at[b], ld_m.at[b]))
        return cps

    def start_loads(u):
        for b, (k, j) in enumerate(unit_blocks(u)):
            @pl.when(k != c)
            def _(k=k, j=j):
                for kind in (0, 1, 2):
                    push_arrival(kind, k, j).wait_recv()

            @pl.when(jnp.logical_and(u == 0, k == c))
            def _(b=b, k=k, j=j):
                for cp in block_loads(u, b, k, j, True):
                    cp.start()
                mv[b] = om[...]

            @pl.when(jnp.logical_or(u != 0, k != c))
            def _(b=b, k=k, j=j):
                for cp in block_loads(u, b, k, j, False):
                    cp.start()

    def wait_loads(u):
        for b, (k, j) in enumerate(unit_blocks(u)):
            for cp in block_loads(u, b, k, j, True):
                cp.wait()

            @pl.when(jnp.logical_or(u != 0, k != c))
            def _(b=b, k=k, j=j):
                pltpu.make_async_copy(mb.at[k, j], mv.at[b], ld_m.at[b]).wait()

    def ag_part(kinds, t):
        for kind in kinds:
            for q in range(2):
                j = (me - t + N) % N if q == 0 else (me + t) % N
                reach = H if (q == 1) == (kind == 2) else H - 1

                @pl.when(t <= reach)
                def _(kind=kind, q=q, j=j, reach=reach):
                    ag_copy(q, kind, t - 1, j).wait_recv()

                    @pl.when(t < reach)
                    def _():
                        ag_copy(q, kind, t, j).start()

                    push(kind, j).start()

    def rs_dest(q, s):
        return (me - 1 - s + 2 * N) % N if q == 0 else (me + 1 + s) % N

    def rows_of(h):
        return pl.ds(pl.multiple_of(h * part, part), part)

    def rs_loads(q, e):
        s, h = e // parts, e % parts
        dst = rs_dest(q, s)
        rows = rows_of(h)
        p0 = pltpu.make_async_copy(pown.at[dst, q, rows], pv.at[q, 0], ld_p.at[q, 0])
        p1 = pltpu.make_async_copy(psib.at[dst, q, rows], pv.at[q, 1], ld_p.at[q, 1])
        r = pltpu.make_async_copy(rin.at[q, jnp.maximum(s - 1, 0), rows], ov.at[q, h], ld_r.at[q])
        return p0, p1, r

    def rs_copy(q, e):
        s, h = e // parts, e % parts
        return rcopy(ov.at[q, h], rin.at[q, s, rows_of(h)], rs_send.at[q, h], rs_recv.at[q, s, h], ring[q])

    def rs_start(q, e):
        s, h = e // parts, e % parts
        fresh = s <= H - 2
        if q == 0:
            fresh = jnp.logical_or(fresh, jnp.logical_or(s == H - 1, s == N - 1))

        @pl.when(jnp.logical_and(h == 0, fresh))
        def _():
            dst = rs_dest(q, s)
            rcopy(psib.at[dst], psib.at[dst], st_rem.at[0], part_recv.at[dst], sib).wait_recv()

        p0, p1, r = rs_loads(q, e)
        p0.start()
        p1.start()

        @pl.when(e >= parts)
        def _():
            rs_copy(q, e - parts).wait_send()
            rs_copy(q, e - parts).wait_recv()
            r.start()

    def rs_finish(q, e):
        h = e % parts
        p0, p1, r = rs_loads(q, e)
        p0.wait()
        p1.wait()
        step = min(64, part)

        def add(first):
            def body(i, carry):
                rr = pl.ds(pl.multiple_of(i * step, step), step)
                total = pv[q, 0, rr, :] + pv[q, 1, rr, :]
                ov[q, h, rr, :] = total if first else ov[q, h, rr, :] + total
                return carry
            lax.fori_loop(0, part // step, body, 0)

        @pl.when(e < parts)
        def _():
            add(True)

        @pl.when(e >= parts)
        def _():
            r.wait()
            add(False)

        @pl.when(e < parts * (N - 1))
        def _():
            rs_copy(q, e).start()

    def stage_loc(b, j):
        return pltpu.make_async_copy(stage.at[b], pown.at[j], st_loc.at[b])

    def stage_rem(b, j):
        return rcopy(stage.at[b], psib.at[j], st_rem.at[b], part_recv.at[j], sib)

    def source_rank(k, j):
        px, py = cycle_chip(k, n, j)
        return py * (2 * n) + 2 * px + k

    def dg_copy(u, b, p):
        return rcopy(dg_out.at[p], dg_in.at[rank], dg_send.at[u, b], dg_recv, peer(p))

    def stage_start(u):
        for b, (k, j) in enumerate(unit_blocks(u)):
            @pl.when(k == c)
            def _(b=b, j=j):
                stage_loc(b, j).start()

            @pl.when(k != c)
            def _(b=b, j=j):
                stage_rem(b, j).start()

            p = source_rank(k, j)

            @pl.when(p != rank)
            def _(b=b, p=p):
                dg_copy(u, b, p).start()

    def stage_wait(u, local):
        for b, (k, j) in enumerate(unit_blocks(u)):
            if local:
                @pl.when(k == c)
                def _(b=b, j=j):
                    stage_loc(b, j).wait()
            else:
                @pl.when(k != c)
                def _(b=b, j=j):
                    stage_rem(b, j).wait_send()

    start_loads(0)
    tri_ref[...] = (lax.broadcasted_iota(jnp.int32, (tok, tok), 0) <= lax.broadcasted_iota(jnp.int32, (tok, tok), 1)).astype(F32).astype(BF)
    for e in range(el):
        acc1[e] = jnp.zeros(acc1.shape[1:], F32)
        acc3[e] = jnp.zeros(acc3.shape[1:], F32)
        acc2[e] = jnp.zeros(acc2.shape[1:], F32)

    def gather_stage(u):
        rows = lax.broadcasted_iota(jnp.int32, (cap, tok), 0).astype(F32)
        lanes = lax.broadcasted_iota(jnp.int32, (tok, cap), 1).astype(F32)
        for b in range(2):
            ids = mv[b, :top, :]
            gts = mv[b, top:, :]
            masks, gws = [], []
            for e in range(el):
                hit = ids == (first + e).astype(F32)
                masks.append(jnp.sum(jnp.where(hit, 1.0, 0.0), axis=0, keepdims=True))
                gws.append(jnp.sum(jnp.where(hit, gts, 0.0), axis=0, keepdims=True))
            mask = jnp.concatenate(masks + [jnp.zeros((8 - el, tok), F32)], axis=0)
            cum = mm(mask.astype(BF), tri_ref[...])
            pos = jnp.where(mask > 0.0, cum - 1.0, -1.0)
            gw = jnp.concatenate(gws + [jnp.zeros((8 - el, tok), F32)], axis=0)
            cols = jnp.concatenate([pos, gw], axis=0).T
            gc_ref[b] = cols
            picks = []
            scales = []
            for e in range(el):
                hit = rows == pos[e:e + 1, :]
                picks.append(jnp.where(hit, 1.0, 0.0).astype(BF))
                scales.append(jnp.sum(jnp.where(hit, gw[e:e + 1, :], 0.0), axis=1, keepdims=True))
                pt_ref[b, :, e * cap:(e + 1) * cap] = jnp.where(lanes == cols[:, e:e + 1], 1.0, 0.0).astype(BF)
            p = jnp.concatenate(picks, axis=0)
            xr = mm(p, xv[b]).astype(BF)
            dr = (jnp.concatenate(scales, axis=0) * mm(p, dv_[u % 2, b])).astype(BF)
            for e in range(el):
                xs_ref[e, b * cap:(b + 1) * cap, :] = xr[e * cap:(e + 1) * cap]
                do_ref[e, b * cap:(b + 1) * cap, :] = dr[e * cap:(e + 1) * cap]

    def expert_a(e):
        xs = xs_ref[e]
        uu = mm(xs, w1_ref[e]).astype(BF).astype(F32)
        vv = mm(xs, w3_ref[e]).astype(BF).astype(F32)
        sg = jax.nn.sigmoid(uu)
        a = (uu * sg * vv).astype(BF)
        o_ref[e] = mm(a, w2_ref[e]).astype(BF)
        do = do_ref[e]
        da = mm(do, w2_ref[e], ((1,), (1,)))
        du_ref[e] = (da * vv * sg * (1.0 + uu * (1.0 - sg))).astype(BF)
        dw_ref[e] = (da * uu * sg).astype(BF)
        acc2[e] += mm(a, do, ((0,), (0,)))

    def expert_b(e):
        xs = xs_ref[e]
        du = du_ref[e]
        dw = dw_ref[e]
        dxs = (mm(du, w1_ref[e], ((1,), (1,))) + mm(dw, w3_ref[e], ((1,), (1,)))).astype(BF)
        for b in range(2):
            dxs_ref[b, e * cap:(e + 1) * cap, :] = dxs[b * cap:(b + 1) * cap, :]
        acc1[e] += mm(xs, du, ((0,), (0,)))
        acc3[e] += mm(xs, dw, ((0,), (0,)))

    def scatter_stage(u):
        for b, (k, j) in enumerate(unit_blocks(u)):
            dyf = dv_[u % 2, b].astype(F32)
            yacc = None
            dgs = []
            for e in range(el):
                so = mm(pt_ref[b, :, e * cap:(e + 1) * cap], o_ref[e, b * cap:(b + 1) * cap, :])
                dgs.append(jnp.sum(dyf * so, axis=1, keepdims=True))
                term = gc_ref[b, :, 8 + e:9 + e] * so
                yacc = term if yacc is None else yacc + term
            stage[b, 0] = yacc
            stage[b, 1] = mm(pt_ref[b], dxs_ref[b])
            dg = jnp.concatenate(dgs + [jnp.zeros((tok, 8 - el), F32)], axis=1).T
            pieces = [dg[e:e + 1, i * lane:(i + 1) * lane] for e in range(el) for i in range(chunks)]
            if len(pieces) < 8:
                pieces.append(jnp.zeros((8 - len(pieces), lane), F32))
            dg = jnp.concatenate(pieces, axis=0)
            p = source_rank(k, j)
            dg_out[p] = dg

            @pl.when(p == rank)
            def _(dg=dg):
                dg_in[rank] = dg

    def unit(u, carry):
        def tick(i):
            tau = ticks * u + i
            ahead = tau - 4
            t = ahead // 4 + 2
            due = jnp.logical_and(ahead >= 0, t <= H)

            @pl.when(jnp.logical_and(due, ahead % 4 == 0))
            def _():
                ag_part((0, 1), t)

            @pl.when(jnp.logical_and(due, ahead % 4 == 2))
            def _():
                ag_part((2,), t)

            ev = tau - rs_first

            @pl.when(ev >= 1)
            def _():
                rs_finish(0, ev - 1)
                rs_finish(1, ev - 1)

            @pl.when(ev >= 0)
            def _():
                rs_start(0, ev)
                rs_start(1, ev)

        wait_loads(u)

        @pl.when(u == 0)
        def _():
            for i, (src, dst) in enumerate(weights):
                pltpu.make_async_copy(src, dst, ld_w.at[i]).wait()

        gather_stage(u)
        expert_a(0)
        tick(0)
        expert_a(1)
        expert_b(0)
        tick(1)

        @pl.when(u >= 1)
        def _():
            stage_wait(u - 1, True)
            stage_wait(u - 1, False)

            @pl.when(u < N - 1)
            def _():
                start_loads(u + 1)

        expert_b(1)
        scatter_stage(u)
        stage_start(u)
        tick(2)

        @pl.when(u == 0)
        def _():
            ag_part((0, 1, 2), 1)
            start_loads(1)

        return carry

    lax.fori_loop(0, N, unit, 0)
    stage_wait(N - 1, True)
    def drain_sends():
        for kind in (0, 1, 2):
            for q in range(2):
                def drain(t, carry, kind=kind, q=q):
                    ag_copy(q, kind, t, me).wait_send()
                    return carry
                lax.fori_loop(0, H if (q == 1) == (kind == 2) else H - 1, drain, 0)

            def drain_push(j, carry, kind=kind):
                push(kind, j).wait_send()
                return carry
            lax.fori_loop(0, N, drain_push, 0)

        def drain_dg(u, carry):
            for b in range(2):
                @pl.when(jnp.logical_or(u > 0, c != b))
                def _(b=b):
                    dg_copy(u, b, rank).wait_send()
            return carry
        lax.fori_loop(0, N, drain_dg, 0)
        stage_wait(N - 1, False)

    def finish_dgates():
        rcopy(dg_in.at[pl.ds(0, nd - 1)], dg_in.at[pl.ds(0, nd - 1)], dg_send.at[0, 0], dg_recv, sib).wait_recv()
        for i in range(chunks):
            lanes = slice(i * lane, (i + 1) * lane)
            ids = om[:top, lanes]

            def pick(p, total, ids=ids, i=i):
                for e in range(el):
                    r = e * chunks + i
                    total = total + jnp.where(ids == (p * el + e).astype(F32), dg_in[p, r:r + 1, :], 0.0)
                return total

            dgates_ref[:, lanes] = lax.fori_loop(0, nd, pick, jnp.zeros((top, lane), F32))

    def tail(e, carry):
        rs_start(0, e)
        rs_start(1, e)
        rs_finish(0, e)
        rs_finish(1, e)

        @pl.when(e == rs_done + 2)
        def _():
            drain_sends()

        @pl.when(e == parts * (N - 2))
        def _():
            finish_dgates()

        @pl.when(e >= parts * (N - 1))
        def _():
            rows = rows_of(e % parts)
            for q, out in ((0, y_ref), (1, dx_ref)):
                out[rows, :] = ov[q, e % parts].astype(BF)
        return carry

    rs_finish(0, rs_done - 1)
    rs_finish(1, rs_done - 1)
    lax.fori_loop(rs_done, parts * N, tail, 0)


def store_kernel(*refs):
    k = len(refs) // 2
    copies = [pltpu.make_async_copy(refs[i], refs[k + i], refs[2 * k].at[i]) for i in range(k)]
    for cp in copies:
        cp.start()
    for cp in copies:
        cp.wait()


def store_call(arrays):
    vm = pl.BlockSpec(memory_space=pltpu.VMEM)
    return pl.pallas_call(
        store_kernel,
        in_specs=[vm] * len(arrays),
        out_specs=[pl.BlockSpec(memory_space=pl.ANY)] * len(arrays),
        out_shape=[pltpu.HBM(a.shape, a.dtype) for a in arrays],
        scratch_shapes=[pltpu.SemaphoreType.DMA((len(arrays),))],
        cost_estimate=pl.CostEstimate(flops=1, bytes_accessed=sum(a.size * a.dtype.itemsize for a in arrays), transcendentals=0),
        compiler_params=pltpu.CompilerParams(vmem_limit_bytes=16 * 1024 * 1024),
    )(*[pltpu.with_memory_space_constraint(a, pltpu.VMEM) for a in arrays])


def moe_call(n, cap, ids, gates, x, dy, w1, w3, w2):
    N = n * n
    tok, d = x.shape
    el, _, f = w1.shape
    parts = 4
    part = tok // parts
    meta = (2 * ids.shape[0], tok)
    any_spec = pl.BlockSpec(memory_space=pl.ANY)
    vm = pl.BlockSpec(memory_space=pltpu.VMEM)
    flops = 13 * 2 * 2 * N * el * cap * d * f
    shape = jax.ShapeDtypeStruct
    dma = pltpu.SemaphoreType.DMA
    outs = pl.pallas_call(
        functools.partial(moe_kernel, n, cap),
        in_specs=[any_spec] * 7,
        out_specs=[vm] * 6 + [any_spec] * 6,
        out_shape=[
            pltpu.VMEM((tok, d), BF),
            pltpu.VMEM((tok, d), BF),
            pltpu.VMEM(ids.shape, F32),
            pltpu.VMEM((el, d, f), F32),
            pltpu.VMEM((el, d, f), F32),
            pltpu.VMEM((el, f, d), F32),
            shape((2, N, tok, d), BF),
            shape((2, N, tok, d), BF),
            shape((2, N) + meta, F32),
            shape((N, 2, tok, d), F32),
            shape((N, 2, tok, d), F32),
            shape((2, N - 1, tok, d), F32),
        ],
        scratch_shapes=[
            pltpu.VMEM((el, d, f), BF),
            pltpu.VMEM((el, d, f), BF),
            pltpu.VMEM((el, f, d), BF),
            pltpu.VMEM((2, tok, d), BF),
            pltpu.VMEM((2,) + meta, F32),
            pltpu.VMEM((2, 2, tok, d), BF),
            pltpu.VMEM((el, 2 * cap, d), BF),
            pltpu.VMEM((el, 2 * cap, d), BF),
            pltpu.VMEM((el, 2 * cap, d), BF),
            pltpu.VMEM((2, el * cap, d), BF),
            pltpu.VMEM((el, 2 * cap, f), BF),
            pltpu.VMEM((el, 2 * cap, f), BF),
            pltpu.VMEM((2, tok, el * cap), BF),
            pltpu.VMEM((2, tok, 16), F32),
            pltpu.VMEM((tok, tok), BF),
            pltpu.VMEM((2, 2, tok, d), F32),
            pltpu.VMEM((2, 2, part, d), F32),
            pltpu.VMEM((2, parts, part, d), F32),
            pltpu.VMEM(meta, F32),
            pltpu.VMEM(ids.shape, jnp.int32),
            pltpu.VMEM((2 * N, 8, tok // max(1, tok // 128)), F32),
            pltpu.VMEM((2 * N, 8, tok // max(1, tok // 128)), F32),
            dma((2, N // 2, 3)),
            dma((2, N // 2, 3)),
            dma((N, 3)),
            dma((N, 3)),
            dma((N,)),
            dma((2, parts)),
            dma((2, N, parts)),
            dma((N, 2)),
            dma(()),
            dma((2,)),
            dma((2,)),
            dma((2,)),
            dma((3,)),
            dma((2,)),
            dma((2,)),
            dma((2, 2)),
            dma((2,)),
            dma((2,)),
        ],
        cost_estimate=pl.CostEstimate(flops=flops, bytes_accessed=2 * N * tok * d * 12, transcendentals=0),
        compiler_params=pltpu.CompilerParams(vmem_limit_bytes=46 * 1024 * 1024, collective_id=0, has_side_effects=True),
    )(x, dy, ids, gates, w1, w3, w2)
    return outs[:6]


def solution(mesh):
    nd = mesh.shape['row'] * mesh.shape['col']
    n = mesh.shape['row']
    grp = ('row', 'col')
    tspec = P(('dp', 'row', 'col'), None)
    wspec = P(grp, None, None)
    gspec = P(('dp', 'row', 'col'), None, None)

    def local(x, ridx, gates, w1, w3, w2, dy):
        tok, d = x.shape
        top = ridx.shape[1]
        el = w1.shape[0]
        ne = el * nd
        cap = min(tok, (4 * tok * top + ne - 1) // ne)
        y, dx, dgt, gw1, gw3, gw2 = store_call(moe_call(n, cap, ridx.T, gates.T, x, dy, w1, w3, w2))
        return y, dx, dgt.T, gw1, gw3, gw2

    return jax.shard_map(local, mesh=mesh, in_specs=(tspec, tspec, tspec, wspec, wspec, wspec, tspec), out_specs=(tspec, tspec, tspec, gspec, gspec, gspec), check_vma=False)
```

```python
import functools

import jax
import jax.numpy as jnp
from jax import lax
from jax.experimental import pallas as pl
from jax.experimental.pallas import tpu as pltpu
from jax.sharding import PartitionSpec as P

BF = jnp.bfloat16
F32 = jnp.float32
MESH = pl.DeviceIdType.MESH


def mm(a, b, dims=((1,), (0,))):
    return lax.dot_general(a, b, (dims, ((), ())), preferred_element_type=F32)


def cycle_index(k, n, x, y):
    return n * ((1 - k) * y + k * x) + (x + y) % n


def cycle_chip(k, n, i):
    r = i // n
    o = (i % n - r + n) % n
    return k * r + (1 - k) * o, k * o + (1 - k) * r


def moe_kernel(n, cap, x_ref, dy_ref, ids_ref, gates_ref, w1_hbm, w3_hbm, w2_hbm,
               y_ref, dx_ref, dgates_ref, acc1, acc3, acc2, xb, db, mb, pown, psib, rin,
               w1_ref, w3_ref, w2_ref, xv, mv, dv_, xs_ref, do_ref, o_ref, dxs_ref, du_ref, dw_ref, pt_ref, gc_ref, tri_ref,
               stage, pv, ov, om, oi, dg_out, dg_in,
               ag_send, ag_recv, push_send, push_recv, part_recv, rs_send, rs_recv, dg_send, dg_recv,
               ld_x, ld_m, ld_d, ld_w, st_loc, st_rem, ld_p, ld_r, ld_o):
    N = n * n
    H = N // 2
    row = lax.axis_index('row')
    col = lax.axis_index('col')
    cx = col // 2
    c = col % 2
    cy = row
    tok, d = x_ref.shape
    top = ids_ref.shape[0]
    el = w1_ref.shape[0]
    parts = ov.shape[1]
    part = tok // parts
    pos_k = (cycle_index(0, n, cx, cy), cycle_index(1, n, cx, cy))
    me = (1 - c) * pos_k[0] + c * pos_k[1]
    rank = cy * (2 * n) + 2 * cx + c
    first = rank * el
    nd = 2 * N
    chunks = max(1, tok // 128)
    lane = tok // chunks
    rs_unit = max(N // 2, 4)
    rs_extra = N - 3
    rs_done = 5 + 3 * (N - 1 - rs_unit) + N - 1 - rs_extra

    def device(i):
        px, py = cycle_chip(c, n, i)
        return {'row': py, 'col': 2 * px + c}

    nxt = device((me + 1) % N)
    prv = device((me + N - 1) % N)
    sib = {'row': row, 'col': 2 * cx + 1 - c}
    ring = (nxt, prv)

    def rcopy(src, dst, ss, rs, dev):
        return pltpu.make_async_remote_copy(src_ref=src, dst_ref=dst, send_sem=ss, recv_sem=rs, device_id=dev, device_id_type=MESH)

    def peer(p):
        return {'row': p // (2 * n), 'col': p % (2 * n)}

    barrier = pltpu.get_barrier_semaphore()
    for dev in (nxt, prv, sib):
        pl.semaphore_signal(barrier, inc=1, device_id=dev, device_id_type=MESH)
    small = (pltpu.make_async_copy(ids_ref, oi, ld_o.at[0]), pltpu.make_async_copy(gates_ref, om.at[pl.ds(top, top)], ld_o.at[1]))
    for cp in small:
        cp.start()
    pl.semaphore_wait(barrier, 3)

    own = (x_ref, om, dy_ref)
    bufs = (xb, mb, db)

    def ag_copy(q, kind, t, j, src=None):
        slot = bufs[kind].at[c, j]
        return rcopy(slot if src is None else src, slot, ag_send.at[q, t, kind], ag_recv.at[q, t, kind], ring[q])

    def push(kind, j, src=None):
        slot = bufs[kind].at[c, j]
        return rcopy(slot if src is None else src, slot, push_send.at[j, kind], push_recv.at[j, kind], sib)

    def push_arrival(kind, k, j):
        slot = bufs[kind].at[k, j]
        return rcopy(slot, slot, push_send.at[j, kind], push_recv.at[j, kind], sib)

    for kind in (0, 1, 2):
        if kind == 1:
            for cp in small:
                cp.wait()
            om[:top, :] = oi[...].astype(F32)
        ag_copy(0, kind, 0, me, own[kind]).start()
        ag_copy(1, kind, 0, me, own[kind]).start()
        push(kind, me, own[kind]).start()

    weights = ((w1_hbm, w1_ref), (w3_hbm, w3_ref), (w2_hbm, w2_ref))
    for i, (src, dst) in enumerate(weights):
        pltpu.make_async_copy(src, dst, ld_w.at[i]).start()

    def unit_blocks(u):
        o = (u + 1) // 2
        ka = jnp.where(u == 0, 0, (u + 1) % 2)
        kb = jnp.where(u == N - 1, 1, (u + 1) % 2)
        ia = (1 - ka) * pos_k[0] + ka * pos_k[1]
        ib = (1 - kb) * pos_k[0] + kb * pos_k[1]
        return ((ka, (ia - o + N) % N), (kb, (ib + o) % N))

    def block_loads(u, b, k, j, local):
        slot = u % 2
        cps = [pltpu.make_async_copy(x_ref if local else xb.at[k, j], xv.at[b], ld_x.at[b]),
               pltpu.make_async_copy(dy_ref if local else db.at[k, j], dv_.at[slot, b], ld_d.at[b])]
        if not local:
            cps.append(pltpu.make_async_copy(mb.at[k, j], mv.at[b], ld_m.at[b]))
        return cps

    def start_loads(u):
        for b, (k, j) in enumerate(unit_blocks(u)):
            @pl.when(k != c)
            def _(k=k, j=j):
                for kind in (0, 1, 2):
                    push_arrival(kind, k, j).wait_recv()

            @pl.when(jnp.logical_and(u == 0, k == c))
            def _(b=b, k=k, j=j):
                for cp in block_loads(u, b, k, j, True):
                    cp.start()
                mv[b] = om[...]

            @pl.when(jnp.logical_or(u != 0, k != c))
            def _(b=b, k=k, j=j):
                for cp in block_loads(u, b, k, j, False):
                    cp.start()

    def wait_loads(u):
        for b, (k, j) in enumerate(unit_blocks(u)):
            for cp in block_loads(u, b, k, j, True):
                cp.wait()

            @pl.when(jnp.logical_or(u != 0, k != c))
            def _(b=b, k=k, j=j):
                pltpu.make_async_copy(mb.at[k, j], mv.at[b], ld_m.at[b]).wait()

    def ag_part(kinds, t):
        for kind in kinds:
            for q in range(2):
                j = (me - t + N) % N if q == 0 else (me + t) % N
                reach = H if (q == 1) == (kind == 2) else H - 1

                @pl.when(t <= reach)
                def _(kind=kind, q=q, j=j, reach=reach):
                    ag_copy(q, kind, t - 1, j).wait_recv()

                    @pl.when(t < reach)
                    def _():
                        ag_copy(q, kind, t, j).start()

                    push(kind, j).start()

    def rs_dest(q, s):
        return (me - 1 - s + 2 * N) % N if q == 0 else (me + 1 + s) % N

    def rows_of(h):
        return pl.ds(pl.multiple_of(h * part, part), part)

    def rs_loads(q, e):
        s, h = e // parts, e % parts
        dst = rs_dest(q, s)
        rows = rows_of(h)
        p0 = pltpu.make_async_copy(pown.at[dst, q, rows], pv.at[q, 0], ld_p.at[q, 0])
        p1 = pltpu.make_async_copy(psib.at[dst, q, rows], pv.at[q, 1], ld_p.at[q, 1])
        r = pltpu.make_async_copy(rin.at[q, jnp.maximum(s - 1, 0), rows], ov.at[q, h], ld_r.at[q])
        return p0, p1, r

    def rs_copy(q, e):
        s, h = e // parts, e % parts
        return rcopy(ov.at[q, h], rin.at[q, s, rows_of(h)], rs_send.at[q, h], rs_recv.at[q, s, h], ring[q])

    def rs_start(q, e):
        s, h = e // parts, e % parts
        fresh = s <= H - 2
        if q == 0:
            fresh = jnp.logical_or(fresh, jnp.logical_or(s == H - 1, s == N - 1))

        @pl.when(jnp.logical_and(h == 0, fresh))
        def _():
            dst = rs_dest(q, s)
            rcopy(psib.at[dst], psib.at[dst], st_rem.at[0], part_recv.at[dst], sib).wait_recv()

        p0, p1, r = rs_loads(q, e)
        p0.start()
        p1.start()

        @pl.when(e >= parts)
        def _():
            rs_copy(q, e - parts).wait_send()
            rs_copy(q, e - parts).wait_recv()
            r.start()

    def rs_finish(q, e):
        h = e % parts
        p0, p1, r = rs_loads(q, e)
        p0.wait()
        p1.wait()
        step = min(64, part)

        def add(first):
            def body(i, carry):
                rr = pl.ds(pl.multiple_of(i * step, step), step)
                total = pv[q, 0, rr, :] + pv[q, 1, rr, :]
                ov[q, h, rr, :] = total if first else ov[q, h, rr, :] + total
                return carry
            lax.fori_loop(0, part // step, body, 0)

        @pl.when(e < parts)
        def _():
            add(True)

        @pl.when(e >= parts)
        def _():
            r.wait()
            add(False)

        @pl.when(e < parts * (N - 1))
        def _():
            rs_copy(q, e).start()

    def stage_loc(b, j):
        return pltpu.make_async_copy(stage.at[b], pown.at[j], st_loc.at[b])

    def stage_rem(b, j):
        return rcopy(stage.at[b], psib.at[j], st_rem.at[b], part_recv.at[j], sib)

    def source_rank(k, j):
        px, py = cycle_chip(k, n, j)
        return py * (2 * n) + 2 * px + k

    def dg_copy(u, b, p):
        return rcopy(dg_out.at[p], dg_in.at[rank], dg_send.at[u, b], dg_recv, peer(p))

    def stage_start(u):
        for b, (k, j) in enumerate(unit_blocks(u)):
            @pl.when(k == c)
            def _(b=b, j=j):
                stage_loc(b, j).start()

            @pl.when(k != c)
            def _(b=b, j=j):
                stage_rem(b, j).start()

            p = source_rank(k, j)

            @pl.when(p != rank)
            def _(b=b, p=p):
                dg_copy(u, b, p).start()

    def stage_wait(u, local):
        for b, (k, j) in enumerate(unit_blocks(u)):
            if local:
                @pl.when(k == c)
                def _(b=b, j=j):
                    stage_loc(b, j).wait()
            else:
                @pl.when(k != c)
                def _(b=b, j=j):
                    stage_rem(b, j).wait_send()

    start_loads(0)
    tri_ref[...] = (lax.broadcasted_iota(jnp.int32, (tok, tok), 0) <= lax.broadcasted_iota(jnp.int32, (tok, tok), 1)).astype(F32).astype(BF)
    for e in range(el):
        acc1[e] = jnp.zeros(acc1.shape[1:], F32)
        acc3[e] = jnp.zeros(acc3.shape[1:], F32)
        acc2[e] = jnp.zeros(acc2.shape[1:], F32)

    def gather_stage(u):
        rows = lax.broadcasted_iota(jnp.int32, (cap, tok), 0).astype(F32)
        lanes = lax.broadcasted_iota(jnp.int32, (tok, cap), 1).astype(F32)
        for b in range(2):
            ids = mv[b, :top, :]
            gts = mv[b, top:, :]
            masks, gws = [], []
            for e in range(el):
                hit = ids == (first + e).astype(F32)
                masks.append(jnp.sum(jnp.where(hit, 1.0, 0.0), axis=0, keepdims=True))
                gws.append(jnp.sum(jnp.where(hit, gts, 0.0), axis=0, keepdims=True))
            mask = jnp.concatenate(masks + [jnp.zeros((8 - el, tok), F32)], axis=0)
            cum = mm(mask.astype(BF), tri_ref[...])
            pos = jnp.where(mask > 0.0, cum - 1.0, -1.0)
            gw = jnp.concatenate(gws + [jnp.zeros((8 - el, tok), F32)], axis=0)
            cols = jnp.concatenate([pos, gw], axis=0).T
            gc_ref[b] = cols
            picks = []
            scales = []
            for e in range(el):
                hit = rows == pos[e:e + 1, :]
                picks.append(jnp.where(hit, 1.0, 0.0).astype(BF))
                scales.append(jnp.sum(jnp.where(hit, gw[e:e + 1, :], 0.0), axis=1, keepdims=True))
                pt_ref[b, :, e * cap:(e + 1) * cap] = jnp.where(lanes == cols[:, e:e + 1], 1.0, 0.0).astype(BF)
            p = jnp.concatenate(picks, axis=0)
            xr = mm(p, xv[b]).astype(BF)
            dr = (jnp.concatenate(scales, axis=0) * mm(p, dv_[u % 2, b])).astype(BF)
            for e in range(el):
                xs_ref[e, b * cap:(b + 1) * cap, :] = xr[e * cap:(e + 1) * cap]
                do_ref[e, b * cap:(b + 1) * cap, :] = dr[e * cap:(e + 1) * cap]

    def expert_a(e):
        xs = xs_ref[e]
        uu = mm(xs, w1_ref[e]).astype(BF).astype(F32)
        vv = mm(xs, w3_ref[e]).astype(BF).astype(F32)
        sg = jax.nn.sigmoid(uu)
        a = (uu * sg * vv).astype(BF)
        o_ref[e] = mm(a, w2_ref[e]).astype(BF)
        do = do_ref[e]
        da = mm(do, w2_ref[e], ((1,), (1,)))
        du_ref[e] = (da * vv * sg * (1.0 + uu * (1.0 - sg))).astype(BF)
        dw_ref[e] = (da * uu * sg).astype(BF)
        acc2[e] += mm(a, do, ((0,), (0,)))

    def expert_b(e):
        xs = xs_ref[e]
        du = du_ref[e]
        dw = dw_ref[e]
        dxs = (mm(du, w1_ref[e], ((1,), (1,))) + mm(dw, w3_ref[e], ((1,), (1,)))).astype(BF)
        for b in range(2):
            dxs_ref[b, e * cap:(e + 1) * cap, :] = dxs[b * cap:(b + 1) * cap, :]
        acc1[e] += mm(xs, du, ((0,), (0,)))
        acc3[e] += mm(xs, dw, ((0,), (0,)))

    def scatter_stage(u):
        for b, (k, j) in enumerate(unit_blocks(u)):
            dyf = dv_[u % 2, b].astype(F32)
            yacc = None
            dgs = []
            for e in range(el):
                so = mm(pt_ref[b, :, e * cap:(e + 1) * cap], o_ref[e, b * cap:(b + 1) * cap, :])
                dgs.append(jnp.sum(dyf * so, axis=1, keepdims=True))
                term = gc_ref[b, :, 8 + e:9 + e] * so
                yacc = term if yacc is None else yacc + term
            stage[b, 0] = yacc
            stage[b, 1] = mm(pt_ref[b], dxs_ref[b])
            dg = jnp.concatenate(dgs + [jnp.zeros((tok, 8 - el), F32)], axis=1).T
            pieces = [dg[e:e + 1, i * lane:(i + 1) * lane] for e in range(el) for i in range(chunks)]
            if len(pieces) < 8:
                pieces.append(jnp.zeros((8 - len(pieces), lane), F32))
            dg = jnp.concatenate(pieces, axis=0)
            p = source_rank(k, j)
            dg_out[p] = dg

            @pl.when(p == rank)
            def _(dg=dg):
                dg_in[rank] = dg

    def unit(u, carry):
        late = u >= rs_extra
        ahead_of = jnp.where(late, u - rs_extra, 0)

        def tick(i):
            if i != 2:
                ahead = 3 * u + min(i, 2) - 4
                t = ahead // 4 + 2
                due = jnp.logical_and(ahead >= 0, t <= H)

                @pl.when(jnp.logical_and(due, ahead % 4 == 0))
                def _():
                    ag_part((0, 1), t)

                @pl.when(jnp.logical_and(due, ahead % 4 == 2))
                def _():
                    ag_part((2,), t)

            ev = 1 + 3 * (u - rs_unit) + ahead_of + min(i, 2)
            if i == 3:
                ev = ev + jnp.where(late, 1, 0)
            live = late if i == 2 else u >= 0

            @pl.when(jnp.logical_and(live, ev >= 1))
            def _():
                rs_finish(0, ev - 1)
                rs_finish(1, ev - 1)

            @pl.when(jnp.logical_and(live, ev >= 0))
            def _():
                rs_start(0, ev)
                rs_start(1, ev)

        wait_loads(u)

        @pl.when(u == 0)
        def _():
            for i, (src, dst) in enumerate(weights):
                pltpu.make_async_copy(src, dst, ld_w.at[i]).wait()

        gather_stage(u)
        expert_a(0)

        @pl.when(u >= 1)
        def _():
            stage_wait(u - 1, True)

        tick(0)
        expert_a(1)
        expert_b(0)
        tick(1)

        @pl.when(jnp.logical_and(u >= 1, u < N - 1))
        def _():
            start_loads(u + 1)

        expert_b(1)
        tick(2)

        @pl.when(u >= 1)
        def _():
            stage_wait(u - 1, False)

        scatter_stage(u)
        stage_start(u)
        tick(3)

        @pl.when(u == 0)
        def _():
            ag_part((0, 1, 2), 1)
            start_loads(1)

        return carry

    lax.fori_loop(0, N, unit, 0)
    stage_wait(N - 1, True)
    def drain_sends():
        for kind in (0, 1, 2):
            for q in range(2):
                def drain(t, carry, kind=kind, q=q):
                    ag_copy(q, kind, t, me).wait_send()
                    return carry
                lax.fori_loop(0, H if (q == 1) == (kind == 2) else H - 1, drain, 0)

            def drain_push(j, carry, kind=kind):
                push(kind, j).wait_send()
                return carry
            lax.fori_loop(0, N, drain_push, 0)

        def drain_dg(u, carry):
            for b in range(2):
                @pl.when(jnp.logical_or(u > 0, c != b))
                def _(b=b):
                    dg_copy(u, b, rank).wait_send()
            return carry
        lax.fori_loop(0, N, drain_dg, 0)
        stage_wait(N - 1, False)

    def finish_dgates():
        rcopy(dg_in.at[pl.ds(0, nd - 1)], dg_in.at[pl.ds(0, nd - 1)], dg_send.at[0, 0], dg_recv, sib).wait_recv()
        for i in range(chunks):
            lanes = slice(i * lane, (i + 1) * lane)
            ids = om[:top, lanes]

            def pick(p, total, ids=ids, i=i):
                for e in range(el):
                    r = e * chunks + i
                    total = total + jnp.where(ids == (p * el + e).astype(F32), dg_in[p, r:r + 1, :], 0.0)
                return total

            dgates_ref[:, lanes] = lax.fori_loop(0, nd, pick, jnp.zeros((top, lane), F32))

    def tail(e, carry):
        rs_start(0, e)
        rs_start(1, e)
        rs_finish(0, e)
        rs_finish(1, e)

        @pl.when(e == rs_done + 2)
        def _():
            drain_sends()

        @pl.when(e == parts * (N - 2))
        def _():
            finish_dgates()

        @pl.when(e >= parts * (N - 1))
        def _():
            rows = rows_of(e % parts)
            for q, out in ((0, y_ref), (1, dx_ref)):
                out[rows, :] = ov[q, e % parts].astype(BF)
        return carry

    rs_finish(0, rs_done - 1)
    rs_finish(1, rs_done - 1)
    lax.fori_loop(rs_done, parts * N, tail, 0)


def store_kernel(*refs):
    k = len(refs) // 2
    copies = [pltpu.make_async_copy(refs[i], refs[k + i], refs[2 * k].at[i]) for i in range(k)]
    for cp in copies:
        cp.start()
    for cp in copies:
        cp.wait()


def store_call(arrays):
    vm = pl.BlockSpec(memory_space=pltpu.VMEM)
    return pl.pallas_call(
        store_kernel,
        in_specs=[vm] * len(arrays),
        out_specs=[pl.BlockSpec(memory_space=pl.ANY)] * len(arrays),
        out_shape=[pltpu.HBM(a.shape, a.dtype) for a in arrays],
        scratch_shapes=[pltpu.SemaphoreType.DMA((len(arrays),))],
        cost_estimate=pl.CostEstimate(flops=1, bytes_accessed=sum(a.size * a.dtype.itemsize for a in arrays), transcendentals=0),
        compiler_params=pltpu.CompilerParams(vmem_limit_bytes=16 * 1024 * 1024),
    )(*[pltpu.with_memory_space_constraint(a, pltpu.VMEM) for a in arrays])


def moe_call(n, cap, ids, gates, x, dy, w1, w3, w2):
    N = n * n
    tok, d = x.shape
    el, _, f = w1.shape
    parts = 4
    part = tok // parts
    meta = (2 * ids.shape[0], tok)
    any_spec = pl.BlockSpec(memory_space=pl.ANY)
    vm = pl.BlockSpec(memory_space=pltpu.VMEM)
    flops = 13 * 2 * 2 * N * el * cap * d * f
    shape = jax.ShapeDtypeStruct
    dma = pltpu.SemaphoreType.DMA
    outs = pl.pallas_call(
        functools.partial(moe_kernel, n, cap),
        in_specs=[any_spec] * 7,
        out_specs=[vm] * 6 + [any_spec] * 6,
        out_shape=[
            pltpu.VMEM((tok, d), BF),
            pltpu.VMEM((tok, d), BF),
            pltpu.VMEM(ids.shape, F32),
            pltpu.VMEM((el, d, f), F32),
            pltpu.VMEM((el, d, f), F32),
            pltpu.VMEM((el, f, d), F32),
            shape((2, N, tok, d), BF),
            shape((2, N, tok, d), BF),
            shape((2, N) + meta, F32),
            shape((N, 2, tok, d), F32),
            shape((N, 2, tok, d), F32),
            shape((2, N - 1, tok, d), F32),
        ],
        scratch_shapes=[
            pltpu.VMEM((el, d, f), BF),
            pltpu.VMEM((el, d, f), BF),
            pltpu.VMEM((el, f, d), BF),
            pltpu.VMEM((2, tok, d), BF),
            pltpu.VMEM((2,) + meta, F32),
            pltpu.VMEM((2, 2, tok, d), BF),
            pltpu.VMEM((el, 2 * cap, d), BF),
            pltpu.VMEM((el, 2 * cap, d), BF),
            pltpu.VMEM((el, 2 * cap, d), BF),
            pltpu.VMEM((2, el * cap, d), BF),
            pltpu.VMEM((el, 2 * cap, f), BF),
            pltpu.VMEM((el, 2 * cap, f), BF),
            pltpu.VMEM((2, tok, el * cap), BF),
            pltpu.VMEM((2, tok, 16), F32),
            pltpu.VMEM((tok, tok), BF),
            pltpu.VMEM((2, 2, tok, d), F32),
            pltpu.VMEM((2, 2, part, d), F32),
            pltpu.VMEM((2, parts, part, d), F32),
            pltpu.VMEM(meta, F32),
            pltpu.VMEM(ids.shape, jnp.int32),
            pltpu.VMEM((2 * N, 8, tok // max(1, tok // 128)), F32),
            pltpu.VMEM((2 * N, 8, tok // max(1, tok // 128)), F32),
            dma((2, N // 2, 3)),
            dma((2, N // 2, 3)),
            dma((N, 3)),
            dma((N, 3)),
            dma((N,)),
            dma((2, parts)),
            dma((2, N, parts)),
            dma((N, 2)),
            dma(()),
            dma((2,)),
            dma((2,)),
            dma((2,)),
            dma((3,)),
            dma((2,)),
            dma((2,)),
            dma((2, 2)),
            dma((2,)),
            dma((2,)),
        ],
        cost_estimate=pl.CostEstimate(flops=flops, bytes_accessed=2 * N * tok * d * 12, transcendentals=0),
        compiler_params=pltpu.CompilerParams(vmem_limit_bytes=46 * 1024 * 1024, collective_id=0, has_side_effects=True),
    )(x, dy, ids, gates, w1, w3, w2)
    return outs[:6]


def solution(mesh):
    nd = mesh.shape['row'] * mesh.shape['col']
    n = mesh.shape['row']
    grp = ('row', 'col')
    tspec = P(('dp', 'row', 'col'), None)
    wspec = P(grp, None, None)
    gspec = P(('dp', 'row', 'col'), None, None)

    def local(x, ridx, gates, w1, w3, w2, dy):
        tok, d = x.shape
        top = ridx.shape[1]
        el = w1.shape[0]
        ne = el * nd
        cap = min(tok, (4 * tok * top + ne - 1) // ne)
        y, dx, dgt, gw1, gw3, gw2 = store_call(moe_call(n, cap, ridx.T, gates.T, x, dy, w1, w3, w2))
        return y, dx, dgt.T, gw1, gw3, gw2

    return jax.shard_map(local, mesh=mesh, in_specs=(tspec, tspec, tspec, wspec, wspec, wspec, tspec), out_specs=(tspec, tspec, tspec, gspec, gspec, gspec), check_vma=False)
```

```python
import functools

import jax
import jax.numpy as jnp
from jax import lax
from jax.experimental import pallas as pl
from jax.experimental.pallas import tpu as pltpu
from jax.sharding import PartitionSpec as P

BF = jnp.bfloat16
F32 = jnp.float32
MESH = pl.DeviceIdType.MESH


def mm(a, b, dims=((1,), (0,))):
    return lax.dot_general(a, b, (dims, ((), ())), preferred_element_type=F32)


def cycle_index(k, n, x, y):
    return n * ((1 - k) * y + k * x) + (x + y) % n


def cycle_chip(k, n, i):
    r = i // n
    o = (i % n - r + n) % n
    return k * r + (1 - k) * o, k * o + (1 - k) * r


def moe_kernel(n, cap, x_ref, dy_ref, ids_ref, gates_ref, w1_hbm, w3_hbm, w2_hbm,
               y_ref, dx_ref, dgates_ref, acc1, acc3, acc2, xb, db, mb, pown, psib, rin,
               w1_ref, w3_ref, w2_ref, xv, mv, dv_, xs_ref, do_ref, o_ref, dxs_ref, du_ref, dw_ref, pk_ref, pt_ref, gc_ref, tri_ref,
               stage, pv, ov, om, oi, dg_out, dg_in,
               ag_send, ag_recv, push_send, push_recv, part_recv, rs_send, rs_recv, dg_send, dg_recv,
               ld_x, ld_m, ld_d, ld_w, st_loc, st_rem, ld_p, ld_r, ld_o):
    N = n * n
    H = N // 2
    row = lax.axis_index('row')
    col = lax.axis_index('col')
    cx = col // 2
    c = col % 2
    cy = row
    tok, d = x_ref.shape
    top = ids_ref.shape[0]
    el = w1_ref.shape[0]
    parts = ov.shape[1]
    part = tok // parts
    pos_k = (cycle_index(0, n, cx, cy), cycle_index(1, n, cx, cy))
    me = (1 - c) * pos_k[0] + c * pos_k[1]
    rank = cy * (2 * n) + 2 * cx + c
    first = rank * el
    nd = 2 * N
    chunks = max(1, tok // 128)
    lane = tok // chunks
    rs_unit = max(N // 2, 4)
    rs_extra = N - 3
    rs_done = 5 + 3 * (N - 1 - rs_unit) + N - 1 - rs_extra

    def device(i):
        px, py = cycle_chip(c, n, i)
        return {'row': py, 'col': 2 * px + c}

    nxt = device((me + 1) % N)
    prv = device((me + N - 1) % N)
    sib = {'row': row, 'col': 2 * cx + 1 - c}
    ring = (nxt, prv)

    def rcopy(src, dst, ss, rs, dev):
        return pltpu.make_async_remote_copy(src_ref=src, dst_ref=dst, send_sem=ss, recv_sem=rs, device_id=dev, device_id_type=MESH)

    def peer(p):
        return {'row': p // (2 * n), 'col': p % (2 * n)}

    barrier = pltpu.get_barrier_semaphore()
    for dev in (nxt, prv, sib):
        pl.semaphore_signal(barrier, inc=1, device_id=dev, device_id_type=MESH)
    small = (pltpu.make_async_copy(ids_ref, oi, ld_o.at[0]), pltpu.make_async_copy(gates_ref, om.at[pl.ds(top, top)], ld_o.at[1]))
    for cp in small:
        cp.start()
    pl.semaphore_wait(barrier, 3)

    own = (x_ref, om, dy_ref)
    bufs = (xb, mb, db)

    def ag_copy(q, kind, t, j, src=None):
        slot = bufs[kind].at[c, j]
        return rcopy(slot if src is None else src, slot, ag_send.at[q, t, kind], ag_recv.at[q, t, kind], ring[q])

    def push(kind, j, src=None):
        slot = bufs[kind].at[c, j]
        return rcopy(slot if src is None else src, slot, push_send.at[j, kind], push_recv.at[j, kind], sib)

    def push_arrival(kind, k, j):
        slot = bufs[kind].at[k, j]
        return rcopy(slot, slot, push_send.at[j, kind], push_recv.at[j, kind], sib)

    for kind in (0, 1, 2):
        if kind == 1:
            for cp in small:
                cp.wait()
            om[:top, :] = oi[...].astype(F32)
        ag_copy(0, kind, 0, me, own[kind]).start()
        ag_copy(1, kind, 0, me, own[kind]).start()
        push(kind, me, own[kind]).start()

    weights = ((w1_hbm, w1_ref), (w3_hbm, w3_ref), (w2_hbm, w2_ref))
    for i, (src, dst) in enumerate(weights):
        pltpu.make_async_copy(src, dst, ld_w.at[i]).start()

    def unit_blocks(u):
        o = (u + 1) // 2
        ka = jnp.where(u == 0, 0, (u + 1) % 2)
        kb = jnp.where(u == N - 1, 1, (u + 1) % 2)
        ia = (1 - ka) * pos_k[0] + ka * pos_k[1]
        ib = (1 - kb) * pos_k[0] + kb * pos_k[1]
        return ((ka, (ia - o + N) % N), (kb, (ib + o) % N))

    def block_loads(u, b, k, j, local):
        slot = u % 2
        cps = [pltpu.make_async_copy(x_ref if local else xb.at[k, j], xv.at[b], ld_x.at[b]),
               pltpu.make_async_copy(dy_ref if local else db.at[k, j], dv_.at[slot, b], ld_d.at[b])]
        if not local:
            cps.append(pltpu.make_async_copy(mb.at[k, j], mv.at[b], ld_m.at[b]))
        return cps

    def start_loads(u):
        for b, (k, j) in enumerate(unit_blocks(u)):
            @pl.when(k != c)
            def _(k=k, j=j):
                for kind in (0, 1, 2):
                    push_arrival(kind, k, j).wait_recv()

            @pl.when(jnp.logical_and(u == 0, k == c))
            def _(b=b, k=k, j=j):
                for cp in block_loads(u, b, k, j, True):
                    cp.start()
                mv[b] = om[...]

            @pl.when(jnp.logical_or(u != 0, k != c))
            def _(b=b, k=k, j=j):
                for cp in block_loads(u, b, k, j, False):
                    cp.start()

    def wait_loads(u):
        for b, (k, j) in enumerate(unit_blocks(u)):
            for cp in block_loads(u, b, k, j, True):
                cp.wait()

            @pl.when(jnp.logical_or(u != 0, k != c))
            def _(b=b, k=k, j=j):
                pltpu.make_async_copy(mb.at[k, j], mv.at[b], ld_m.at[b]).wait()

    def ag_part(kinds, t):
        for kind in kinds:
            for q in range(2):
                j = (me - t + N) % N if q == 0 else (me + t) % N
                reach = H if (q == 1) == (kind == 2) else H - 1

                @pl.when(t <= reach)
                def _(kind=kind, q=q, j=j, reach=reach):
                    ag_copy(q, kind, t - 1, j).wait_recv()

                    @pl.when(t < reach)
                    def _():
                        ag_copy(q, kind, t, j).start()

                    push(kind, j).start()

    def rs_dest(q, s):
        return (me - 1 - s + 2 * N) % N if q == 0 else (me + 1 + s) % N

    def rows_of(h):
        return pl.ds(pl.multiple_of(h * part, part), part)

    def rs_loads(q, e):
        s, h = e // parts, e % parts
        dst = rs_dest(q, s)
        rows = rows_of(h)
        p0 = pltpu.make_async_copy(pown.at[dst, q, rows], pv.at[q, 0], ld_p.at[q, 0])
        p1 = pltpu.make_async_copy(psib.at[dst, q, rows], pv.at[q, 1], ld_p.at[q, 1])
        r = pltpu.make_async_copy(rin.at[q, jnp.maximum(s - 1, 0), rows], ov.at[q, h], ld_r.at[q])
        return p0, p1, r

    def rs_copy(q, e):
        s, h = e // parts, e % parts
        return rcopy(ov.at[q, h], rin.at[q, s, rows_of(h)], rs_send.at[q, h], rs_recv.at[q, s, h], ring[q])

    def rs_start(q, e):
        s, h = e // parts, e % parts
        fresh = s <= H - 2
        if q == 0:
            fresh = jnp.logical_or(fresh, jnp.logical_or(s == H - 1, s == N - 1))

        @pl.when(jnp.logical_and(h == 0, fresh))
        def _():
            dst = rs_dest(q, s)
            rcopy(psib.at[dst], psib.at[dst], st_rem.at[0], part_recv.at[dst], sib).wait_recv()

        p0, p1, r = rs_loads(q, e)
        p0.start()
        p1.start()

        @pl.when(e >= parts)
        def _():
            rs_copy(q, e - parts).wait_send()
            rs_copy(q, e - parts).wait_recv()
            r.start()

    def rs_finish(e):
        h = e % parts
        loads = [rs_loads(q, e) for q in range(2)]
        for p0, p1, _ in loads:
            p0.wait()
            p1.wait()
        step = min(64, part)

        def add(first):
            def body(i, carry):
                rr = pl.ds(pl.multiple_of(i * step, step), step)
                for q in range(2):
                    total = pv[q, 0, rr, :] + pv[q, 1, rr, :]
                    ov[q, h, rr, :] = total if first else ov[q, h, rr, :] + total
                return carry
            lax.fori_loop(0, part // step, body, 0)

        @pl.when(e < parts)
        def _():
            add(True)

        @pl.when(e >= parts)
        def _():
            for _, _, r in loads:
                r.wait()
            add(False)

        @pl.when(e < parts * (N - 1))
        def _():
            for q in range(2):
                rs_copy(q, e).start()

    def stage_loc(b, j):
        return pltpu.make_async_copy(stage.at[b], pown.at[j], st_loc.at[b])

    def stage_rem(b, j):
        return rcopy(stage.at[b], psib.at[j], st_rem.at[b], part_recv.at[j], sib)

    def source_rank(k, j):
        px, py = cycle_chip(k, n, j)
        return py * (2 * n) + 2 * px + k

    def dg_copy(u, b, p):
        return rcopy(dg_out.at[p], dg_in.at[rank], dg_send.at[u, b], dg_recv, peer(p))

    def stage_start(u):
        for b, (k, j) in enumerate(unit_blocks(u)):
            @pl.when(k == c)
            def _(b=b, j=j):
                stage_loc(b, j).start()

            @pl.when(k != c)
            def _(b=b, j=j):
                stage_rem(b, j).start()

            p = source_rank(k, j)

            @pl.when(p != rank)
            def _(b=b, p=p):
                dg_copy(u, b, p).start()

    def stage_wait(u, local):
        for b, (k, j) in enumerate(unit_blocks(u)):
            if local:
                @pl.when(k == c)
                def _(b=b, j=j):
                    stage_loc(b, j).wait()
            else:
                @pl.when(k != c)
                def _(b=b, j=j):
                    stage_rem(b, j).wait_send()

    start_loads(0)
    tri_ref[...] = (lax.broadcasted_iota(jnp.int32, (tok, tok), 0) <= lax.broadcasted_iota(jnp.int32, (tok, tok), 1)).astype(F32).astype(BF)
    for e in range(el):
        acc1[e] = jnp.zeros(acc1.shape[1:], F32)
        acc3[e] = jnp.zeros(acc3.shape[1:], F32)
        acc2[e] = jnp.zeros(acc2.shape[1:], F32)

    def gather_stage(u):
        rows = lax.broadcasted_iota(jnp.int32, (cap, tok), 0).astype(F32)
        lanes = lax.broadcasted_iota(jnp.int32, (tok, cap), 1).astype(F32)
        scale_all = []
        for b in range(2):
            ids = mv[b, :top, :]
            gts = mv[b, top:, :]
            masks, gws = [], []
            for e in range(el):
                hit = ids == (first + e).astype(F32)
                masks.append(jnp.sum(jnp.where(hit, 1.0, 0.0), axis=0, keepdims=True))
                gws.append(jnp.sum(jnp.where(hit, gts, 0.0), axis=0, keepdims=True))
            mask = jnp.concatenate(masks + [jnp.zeros((8 - el, tok), F32)], axis=0)
            cum = mm(mask.astype(BF), tri_ref[...])
            pos = jnp.where(mask > 0.0, cum - 1.0, -1.0)
            gw = jnp.concatenate(gws + [jnp.zeros((8 - el, tok), F32)], axis=0)
            cols = jnp.concatenate([pos, gw], axis=0).T
            gc_ref[b] = cols
            scales = []
            for e in range(el):
                hit = rows == pos[e:e + 1, :]
                pk_ref[b, e * cap:(e + 1) * cap, :] = jnp.where(hit, 1.0, 0.0).astype(BF)
                scales.append(jnp.sum(jnp.where(hit, gw[e:e + 1, :], 0.0), axis=1, keepdims=True))
                pt_ref[b, :, e * cap:(e + 1) * cap] = jnp.where(lanes == cols[:, e:e + 1], 1.0, 0.0).astype(BF)
            scale_all.append(jnp.concatenate(scales, axis=0))
        for b in range(2):
            p = pk_ref[b]
            xr = mm(p, xv[b]).astype(BF)
            dr = (scale_all[b] * mm(p, dv_[u % 2, b])).astype(BF)
            for e in range(el):
                xs_ref[e, b * cap:(b + 1) * cap, :] = xr[e * cap:(e + 1) * cap]
                do_ref[e, b * cap:(b + 1) * cap, :] = dr[e * cap:(e + 1) * cap]

    def expert_a(e):
        xs = xs_ref[e]
        uu = mm(xs, w1_ref[e]).astype(BF).astype(F32)
        vv = mm(xs, w3_ref[e]).astype(BF).astype(F32)
        sg = jax.nn.sigmoid(uu)
        a = (uu * sg * vv).astype(BF)
        o_ref[e] = mm(a, w2_ref[e]).astype(BF)
        do = do_ref[e]
        da = mm(do, w2_ref[e], ((1,), (1,)))
        du_ref[e] = (da * vv * sg * (1.0 + uu * (1.0 - sg))).astype(BF)
        dw_ref[e] = (da * uu * sg).astype(BF)
        acc2[e] += mm(a, do, ((0,), (0,)))

    def expert_b(e):
        xs = xs_ref[e]
        du = du_ref[e]
        dw = dw_ref[e]
        dxs = (mm(du, w1_ref[e], ((1,), (1,))) + mm(dw, w3_ref[e], ((1,), (1,)))).astype(BF)
        for b in range(2):
            dxs_ref[b, e * cap:(e + 1) * cap, :] = dxs[b * cap:(b + 1) * cap, :]
        acc1[e] += mm(xs, du, ((0,), (0,)))
        acc3[e] += mm(xs, dw, ((0,), (0,)))

    def scatter_stage(u):
        for b, (k, j) in enumerate(unit_blocks(u)):
            dyf = dv_[u % 2, b].astype(F32)
            yacc = None
            dgs = []
            for e in range(el):
                so = mm(pt_ref[b, :, e * cap:(e + 1) * cap], o_ref[e, b * cap:(b + 1) * cap, :])
                dgs.append(jnp.sum(dyf * so, axis=1, keepdims=True))
                term = gc_ref[b, :, 8 + e:9 + e] * so
                yacc = term if yacc is None else yacc + term
            stage[b, 0] = yacc
            stage[b, 1] = mm(pt_ref[b], dxs_ref[b])
            dg = jnp.concatenate(dgs + [jnp.zeros((tok, 8 - el), F32)], axis=1).T
            pieces = [dg[e:e + 1, i * lane:(i + 1) * lane] for e in range(el) for i in range(chunks)]
            if len(pieces) < 8:
                pieces.append(jnp.zeros((8 - len(pieces), lane), F32))
            dg = jnp.concatenate(pieces, axis=0)
            p = source_rank(k, j)
            dg_out[p] = dg

    def unit(u, carry):
        late = u >= rs_extra
        ahead_of = jnp.where(late, u - rs_extra, 0)

        def tick(i):
            if i != 2:
                ahead = 3 * u + min(i, 2) - 4
                t = ahead // 4 + 2
                due = jnp.logical_and(ahead >= 0, t <= H)

                @pl.when(jnp.logical_and(due, ahead % 4 == 0))
                def _():
                    ag_part((0, 1), t)

                @pl.when(jnp.logical_and(due, ahead % 4 == 2))
                def _():
                    ag_part((2,), t)

            ev = 1 + 3 * (u - rs_unit) + ahead_of + min(i, 2)
            if i == 3:
                ev = ev + jnp.where(late, 1, 0)
            live = late if i == 2 else u >= 0

            @pl.when(jnp.logical_and(live, ev >= 1))
            def _():
                rs_finish(ev - 1)

            @pl.when(jnp.logical_and(live, ev >= 0))
            def _():
                rs_start(0, ev)
                rs_start(1, ev)

        wait_loads(u)

        @pl.when(u == 0)
        def _():
            for i, (src, dst) in enumerate(weights):
                pltpu.make_async_copy(src, dst, ld_w.at[i]).wait()

        gather_stage(u)
        expert_a(0)

        @pl.when(u >= 1)
        def _():
            stage_wait(u - 1, True)

        tick(0)
        expert_a(1)
        expert_b(0)
        tick(1)

        @pl.when(jnp.logical_and(u >= 1, u < N - 1))
        def _():
            start_loads(u + 1)

        expert_b(1)
        tick(2)

        @pl.when(u >= 1)
        def _():
            stage_wait(u - 1, False)

        scatter_stage(u)
        stage_start(u)
        tick(3)

        @pl.when(u == 0)
        def _():
            ag_part((0, 1, 2), 1)
            start_loads(1)

        return carry

    lax.fori_loop(0, N, unit, 0)
    stage_wait(N - 1, True)
    def drain_sends():
        for kind in (0, 1, 2):
            for q in range(2):
                def drain(t, carry, kind=kind, q=q):
                    ag_copy(q, kind, t, me).wait_send()
                    return carry
                lax.fori_loop(0, H if (q == 1) == (kind == 2) else H - 1, drain, 0)

            def drain_push(j, carry, kind=kind):
                push(kind, j).wait_send()
                return carry
            lax.fori_loop(0, N, drain_push, 0)

        def drain_dg(u, carry):
            for b in range(2):
                @pl.when(jnp.logical_or(u > 0, c != b))
                def _(b=b):
                    dg_copy(u, b, rank).wait_send()
            return carry
        lax.fori_loop(0, N, drain_dg, 0)
        stage_wait(N - 1, False)

    def finish_dgates():
        dg_in[rank] = dg_out[rank]
        rcopy(dg_in.at[pl.ds(0, nd - 1)], dg_in.at[pl.ds(0, nd - 1)], dg_send.at[0, 0], dg_recv, sib).wait_recv()
        for i in range(chunks):
            lanes = slice(i * lane, (i + 1) * lane)
            ids = om[:top, lanes]

            def pick(p, total, ids=ids, i=i):
                for e in range(el):
                    r = e * chunks + i
                    total = total + jnp.where(ids == (p * el + e).astype(F32), dg_in[p, r:r + 1, :], 0.0)
                return total

            dgates_ref[:, lanes] = lax.fori_loop(0, nd, pick, jnp.zeros((top, lane), F32))

    def tail(e, carry):
        rs_start(0, e)
        rs_start(1, e)
        rs_finish(e)

        @pl.when(e == rs_done + 2)
        def _():
            drain_sends()

        @pl.when(e == parts * (N - 2))
        def _():
            finish_dgates()

        @pl.when(e >= parts * (N - 1))
        def _():
            rows = rows_of(e % parts)
            for q, out in ((0, y_ref), (1, dx_ref)):
                out[rows, :] = ov[q, e % parts].astype(BF)
        return carry

    rs_finish(rs_done - 1)
    lax.fori_loop(rs_done, parts * N, tail, 0)


def store_kernel(*refs):
    k = len(refs) // 2
    copies = [pltpu.make_async_copy(refs[i], refs[k + i], refs[2 * k].at[i]) for i in range(k)]
    for cp in copies:
        cp.start()
    for cp in copies:
        cp.wait()


def store_call(arrays):
    vm = pl.BlockSpec(memory_space=pltpu.VMEM)
    return pl.pallas_call(
        store_kernel,
        in_specs=[vm] * len(arrays),
        out_specs=[pl.BlockSpec(memory_space=pl.ANY)] * len(arrays),
        out_shape=[pltpu.HBM(a.shape, a.dtype) for a in arrays],
        scratch_shapes=[pltpu.SemaphoreType.DMA((len(arrays),))],
        cost_estimate=pl.CostEstimate(flops=1, bytes_accessed=sum(a.size * a.dtype.itemsize for a in arrays), transcendentals=0),
        compiler_params=pltpu.CompilerParams(vmem_limit_bytes=16 * 1024 * 1024),
    )(*[pltpu.with_memory_space_constraint(a, pltpu.VMEM) for a in arrays])


def moe_call(n, cap, ids, gates, x, dy, w1, w3, w2):
    N = n * n
    tok, d = x.shape
    el, _, f = w1.shape
    parts = 4
    part = tok // parts
    meta = (2 * ids.shape[0], tok)
    any_spec = pl.BlockSpec(memory_space=pl.ANY)
    vm = pl.BlockSpec(memory_space=pltpu.VMEM)
    flops = 13 * 2 * 2 * N * el * cap * d * f
    shape = jax.ShapeDtypeStruct
    dma = pltpu.SemaphoreType.DMA
    outs = pl.pallas_call(
        functools.partial(moe_kernel, n, cap),
        in_specs=[any_spec] * 7,
        out_specs=[vm] * 6 + [any_spec] * 6,
        out_shape=[
            pltpu.VMEM((tok, d), BF),
            pltpu.VMEM((tok, d), BF),
            pltpu.VMEM(ids.shape, F32),
            pltpu.VMEM((el, d, f), F32),
            pltpu.VMEM((el, d, f), F32),
            pltpu.VMEM((el, f, d), F32),
            shape((2, N, tok, d), BF),
            shape((2, N, tok, d), BF),
            shape((2, N) + meta, F32),
            shape((N, 2, tok, d), F32),
            shape((N, 2, tok, d), F32),
            shape((2, N - 1, tok, d), F32),
        ],
        scratch_shapes=[
            pltpu.VMEM((el, d, f), BF),
            pltpu.VMEM((el, d, f), BF),
            pltpu.VMEM((el, f, d), BF),
            pltpu.VMEM((2, tok, d), BF),
            pltpu.VMEM((2,) + meta, F32),
            pltpu.VMEM((2, 2, tok, d), BF),
            pltpu.VMEM((el, 2 * cap, d), BF),
            pltpu.VMEM((el, 2 * cap, d), BF),
            pltpu.VMEM((el, 2 * cap, d), BF),
            pltpu.VMEM((2, el * cap, d), BF),
            pltpu.VMEM((el, 2 * cap, f), BF),
            pltpu.VMEM((el, 2 * cap, f), BF),
            pltpu.VMEM((2, el * cap, tok), BF),
            pltpu.VMEM((2, tok, el * cap), BF),
            pltpu.VMEM((2, tok, 16), F32),
            pltpu.VMEM((tok, tok), BF),
            pltpu.VMEM((2, 2, tok, d), F32),
            pltpu.VMEM((2, 2, part, d), F32),
            pltpu.VMEM((2, parts, part, d), F32),
            pltpu.VMEM(meta, F32),
            pltpu.VMEM(ids.shape, jnp.int32),
            pltpu.VMEM((2 * N, 8, tok // max(1, tok // 128)), F32),
            pltpu.VMEM((2 * N, 8, tok // max(1, tok // 128)), F32),
            dma((2, N // 2, 3)),
            dma((2, N // 2, 3)),
            dma((N, 3)),
            dma((N, 3)),
            dma((N,)),
            dma((2, parts)),
            dma((2, N, parts)),
            dma((N, 2)),
            dma(()),
            dma((2,)),
            dma((2,)),
            dma((2,)),
            dma((3,)),
            dma((2,)),
            dma((2,)),
            dma((2, 2)),
            dma((2,)),
            dma((2,)),
        ],
        cost_estimate=pl.CostEstimate(flops=flops, bytes_accessed=2 * N * tok * d * 12, transcendentals=0),
        compiler_params=pltpu.CompilerParams(vmem_limit_bytes=46 * 1024 * 1024, collective_id=0, has_side_effects=True),
    )(x, dy, ids, gates, w1, w3, w2)
    return outs[:6]


def solution(mesh):
    nd = mesh.shape['row'] * mesh.shape['col']
    n = mesh.shape['row']
    grp = ('row', 'col')
    tspec = P(('dp', 'row', 'col'), None)
    wspec = P(grp, None, None)
    gspec = P(('dp', 'row', 'col'), None, None)

    def local(x, ridx, gates, w1, w3, w2, dy):
        tok, d = x.shape
        top = ridx.shape[1]
        el = w1.shape[0]
        ne = el * nd
        cap = min(tok, (4 * tok * top + ne - 1) // ne)
        y, dx, dgt, gw1, gw3, gw2 = store_call(moe_call(n, cap, ridx.T, gates.T, x, dy, w1, w3, w2))
        return y, dx, dgt.T, gw1, gw3, gw2

    return jax.shard_map(local, mesh=mesh, in_specs=(tspec, tspec, tspec, wspec, wspec, wspec, tspec), out_specs=(tspec, tspec, tspec, gspec, gspec, gspec), check_vma=False)
```

```python
import functools

import jax
import jax.numpy as jnp
from jax import lax
from jax.experimental import pallas as pl
from jax.experimental.pallas import tpu as pltpu
from jax.sharding import PartitionSpec as P

BF = jnp.bfloat16
F32 = jnp.float32
MESH = pl.DeviceIdType.MESH


def mm(a, b, dims=((1,), (0,))):
    return lax.dot_general(a, b, (dims, ((), ())), preferred_element_type=F32)


def cycle_index(k, n, x, y):
    return n * ((1 - k) * y + k * x) + (x + y) % n


def cycle_chip(k, n, i):
    r = i // n
    o = (i % n - r + n) % n
    return k * r + (1 - k) * o, k * o + (1 - k) * r


def moe_kernel(n, cap, x_ref, dy_ref, ids_ref, gates_ref, w1_hbm, w3_hbm, w2_hbm,
               y_ref, dx_ref, dgates_ref, acc1, acc3, acc2, xb, db, mb, pown, psib, rin,
               w1_ref, w3_ref, w2_ref, xv, mv, dv_, xs_ref, do_ref, o_ref, dxs_ref, du_ref, dw_ref, pk_ref, pt_ref, gc_ref, tri_ref,
               stage, pv, ov, land, om, oi, dg_out, dg_in,
               ag_send, ag_recv, push_send, push_recv, part_recv, rs_send, rs_recv, dg_send, dg_recv,
               ld_x, ld_m, ld_d, ld_w, st_loc, st_rem, ld_p, ld_r, ld_o):
    N = n * n
    H = N // 2
    row = lax.axis_index('row')
    col = lax.axis_index('col')
    cx = col // 2
    c = col % 2
    cy = row
    tok, d = x_ref.shape
    top = ids_ref.shape[0]
    el = w1_ref.shape[0]
    parts = ov.shape[1]
    part = tok // parts
    pos_k = (cycle_index(0, n, cx, cy), cycle_index(1, n, cx, cy))
    me = (1 - c) * pos_k[0] + c * pos_k[1]
    rank = cy * (2 * n) + 2 * cx + c
    first = rank * el
    nd = 2 * N
    chunks = max(1, tok // 128)
    lane = tok // chunks
    rs_unit = max(N // 2, 4)
    rs_extra = N - 3
    rs_done = 5 + 3 * (N - 1 - rs_unit) + N - 1 - rs_extra

    def device(i):
        px, py = cycle_chip(c, n, i)
        return {'row': py, 'col': 2 * px + c}

    nxt = device((me + 1) % N)
    prv = device((me + N - 1) % N)
    sib = {'row': row, 'col': 2 * cx + 1 - c}
    ring = (nxt, prv)

    def rcopy(src, dst, ss, rs, dev):
        return pltpu.make_async_remote_copy(src_ref=src, dst_ref=dst, send_sem=ss, recv_sem=rs, device_id=dev, device_id_type=MESH)

    def peer(p):
        return {'row': p // (2 * n), 'col': p % (2 * n)}

    barrier = pltpu.get_barrier_semaphore()
    for dev in (nxt, prv, sib):
        pl.semaphore_signal(barrier, inc=1, device_id=dev, device_id_type=MESH)
    small = (pltpu.make_async_copy(ids_ref, oi, ld_o.at[0]), pltpu.make_async_copy(gates_ref, om.at[pl.ds(top, top)], ld_o.at[1]))
    for cp in small:
        cp.start()
    pl.semaphore_wait(barrier, 3)

    own = (x_ref, om, dy_ref)
    bufs = (xb, mb, db)

    def ag_copy(q, kind, t, j, src=None):
        slot = bufs[kind].at[c, j]
        return rcopy(slot if src is None else src, slot, ag_send.at[q, t, kind], ag_recv.at[q, t, kind], ring[q])

    def push(kind, j, src=None):
        slot = bufs[kind].at[c, j]
        return rcopy(slot if src is None else src, slot, push_send.at[j, kind], push_recv.at[j, kind], sib)

    def push_arrival(kind, k, j):
        slot = bufs[kind].at[k, j]
        return rcopy(slot, slot, push_send.at[j, kind], push_recv.at[j, kind], sib)

    for kind in (0, 1, 2):
        if kind == 1:
            for cp in small:
                cp.wait()
            om[:top, :] = oi[...].astype(F32)
        ag_copy(0, kind, 0, me, own[kind]).start()
        ag_copy(1, kind, 0, me, own[kind]).start()
        push(kind, me, own[kind]).start()

    weights = ((w1_hbm, w1_ref), (w3_hbm, w3_ref), (w2_hbm, w2_ref))
    for i, (src, dst) in enumerate(weights):
        pltpu.make_async_copy(src, dst, ld_w.at[i]).start()

    def unit_blocks(u):
        o = (u + 1) // 2
        ka = jnp.where(u == 0, 0, (u + 1) % 2)
        kb = jnp.where(u == N - 1, 1, (u + 1) % 2)
        ia = (1 - ka) * pos_k[0] + ka * pos_k[1]
        ib = (1 - kb) * pos_k[0] + kb * pos_k[1]
        return ((ka, (ia - o + N) % N), (kb, (ib + o) % N))

    def block_loads(u, b, k, j, local):
        slot = u % 2
        cps = [pltpu.make_async_copy(x_ref if local else xb.at[k, j], xv.at[b], ld_x.at[b]),
               pltpu.make_async_copy(dy_ref if local else db.at[k, j], dv_.at[slot, b], ld_d.at[b])]
        if not local:
            cps.append(pltpu.make_async_copy(mb.at[k, j], mv.at[b], ld_m.at[b]))
        return cps

    def start_loads(u):
        for b, (k, j) in enumerate(unit_blocks(u)):
            @pl.when(k != c)
            def _(k=k, j=j):
                for kind in (0, 1, 2):
                    push_arrival(kind, k, j).wait_recv()

            @pl.when(jnp.logical_and(u == 0, k == c))
            def _(b=b, k=k, j=j):
                for cp in block_loads(u, b, k, j, True):
                    cp.start()
                mv[b] = om[...]

            @pl.when(jnp.logical_or(u != 0, k != c))
            def _(b=b, k=k, j=j):
                for cp in block_loads(u, b, k, j, False):
                    cp.start()

    def wait_loads(u):
        for b, (k, j) in enumerate(unit_blocks(u)):
            for cp in block_loads(u, b, k, j, True):
                cp.wait()

            @pl.when(jnp.logical_or(u != 0, k != c))
            def _(b=b, k=k, j=j):
                pltpu.make_async_copy(mb.at[k, j], mv.at[b], ld_m.at[b]).wait()

    def ag_part(kinds, t):
        for kind in kinds:
            for q in range(2):
                j = (me - t + N) % N if q == 0 else (me + t) % N
                reach = H if (q == 1) == (kind == 2) else H - 1

                @pl.when(t <= reach)
                def _(kind=kind, q=q, j=j, reach=reach):
                    ag_copy(q, kind, t - 1, j).wait_recv()

                    @pl.when(t < reach)
                    def _():
                        ag_copy(q, kind, t, j).start()

                    push(kind, j).start()

    def rs_dest(q, s):
        return (me - 1 - s + 2 * N) % N if q == 0 else (me + 1 + s) % N

    def rows_of(h):
        return pl.ds(pl.multiple_of(h * part, part), part)

    def rs_loads(q, e):
        s, h = e // parts, e % parts
        dst = rs_dest(q, s)
        rows = rows_of(h)
        p0 = pltpu.make_async_copy(pown.at[dst, q, rows], pv.at[q, 0], ld_p.at[q, 0])
        p1 = pltpu.make_async_copy(psib.at[dst, q, rows], pv.at[q, 1], ld_p.at[q, 1])
        r = pltpu.make_async_copy(rin.at[q, jnp.maximum(s - 1, 0), rows], ov.at[q, h], ld_r.at[q])
        return p0, p1, r

    def rs_copy(q, e):
        s, h = e // parts, e % parts
        return rcopy(ov.at[q, h], rin.at[q, s, rows_of(h)], rs_send.at[q, h], rs_recv.at[q, s, h], ring[q])

    final = parts * N - 1

    def rs_last(q):
        return rcopy(ov.at[q, parts - 1], land.at[q], rs_send.at[q, parts - 1], rs_recv.at[q, N - 2, parts - 1], ring[q])

    def rs_start(q, e):
        s, h = e // parts, e % parts
        fresh = s <= H - 2
        if q == 0:
            fresh = jnp.logical_or(fresh, jnp.logical_or(s == H - 1, s == N - 1))

        @pl.when(jnp.logical_and(h == 0, fresh))
        def _():
            dst = rs_dest(q, s)
            rcopy(psib.at[dst], psib.at[dst], st_rem.at[0], part_recv.at[dst], sib).wait_recv()

        p0, p1, r = rs_loads(q, e)
        p0.start()
        p1.start()

        @pl.when(jnp.logical_and(e >= parts, e < final))
        def _():
            rs_copy(q, e - parts).wait_send()
            rs_copy(q, e - parts).wait_recv()
            r.start()

        @pl.when(e == final)
        def _():
            rs_last(q).wait()

    def rs_finish(e):
        h = e % parts
        loads = [rs_loads(q, e) for q in range(2)]
        for p0, p1, _ in loads:
            p0.wait()
            p1.wait()
        step = min(64, part)

        def add(base):
            def body(i, carry):
                rr = pl.ds(pl.multiple_of(i * step, step), step)
                for q in range(2):
                    total = pv[q, 0, rr, :] + pv[q, 1, rr, :]
                    if base == 'arrived':
                        total = ov[q, h, rr, :] + total
                    elif base == 'landed':
                        total = land[q, rr, :] + total
                    ov[q, h, rr, :] = total
                return carry
            lax.fori_loop(0, part // step, body, 0)

        @pl.when(e < parts)
        def _():
            add('none')

        @pl.when(jnp.logical_and(e >= parts, e < final))
        def _():
            for _, _, r in loads:
                r.wait()
            add('arrived')

        @pl.when(e == final)
        def _():
            add('landed')

        @pl.when(e < final - parts)
        def _():
            for q in range(2):
                rs_copy(q, e).start()

        @pl.when(e == final - parts)
        def _():
            for q in range(2):
                rs_last(q).start()

    def stage_loc(b, j):
        return pltpu.make_async_copy(stage.at[b], pown.at[j], st_loc.at[b])

    def stage_rem(b, j):
        return rcopy(stage.at[b], psib.at[j], st_rem.at[b], part_recv.at[j], sib)

    def source_rank(k, j):
        px, py = cycle_chip(k, n, j)
        return py * (2 * n) + 2 * px + k

    def dg_copy(u, b, p):
        return rcopy(dg_out.at[p], dg_in.at[rank], dg_send.at[u, b], dg_recv, peer(p))

    def stage_start(u):
        for b, (k, j) in enumerate(unit_blocks(u)):
            @pl.when(k == c)
            def _(b=b, j=j):
                stage_loc(b, j).start()

            @pl.when(k != c)
            def _(b=b, j=j):
                stage_rem(b, j).start()

            p = source_rank(k, j)

            @pl.when(p != rank)
            def _(b=b, p=p):
                dg_copy(u, b, p).start()

    def stage_wait(u, local):
        for b, (k, j) in enumerate(unit_blocks(u)):
            if local:
                @pl.when(k == c)
                def _(b=b, j=j):
                    stage_loc(b, j).wait()
            else:
                @pl.when(k != c)
                def _(b=b, j=j):
                    stage_rem(b, j).wait_send()

    start_loads(0)
    tri_ref[...] = (lax.broadcasted_iota(jnp.int32, (tok, tok), 0) <= lax.broadcasted_iota(jnp.int32, (tok, tok), 1)).astype(F32).astype(BF)
    for e in range(el):
        acc1[e] = jnp.zeros(acc1.shape[1:], F32)
        acc3[e] = jnp.zeros(acc3.shape[1:], F32)
        acc2[e] = jnp.zeros(acc2.shape[1:], F32)

    def gather_stage(u):
        rows = lax.broadcasted_iota(jnp.int32, (cap, tok), 0).astype(F32)
        lanes = lax.broadcasted_iota(jnp.int32, (tok, cap), 1).astype(F32)
        scale_all = []
        for b in range(2):
            ids = mv[b, :top, :]
            gts = mv[b, top:, :]
            masks, gws = [], []
            for e in range(el):
                hit = ids == (first + e).astype(F32)
                masks.append(jnp.sum(jnp.where(hit, 1.0, 0.0), axis=0, keepdims=True))
                gws.append(jnp.sum(jnp.where(hit, gts, 0.0), axis=0, keepdims=True))
            mask = jnp.concatenate(masks + [jnp.zeros((8 - el, tok), F32)], axis=0)
            cum = mm(mask.astype(BF), tri_ref[...])
            pos = jnp.where(mask > 0.0, cum - 1.0, -1.0)
            gw = jnp.concatenate(gws + [jnp.zeros((8 - el, tok), F32)], axis=0)
            cols = jnp.concatenate([pos, gw], axis=0).T
            gc_ref[b] = cols
            scales = []
            for e in range(el):
                hit = rows == pos[e:e + 1, :]
                pk_ref[b, e * cap:(e + 1) * cap, :] = jnp.where(hit, 1.0, 0.0).astype(BF)
                scales.append(jnp.sum(jnp.where(hit, gw[e:e + 1, :], 0.0), axis=1, keepdims=True))
                pt_ref[b, :, e * cap:(e + 1) * cap] = jnp.where(lanes == cols[:, e:e + 1], 1.0, 0.0).astype(BF)
            scale_all.append(jnp.concatenate(scales, axis=0))
        for b in range(2):
            p = pk_ref[b]
            xr = mm(p, xv[b]).astype(BF)
            dr = (scale_all[b] * mm(p, dv_[u % 2, b])).astype(BF)
            for e in range(el):
                xs_ref[e, b * cap:(b + 1) * cap, :] = xr[e * cap:(e + 1) * cap]
                do_ref[e, b * cap:(b + 1) * cap, :] = dr[e * cap:(e + 1) * cap]

    def expert_a(e):
        xs = xs_ref[e]
        uu = mm(xs, w1_ref[e]).astype(BF).astype(F32)
        vv = mm(xs, w3_ref[e]).astype(BF).astype(F32)
        sg = jax.nn.sigmoid(uu)
        a = (uu * sg * vv).astype(BF)
        o_ref[e] = mm(a, w2_ref[e]).astype(BF)
        do = do_ref[e]
        da = mm(do, w2_ref[e], ((1,), (1,)))
        du_ref[e] = (da * vv * sg * (1.0 + uu * (1.0 - sg))).astype(BF)
        dw_ref[e] = (da * uu * sg).astype(BF)
        acc2[e] += mm(a, do, ((0,), (0,)))

    def expert_b(e):
        xs = xs_ref[e]
        du = du_ref[e]
        dw = dw_ref[e]
        dxs = (mm(du, w1_ref[e], ((1,), (1,))) + mm(dw, w3_ref[e], ((1,), (1,)))).astype(BF)
        for b in range(2):
            dxs_ref[b, e * cap:(e + 1) * cap, :] = dxs[b * cap:(b + 1) * cap, :]
        acc1[e] += mm(xs, du, ((0,), (0,)))
        acc3[e] += mm(xs, dw, ((0,), (0,)))

    def scatter_stage(u):
        for b, (k, j) in enumerate(unit_blocks(u)):
            dyf = dv_[u % 2, b].astype(F32)
            yacc = None
            dgs = []
            for e in range(el):
                so = mm(pt_ref[b, :, e * cap:(e + 1) * cap], o_ref[e, b * cap:(b + 1) * cap, :])
                dgs.append(jnp.sum(dyf * so, axis=1, keepdims=True))
                term = gc_ref[b, :, 8 + e:9 + e] * so
                yacc = term if yacc is None else yacc + term
            stage[b, 0] = yacc
            stage[b, 1] = mm(pt_ref[b], dxs_ref[b])
            dg = jnp.concatenate(dgs + [jnp.zeros((tok, 8 - el), F32)], axis=1).T
            pieces = [dg[e:e + 1, i * lane:(i + 1) * lane] for e in range(el) for i in range(chunks)]
            if len(pieces) < 8:
                pieces.append(jnp.zeros((8 - len(pieces), lane), F32))
            dg = jnp.concatenate(pieces, axis=0)
            p = source_rank(k, j)
            dg_out[p] = dg

    def unit(u, carry):
        late = u >= rs_extra
        ahead_of = jnp.where(late, u - rs_extra, 0)

        def tick(i):
            if i != 2:
                ahead = 3 * u + min(i, 2) - 4
                t = ahead // 4 + 2
                due = jnp.logical_and(ahead >= 0, t <= H)

                @pl.when(jnp.logical_and(due, ahead % 4 == 0))
                def _():
                    ag_part((0, 1), t)

                @pl.when(jnp.logical_and(due, ahead % 4 == 2))
                def _():
                    ag_part((2,), t)

            ev = 1 + 3 * (u - rs_unit) + ahead_of + min(i, 2)
            if i == 3:
                ev = ev + jnp.where(late, 1, 0)
            live = late if i == 2 else u >= 0

            @pl.when(jnp.logical_and(live, ev >= 1))
            def _():
                rs_finish(ev - 1)

            @pl.when(jnp.logical_and(live, ev >= 0))
            def _():
                rs_start(0, ev)
                rs_start(1, ev)

        wait_loads(u)

        @pl.when(u == 0)
        def _():
            for i, (src, dst) in enumerate(weights):
                pltpu.make_async_copy(src, dst, ld_w.at[i]).wait()

        gather_stage(u)
        expert_a(0)

        @pl.when(u >= 1)
        def _():
            stage_wait(u - 1, True)

        tick(0)
        expert_a(1)
        expert_b(0)
        tick(1)

        @pl.when(jnp.logical_and(u >= 1, u < N - 1))
        def _():
            start_loads(u + 1)

        expert_b(1)
        tick(2)

        @pl.when(u >= 1)
        def _():
            stage_wait(u - 1, False)

        scatter_stage(u)
        stage_start(u)
        tick(3)

        @pl.when(u == 0)
        def _():
            ag_part((0, 1, 2), 1)
            start_loads(1)

        return carry

    lax.fori_loop(0, N, unit, 0)
    stage_wait(N - 1, True)
    def drain_sends():
        for kind in (0, 1, 2):
            for q in range(2):
                def drain(t, carry, kind=kind, q=q):
                    ag_copy(q, kind, t, me).wait_send()
                    return carry
                lax.fori_loop(0, H if (q == 1) == (kind == 2) else H - 1, drain, 0)

            def drain_push(j, carry, kind=kind):
                push(kind, j).wait_send()
                return carry
            lax.fori_loop(0, N, drain_push, 0)

        def drain_dg(u, carry):
            for b in range(2):
                @pl.when(jnp.logical_or(u > 0, c != b))
                def _(b=b):
                    dg_copy(u, b, rank).wait_send()
            return carry
        lax.fori_loop(0, N, drain_dg, 0)
        stage_wait(N - 1, False)

    def finish_dgates():
        dg_in[rank] = dg_out[rank]
        rcopy(dg_in.at[pl.ds(0, nd - 1)], dg_in.at[pl.ds(0, nd - 1)], dg_send.at[0, 0], dg_recv, sib).wait_recv()
        for i in range(chunks):
            lanes = slice(i * lane, (i + 1) * lane)
            ids = om[:top, lanes]

            def pick(p, total, ids=ids, i=i):
                for e in range(el):
                    r = e * chunks + i
                    total = total + jnp.where(ids == (p * el + e).astype(F32), dg_in[p, r:r + 1, :], 0.0)
                return total

            dgates_ref[:, lanes] = lax.fori_loop(0, nd, pick, jnp.zeros((top, lane), F32))

    def tail(e, carry):
        rs_start(0, e)
        rs_start(1, e)
        rs_finish(e)

        @pl.when(e == rs_done + 2)
        def _():
            drain_sends()

        @pl.when(e == parts * (N - 2))
        def _():
            finish_dgates()

        @pl.when(e >= parts * (N - 1))
        def _():
            rows = rows_of(e % parts)
            for q, out in ((0, y_ref), (1, dx_ref)):
                out[rows, :] = ov[q, e % parts].astype(BF)
        return carry

    rs_finish(rs_done - 1)
    lax.fori_loop(rs_done, parts * N, tail, 0)


def store_kernel(*refs):
    k = len(refs) // 2
    copies = [pltpu.make_async_copy(refs[i], refs[k + i], refs[2 * k].at[i]) for i in range(k)]
    for cp in copies:
        cp.start()
    for cp in copies:
        cp.wait()


def store_call(arrays):
    vm = pl.BlockSpec(memory_space=pltpu.VMEM)
    return pl.pallas_call(
        store_kernel,
        in_specs=[vm] * len(arrays),
        out_specs=[pl.BlockSpec(memory_space=pl.ANY)] * len(arrays),
        out_shape=[pltpu.HBM(a.shape, a.dtype) for a in arrays],
        scratch_shapes=[pltpu.SemaphoreType.DMA((len(arrays),))],
        cost_estimate=pl.CostEstimate(flops=1, bytes_accessed=sum(a.size * a.dtype.itemsize for a in arrays), transcendentals=0),
        compiler_params=pltpu.CompilerParams(vmem_limit_bytes=16 * 1024 * 1024),
    )(*[pltpu.with_memory_space_constraint(a, pltpu.VMEM) for a in arrays])


def moe_call(n, cap, ids, gates, x, dy, w1, w3, w2):
    N = n * n
    tok, d = x.shape
    el, _, f = w1.shape
    parts = 4
    part = tok // parts
    meta = (2 * ids.shape[0], tok)
    any_spec = pl.BlockSpec(memory_space=pl.ANY)
    vm = pl.BlockSpec(memory_space=pltpu.VMEM)
    flops = 13 * 2 * 2 * N * el * cap * d * f
    shape = jax.ShapeDtypeStruct
    dma = pltpu.SemaphoreType.DMA
    outs = pl.pallas_call(
        functools.partial(moe_kernel, n, cap),
        in_specs=[any_spec] * 7,
        out_specs=[vm] * 6 + [any_spec] * 6,
        out_shape=[
            pltpu.VMEM((tok, d), BF),
            pltpu.VMEM((tok, d), BF),
            pltpu.VMEM(ids.shape, F32),
            pltpu.VMEM((el, d, f), F32),
            pltpu.VMEM((el, d, f), F32),
            pltpu.VMEM((el, f, d), F32),
            shape((2, N, tok, d), BF),
            shape((2, N, tok, d), BF),
            shape((2, N) + meta, F32),
            shape((N, 2, tok, d), F32),
            shape((N, 2, tok, d), F32),
            shape((2, N - 1, tok, d), F32),
        ],
        scratch_shapes=[
            pltpu.VMEM((el, d, f), BF),
            pltpu.VMEM((el, d, f), BF),
            pltpu.VMEM((el, f, d), BF),
            pltpu.VMEM((2, tok, d), BF),
            pltpu.VMEM((2,) + meta, F32),
            pltpu.VMEM((2, 2, tok, d), BF),
            pltpu.VMEM((el, 2 * cap, d), BF),
            pltpu.VMEM((el, 2 * cap, d), BF),
            pltpu.VMEM((el, 2 * cap, d), BF),
            pltpu.VMEM((2, el * cap, d), BF),
            pltpu.VMEM((el, 2 * cap, f), BF),
            pltpu.VMEM((el, 2 * cap, f), BF),
            pltpu.VMEM((2, el * cap, tok), BF),
            pltpu.VMEM((2, tok, el * cap), BF),
            pltpu.VMEM((2, tok, 16), F32),
            pltpu.VMEM((tok, tok), BF),
            pltpu.VMEM((2, 2, tok, d), F32),
            pltpu.VMEM((2, 2, part, d), F32),
            pltpu.VMEM((2, parts, part, d), F32),
            pltpu.VMEM((2, part, d), F32),
            pltpu.VMEM(meta, F32),
            pltpu.VMEM(ids.shape, jnp.int32),
            pltpu.VMEM((2 * N, 8, tok // max(1, tok // 128)), F32),
            pltpu.VMEM((2 * N, 8, tok // max(1, tok // 128)), F32),
            dma((2, N // 2, 3)),
            dma((2, N // 2, 3)),
            dma((N, 3)),
            dma((N, 3)),
            dma((N,)),
            dma((2, parts)),
            dma((2, N, parts)),
            dma((N, 2)),
            dma(()),
            dma((2,)),
            dma((2,)),
            dma((2,)),
            dma((3,)),
            dma((2,)),
            dma((2,)),
            dma((2, 2)),
            dma((2,)),
            dma((2,)),
        ],
        cost_estimate=pl.CostEstimate(flops=flops, bytes_accessed=2 * N * tok * d * 12, transcendentals=0),
        compiler_params=pltpu.CompilerParams(vmem_limit_bytes=46 * 1024 * 1024, collective_id=0, has_side_effects=True),
    )(x, dy, ids, gates, w1, w3, w2)
    return outs[:6]


def solution(mesh):
    nd = mesh.shape['row'] * mesh.shape['col']
    n = mesh.shape['row']
    grp = ('row', 'col')
    tspec = P(('dp', 'row', 'col'), None)
    wspec = P(grp, None, None)
    gspec = P(('dp', 'row', 'col'), None, None)

    def local(x, ridx, gates, w1, w3, w2, dy):
        tok, d = x.shape
        top = ridx.shape[1]
        el = w1.shape[0]
        ne = el * nd
        cap = min(tok, (4 * tok * top + ne - 1) // ne)
        y, dx, dgt, gw1, gw3, gw2 = store_call(moe_call(n, cap, ridx.T, gates.T, x, dy, w1, w3, w2))
        return y, dx, dgt.T, gw1, gw3, gw2

    return jax.shard_map(local, mesh=mesh, in_specs=(tspec, tspec, tspec, wspec, wspec, wspec, tspec), out_specs=(tspec, tspec, tspec, gspec, gspec, gspec), check_vma=False)
```

```python
import functools

import jax
import jax.numpy as jnp
from jax import lax
from jax.experimental import pallas as pl
from jax.experimental.pallas import tpu as pltpu
from jax.sharding import PartitionSpec as P

BF = jnp.bfloat16
F32 = jnp.float32
MESH = pl.DeviceIdType.MESH


def mm(a, b, dims=((1,), (0,))):
    return lax.dot_general(a, b, (dims, ((), ())), preferred_element_type=F32)


def cycle_index(k, n, x, y):
    return n * ((1 - k) * y + k * x) + (x + y) % n


def cycle_chip(k, n, i):
    r = i // n
    o = (i % n - r + n) % n
    return k * r + (1 - k) * o, k * o + (1 - k) * r


def moe_kernel(n, cap, x_ref, dy_ref, ids_ref, gates_ref, w1_hbm, w3_hbm, w2_hbm,
               y_ref, dx_ref, dgates_ref, acc1, acc3, acc2, xb, db, mb, ib, pown, psib, rin,
               w1_ref, w3_ref, w2_ref, xv, mv, iv, dv_, xs_ref, do_ref, o_ref, dxs_ref, du_ref, dw_ref, pk_ref, pt_ref, gc_ref, tri_ref,
               stage, pv, ov, land, oi, oh, dg_out, dg_in,
               ag_send, ag_recv, push_send, push_recv, part_recv, rs_send, rs_recv, dg_send, dg_recv,
               ld_x, ld_m, ld_i, ld_d, ld_w, st_loc, st_rem, ld_p, ld_r, ld_o):
    N = n * n
    H = N // 2
    row = lax.axis_index('row')
    col = lax.axis_index('col')
    cx = col // 2
    c = col % 2
    cy = row
    tok, d = x_ref.shape
    top = ids_ref.shape[0]
    el = w1_ref.shape[0]
    parts = ov.shape[1]
    part = tok // parts
    pos_k = (cycle_index(0, n, cx, cy), cycle_index(1, n, cx, cy))
    me = (1 - c) * pos_k[0] + c * pos_k[1]
    rank = cy * (2 * n) + 2 * cx + c
    first = rank * el
    nd = 2 * N
    chunks = max(1, tok // 128)
    lane = tok // chunks
    rs_unit = max(N // 2, 4)
    rs_extra = N - 3
    rs_done = 5 + 3 * (N - 1 - rs_unit) + N - 1 - rs_extra

    def device(i):
        px, py = cycle_chip(c, n, i)
        return {'row': py, 'col': 2 * px + c}

    nxt = device((me + 1) % N)
    prv = device((me + N - 1) % N)
    sib = {'row': row, 'col': 2 * cx + 1 - c}
    ring = (nxt, prv)

    def rcopy(src, dst, ss, rs, dev):
        return pltpu.make_async_remote_copy(src_ref=src, dst_ref=dst, send_sem=ss, recv_sem=rs, device_id=dev, device_id_type=MESH)

    def peer(p):
        return {'row': p // (2 * n), 'col': p % (2 * n)}

    barrier = pltpu.get_barrier_semaphore()
    for dev in (nxt, prv, sib):
        pl.semaphore_signal(barrier, inc=1, device_id=dev, device_id_type=MESH)
    own_ids = pltpu.make_async_copy(ids_ref, oi, ld_o)
    own_ids.start()
    pl.semaphore_wait(barrier, 3)

    own = (x_ref, gates_ref, dy_ref, oh)
    bufs = (xb, mb, db, ib)

    def ag_copy(q, kind, t, j, src=None):
        slot = bufs[kind].at[c, j]
        return rcopy(slot if src is None else src, slot, ag_send.at[q, t, kind], ag_recv.at[q, t, kind], ring[q])

    def push(kind, j, src=None):
        slot = bufs[kind].at[c, j]
        return rcopy(slot if src is None else src, slot, push_send.at[j, kind], push_recv.at[j, kind], sib)

    def push_arrival(kind, k, j):
        slot = bufs[kind].at[k, j]
        return rcopy(slot, slot, push_send.at[j, kind], push_recv.at[j, kind], sib)

    for kind in (0, 1, 3, 2):
        if kind == 3:
            own_ids.wait()
            oh[:top, :] = oi[:, :tok // 2].astype(F32).astype(BF)
            oh[top:, :] = oi[:, tok // 2:].astype(F32).astype(BF)
        ag_copy(0, kind, 0, me, own[kind]).start()
        ag_copy(1, kind, 0, me, own[kind]).start()
        push(kind, me, own[kind]).start()

    weights = ((w1_hbm, w1_ref), (w3_hbm, w3_ref), (w2_hbm, w2_ref))
    for i, (src, dst) in enumerate(weights):
        pltpu.make_async_copy(src, dst, ld_w.at[i]).start()

    def unit_blocks(u):
        o = (u + 1) // 2
        ka = jnp.where(u == 0, 0, (u + 1) % 2)
        kb = jnp.where(u == N - 1, 1, (u + 1) % 2)
        ia = (1 - ka) * pos_k[0] + ka * pos_k[1]
        ib = (1 - kb) * pos_k[0] + kb * pos_k[1]
        return ((ka, (ia - o + N) % N), (kb, (ib + o) % N))

    def block_loads(u, b, k, j, local):
        slot = u % 2
        cps = [pltpu.make_async_copy(x_ref if local else xb.at[k, j], xv.at[b], ld_x.at[b]),
               pltpu.make_async_copy(dy_ref if local else db.at[k, j], dv_.at[slot, b], ld_d.at[b])]
        cps.append(pltpu.make_async_copy(gates_ref if local else mb.at[k, j], mv.at[b], ld_m.at[b]))
        if not local:
            cps.append(pltpu.make_async_copy(ib.at[k, j], iv.at[b], ld_i.at[b]))
        return cps

    def start_loads(u):
        for b, (k, j) in enumerate(unit_blocks(u)):
            @pl.when(k != c)
            def _(k=k, j=j):
                for kind in (0, 1, 2, 3):
                    push_arrival(kind, k, j).wait_recv()

            @pl.when(jnp.logical_and(u == 0, k == c))
            def _(b=b, k=k, j=j):
                for cp in block_loads(u, b, k, j, True):
                    cp.start()
                iv[b] = oh[...]

            @pl.when(jnp.logical_or(u != 0, k != c))
            def _(b=b, k=k, j=j):
                for cp in block_loads(u, b, k, j, False):
                    cp.start()

    def wait_loads(u):
        for b, (k, j) in enumerate(unit_blocks(u)):
            for cp in block_loads(u, b, k, j, True):
                cp.wait()

            @pl.when(jnp.logical_or(u != 0, k != c))
            def _(b=b, k=k, j=j):
                pltpu.make_async_copy(ib.at[k, j], iv.at[b], ld_i.at[b]).wait()

    def ag_part(kinds, t):
        for kind in kinds:
            for q in range(2):
                j = (me - t + N) % N if q == 0 else (me + t) % N
                reach = H if (q == 1) == (kind == 2) else H - 1

                @pl.when(t <= reach)
                def _(kind=kind, q=q, j=j, reach=reach):
                    ag_copy(q, kind, t - 1, j).wait_recv()

                    @pl.when(t < reach)
                    def _():
                        ag_copy(q, kind, t, j).start()

                    push(kind, j).start()

    def rs_dest(q, s):
        return (me - 1 - s + 2 * N) % N if q == 0 else (me + 1 + s) % N

    def rows_of(h):
        return pl.ds(pl.multiple_of(h * part, part), part)

    def rs_loads(q, e):
        s, h = e // parts, e % parts
        dst = rs_dest(q, s)
        rows = rows_of(h)
        p0 = pltpu.make_async_copy(pown.at[dst, q, rows], pv.at[q, 0], ld_p.at[q, 0])
        p1 = pltpu.make_async_copy(psib.at[dst, q, rows], pv.at[q, 1], ld_p.at[q, 1])
        r = pltpu.make_async_copy(rin.at[q, jnp.maximum(s - 1, 0), rows], ov.at[q, h], ld_r.at[q])
        return p0, p1, r

    def rs_copy(q, e):
        s, h = e // parts, e % parts
        return rcopy(ov.at[q, h], rin.at[q, s, rows_of(h)], rs_send.at[q, h], rs_recv.at[q, s, h], ring[q])

    final = parts * N - 1

    def rs_last(q):
        return rcopy(ov.at[q, parts - 1], land.at[q], rs_send.at[q, parts - 1], rs_recv.at[q, N - 2, parts - 1], ring[q])

    def rs_start(q, e):
        s, h = e // parts, e % parts
        fresh = s <= H - 2
        if q == 0:
            fresh = jnp.logical_or(fresh, jnp.logical_or(s == H - 1, s == N - 1))

        @pl.when(jnp.logical_and(h == 0, fresh))
        def _():
            dst = rs_dest(q, s)
            rcopy(psib.at[dst], psib.at[dst], st_rem.at[0], part_recv.at[dst], sib).wait_recv()

        p0, p1, r = rs_loads(q, e)
        p0.start()
        p1.start()

        @pl.when(jnp.logical_and(e >= parts, e < final))
        def _():
            rs_copy(q, e - parts).wait_send()
            rs_copy(q, e - parts).wait_recv()
            r.start()

        @pl.when(e == final)
        def _():
            rs_last(q).wait()

    def rs_finish(e):
        h = e % parts
        loads = [rs_loads(q, e) for q in range(2)]
        for p0, p1, _ in loads:
            p0.wait()
            p1.wait()
        step = min(64, part)

        def add(base):
            def body(i, carry):
                rr = pl.ds(pl.multiple_of(i * step, step), step)
                for q in range(2):
                    total = pv[q, 0, rr, :] + pv[q, 1, rr, :]
                    if base == 'arrived':
                        total = ov[q, h, rr, :] + total
                    elif base == 'landed':
                        total = land[q, rr, :] + total
                    ov[q, h, rr, :] = total
                return carry
            lax.fori_loop(0, part // step, body, 0)

        @pl.when(e < parts)
        def _():
            add('none')

        @pl.when(jnp.logical_and(e >= parts, e < final))
        def _():
            for _, _, r in loads:
                r.wait()
            add('arrived')

        @pl.when(e == final)
        def _():
            add('landed')

        @pl.when(e < final - parts)
        def _():
            for q in range(2):
                rs_copy(q, e).start()

        @pl.when(e == final - parts)
        def _():
            for q in range(2):
                rs_last(q).start()

    def stage_loc(b, j):
        return pltpu.make_async_copy(stage.at[b], pown.at[j], st_loc.at[b])

    def stage_rem(b, j):
        return rcopy(stage.at[b], psib.at[j], st_rem.at[b], part_recv.at[j], sib)

    def source_rank(k, j):
        px, py = cycle_chip(k, n, j)
        return py * (2 * n) + 2 * px + k

    def dg_copy(u, b, p):
        return rcopy(dg_out.at[p], dg_in.at[rank], dg_send.at[u, b], dg_recv, peer(p))

    def stage_start(u):
        for b, (k, j) in enumerate(unit_blocks(u)):
            @pl.when(k == c)
            def _(b=b, j=j):
                stage_loc(b, j).start()

            @pl.when(k != c)
            def _(b=b, j=j):
                stage_rem(b, j).start()

            p = source_rank(k, j)

            @pl.when(p != rank)
            def _(b=b, p=p):
                dg_copy(u, b, p).start()

    def stage_wait(u, local):
        for b, (k, j) in enumerate(unit_blocks(u)):
            if local:
                @pl.when(k == c)
                def _(b=b, j=j):
                    stage_loc(b, j).wait()
            else:
                @pl.when(k != c)
                def _(b=b, j=j):
                    stage_rem(b, j).wait_send()

    start_loads(0)
    tri_ref[...] = (lax.broadcasted_iota(jnp.int32, (tok, tok), 0) <= lax.broadcasted_iota(jnp.int32, (tok, tok), 1)).astype(F32).astype(BF)
    for e in range(el):
        acc1[e] = jnp.zeros(acc1.shape[1:], F32)
        acc3[e] = jnp.zeros(acc3.shape[1:], F32)
        acc2[e] = jnp.zeros(acc2.shape[1:], F32)

    def gather_stage(u):
        rows = lax.broadcasted_iota(jnp.int32, (cap, tok), 0).astype(F32)
        lanes = lax.broadcasted_iota(jnp.int32, (tok, cap), 1).astype(F32)
        scale_all = []
        for b in range(2):
            halves = iv[b].astype(F32)
            ids = jnp.concatenate([halves[:top], halves[top:]], axis=1)
            gts = mv[b]
            masks, gws = [], []
            for e in range(el):
                hit = ids == (first + e).astype(F32)
                masks.append(jnp.sum(jnp.where(hit, 1.0, 0.0), axis=0, keepdims=True))
                gws.append(jnp.sum(jnp.where(hit, gts, 0.0), axis=0, keepdims=True))
            mask = jnp.concatenate(masks + [jnp.zeros((8 - el, tok), F32)], axis=0)
            cum = mm(mask.astype(BF), tri_ref[...])
            pos = jnp.where(mask > 0.0, cum - 1.0, -1.0)
            gw = jnp.concatenate(gws + [jnp.zeros((8 - el, tok), F32)], axis=0)
            cols = jnp.concatenate([pos, gw], axis=0).T
            gc_ref[b] = cols
            scales = []
            for e in range(el):
                hit = rows == pos[e:e + 1, :]
                pk_ref[b, e * cap:(e + 1) * cap, :] = jnp.where(hit, 1.0, 0.0).astype(BF)
                scales.append(jnp.sum(jnp.where(hit, gw[e:e + 1, :], 0.0), axis=1, keepdims=True))
                pt_ref[b, :, e * cap:(e + 1) * cap] = jnp.where(lanes == cols[:, e:e + 1], 1.0, 0.0).astype(BF)
            scale_all.append(jnp.concatenate(scales, axis=0))
        for b in range(2):
            p = pk_ref[b]
            xr = mm(p, xv[b]).astype(BF)
            dr = (scale_all[b] * mm(p, dv_[u % 2, b])).astype(BF)
            for e in range(el):
                xs_ref[e, b * cap:(b + 1) * cap, :] = xr[e * cap:(e + 1) * cap]
                do_ref[e, b * cap:(b + 1) * cap, :] = dr[e * cap:(e + 1) * cap]

    def expert_a(e):
        xs = xs_ref[e]
        uu = mm(xs, w1_ref[e]).astype(BF).astype(F32)
        vv = mm(xs, w3_ref[e]).astype(BF).astype(F32)
        sg = jax.nn.sigmoid(uu)
        a = (uu * sg * vv).astype(BF)
        o_ref[e] = mm(a, w2_ref[e]).astype(BF)
        do = do_ref[e]
        da = mm(do, w2_ref[e], ((1,), (1,)))
        du_ref[e] = (da * vv * sg * (1.0 + uu * (1.0 - sg))).astype(BF)
        dw_ref[e] = (da * uu * sg).astype(BF)
        acc2[e] += mm(a, do, ((0,), (0,)))

    def expert_b(e):
        xs = xs_ref[e]
        du = du_ref[e]
        dw = dw_ref[e]
        dxs = (mm(du, w1_ref[e], ((1,), (1,))) + mm(dw, w3_ref[e], ((1,), (1,)))).astype(BF)
        for b in range(2):
            dxs_ref[b, e * cap:(e + 1) * cap, :] = dxs[b * cap:(b + 1) * cap, :]
        acc1[e] += mm(xs, du, ((0,), (0,)))
        acc3[e] += mm(xs, dw, ((0,), (0,)))

    def scatter_stage(u):
        for b, (k, j) in enumerate(unit_blocks(u)):
            dyf = dv_[u % 2, b].astype(F32)
            yacc = None
            dgs = []
            for e in range(el):
                so = mm(pt_ref[b, :, e * cap:(e + 1) * cap], o_ref[e, b * cap:(b + 1) * cap, :])
                dgs.append(jnp.sum(dyf * so, axis=1, keepdims=True))
                term = gc_ref[b, :, 8 + e:9 + e] * so
                yacc = term if yacc is None else yacc + term
            stage[b, 0] = yacc
            stage[b, 1] = mm(pt_ref[b], dxs_ref[b])
            dg = jnp.concatenate(dgs + [jnp.zeros((tok, 8 - el), F32)], axis=1).T
            pieces = [dg[e:e + 1, i * lane:(i + 1) * lane] for e in range(el) for i in range(chunks)]
            if len(pieces) < 8:
                pieces.append(jnp.zeros((8 - len(pieces), lane), F32))
            dg = jnp.concatenate(pieces, axis=0)
            p = source_rank(k, j)
            dg_out[p] = dg

    def unit(u, carry):
        late = u >= rs_extra
        ahead_of = jnp.where(late, u - rs_extra, 0)

        def tick(i):
            if i != 2:
                ahead = 3 * u + min(i, 2) - 4
                t = ahead // 4 + 2
                due = jnp.logical_and(ahead >= 0, t <= H)

                @pl.when(jnp.logical_and(due, ahead % 4 == 0))
                def _():
                    ag_part((0, 1, 3), t)

                @pl.when(jnp.logical_and(due, ahead % 4 == 2))
                def _():
                    ag_part((2,), t)

            ev = 1 + 3 * (u - rs_unit) + ahead_of + min(i, 2)
            if i == 3:
                ev = ev + jnp.where(late, 1, 0)
            live = late if i == 2 else u >= 0

            @pl.when(jnp.logical_and(live, ev >= 1))
            def _():
                rs_finish(ev - 1)

            @pl.when(jnp.logical_and(live, ev >= 0))
            def _():
                rs_start(0, ev)
                rs_start(1, ev)

        wait_loads(u)

        @pl.when(u == 0)
        def _():
            for i, (src, dst) in enumerate(weights):
                pltpu.make_async_copy(src, dst, ld_w.at[i]).wait()

        gather_stage(u)
        expert_a(0)

        @pl.when(u >= 1)
        def _():
            stage_wait(u - 1, True)

        tick(0)
        expert_a(1)
        expert_b(0)
        tick(1)

        @pl.when(jnp.logical_and(u >= 1, u < N - 1))
        def _():
            start_loads(u + 1)

        expert_b(1)
        tick(2)

        @pl.when(u >= 1)
        def _():
            stage_wait(u - 1, False)

        scatter_stage(u)
        stage_start(u)
        tick(3)

        @pl.when(u == 0)
        def _():
            ag_part((0, 1, 3, 2), 1)
            start_loads(1)

        return carry

    lax.fori_loop(0, N, unit, 0)
    stage_wait(N - 1, True)
    def drain_sends():
        for kind in (0, 1, 2, 3):
            for q in range(2):
                def drain(t, carry, kind=kind, q=q):
                    ag_copy(q, kind, t, me).wait_send()
                    return carry
                lax.fori_loop(0, H if (q == 1) == (kind == 2) else H - 1, drain, 0)

            def drain_push(j, carry, kind=kind):
                push(kind, j).wait_send()
                return carry
            lax.fori_loop(0, N, drain_push, 0)

        def drain_dg(u, carry):
            for b in range(2):
                @pl.when(jnp.logical_or(u > 0, c != b))
                def _(b=b):
                    dg_copy(u, b, rank).wait_send()
            return carry
        lax.fori_loop(0, N, drain_dg, 0)
        stage_wait(N - 1, False)

    def finish_dgates():
        dg_in[rank] = dg_out[rank]
        rcopy(dg_in.at[pl.ds(0, nd - 1)], dg_in.at[pl.ds(0, nd - 1)], dg_send.at[0, 0], dg_recv, sib).wait_recv()
        for i in range(chunks):
            lanes = slice(i * lane, (i + 1) * lane)
            ids = oi[:, lanes].astype(F32)

            def pick(p, total, ids=ids, i=i):
                for e in range(el):
                    r = e * chunks + i
                    total = total + jnp.where(ids == (p * el + e).astype(F32), dg_in[p, r:r + 1, :], 0.0)
                return total

            dgates_ref[:, lanes] = lax.fori_loop(0, nd, pick, jnp.zeros((top, lane), F32))

    def tail(e, carry):
        rs_start(0, e)
        rs_start(1, e)
        rs_finish(e)

        @pl.when(e == rs_done + 2)
        def _():
            drain_sends()

        @pl.when(e == parts * (N - 2))
        def _():
            finish_dgates()

        @pl.when(e >= parts * (N - 1))
        def _():
            rows = rows_of(e % parts)
            for q, out in ((0, y_ref), (1, dx_ref)):
                out[rows, :] = ov[q, e % parts].astype(BF)
        return carry

    rs_finish(rs_done - 1)
    lax.fori_loop(rs_done, parts * N, tail, 0)


def store_kernel(*refs):
    k = len(refs) // 2
    copies = [pltpu.make_async_copy(refs[i], refs[k + i], refs[2 * k].at[i]) for i in range(k)]
    for cp in copies:
        cp.start()
    for cp in copies:
        cp.wait()


def store_call(arrays):
    vm = pl.BlockSpec(memory_space=pltpu.VMEM)
    return pl.pallas_call(
        store_kernel,
        in_specs=[vm] * len(arrays),
        out_specs=[pl.BlockSpec(memory_space=pl.ANY)] * len(arrays),
        out_shape=[pltpu.HBM(a.shape, a.dtype) for a in arrays],
        scratch_shapes=[pltpu.SemaphoreType.DMA((len(arrays),))],
        cost_estimate=pl.CostEstimate(flops=1, bytes_accessed=sum(a.size * a.dtype.itemsize for a in arrays), transcendentals=0),
        compiler_params=pltpu.CompilerParams(vmem_limit_bytes=16 * 1024 * 1024),
    )(*[pltpu.with_memory_space_constraint(a, pltpu.VMEM) for a in arrays])


def moe_call(n, cap, ids, gates, x, dy, w1, w3, w2):
    N = n * n
    tok, d = x.shape
    el, _, f = w1.shape
    parts = 4
    part = tok // parts
    meta = ids.shape
    halved = (2 * ids.shape[0], tok // 2)
    any_spec = pl.BlockSpec(memory_space=pl.ANY)
    vm = pl.BlockSpec(memory_space=pltpu.VMEM)
    flops = 13 * 2 * 2 * N * el * cap * d * f
    shape = jax.ShapeDtypeStruct
    dma = pltpu.SemaphoreType.DMA
    outs = pl.pallas_call(
        functools.partial(moe_kernel, n, cap),
        in_specs=[any_spec] * 7,
        out_specs=[vm] * 6 + [any_spec] * 7,
        out_shape=[
            pltpu.VMEM((tok, d), BF),
            pltpu.VMEM((tok, d), BF),
            pltpu.VMEM(ids.shape, F32),
            pltpu.VMEM((el, d, f), F32),
            pltpu.VMEM((el, d, f), F32),
            pltpu.VMEM((el, f, d), F32),
            shape((2, N, tok, d), BF),
            shape((2, N, tok, d), BF),
            shape((2, N) + meta, F32),
            shape((2, N) + halved, BF),
            shape((N, 2, tok, d), F32),
            shape((N, 2, tok, d), F32),
            shape((2, N - 1, tok, d), F32),
        ],
        scratch_shapes=[
            pltpu.VMEM((el, d, f), BF),
            pltpu.VMEM((el, d, f), BF),
            pltpu.VMEM((el, f, d), BF),
            pltpu.VMEM((2, tok, d), BF),
            pltpu.VMEM((2,) + meta, F32),
            pltpu.VMEM((2,) + halved, BF),
            pltpu.VMEM((2, 2, tok, d), BF),
            pltpu.VMEM((el, 2 * cap, d), BF),
            pltpu.VMEM((el, 2 * cap, d), BF),
            pltpu.VMEM((el, 2 * cap, d), BF),
            pltpu.VMEM((2, el * cap, d), BF),
            pltpu.VMEM((el, 2 * cap, f), BF),
            pltpu.VMEM((el, 2 * cap, f), BF),
            pltpu.VMEM((2, el * cap, tok), BF),
            pltpu.VMEM((2, tok, el * cap), BF),
            pltpu.VMEM((2, tok, 16), F32),
            pltpu.VMEM((tok, tok), BF),
            pltpu.VMEM((2, 2, tok, d), F32),
            pltpu.VMEM((2, 2, part, d), F32),
            pltpu.VMEM((2, parts, part, d), F32),
            pltpu.VMEM((2, part, d), F32),
            pltpu.VMEM(ids.shape, jnp.int32),
            pltpu.VMEM(halved, BF),
            pltpu.VMEM((2 * N, 8, tok // max(1, tok // 128)), F32),
            pltpu.VMEM((2 * N, 8, tok // max(1, tok // 128)), F32),
            dma((2, N // 2, 4)),
            dma((2, N // 2, 4)),
            dma((N, 4)),
            dma((N, 4)),
            dma((N,)),
            dma((2, parts)),
            dma((2, N, parts)),
            dma((N, 2)),
            dma(()),
            dma((2,)),
            dma((2,)),
            dma((2,)),
            dma((2,)),
            dma((3,)),
            dma((2,)),
            dma((2,)),
            dma((2, 2)),
            dma((2,)),
            dma(()),
        ],
        cost_estimate=pl.CostEstimate(flops=flops, bytes_accessed=2 * N * tok * d * 12, transcendentals=0),
        compiler_params=pltpu.CompilerParams(vmem_limit_bytes=46 * 1024 * 1024, collective_id=0, has_side_effects=True),
    )(x, dy, ids, gates, w1, w3, w2)
    return outs[:6]


def solution(mesh):
    nd = mesh.shape['row'] * mesh.shape['col']
    n = mesh.shape['row']
    grp = ('row', 'col')
    tspec = P(('dp', 'row', 'col'), None)
    wspec = P(grp, None, None)
    gspec = P(('dp', 'row', 'col'), None, None)

    def local(x, ridx, gates, w1, w3, w2, dy):
        tok, d = x.shape
        top = ridx.shape[1]
        el = w1.shape[0]
        ne = el * nd
        cap = min(tok, (4 * tok * top + ne - 1) // ne)
        y, dx, dgt, gw1, gw3, gw2 = store_call(moe_call(n, cap, ridx.T, gates.T, x, dy, w1, w3, w2))
        return y, dx, dgt.T, gw1, gw3, gw2

    return jax.shard_map(local, mesh=mesh, in_specs=(tspec, tspec, tspec, wspec, wspec, wspec, tspec), out_specs=(tspec, tspec, tspec, gspec, gspec, gspec), check_vma=False)
```

```python
import functools

import jax
import jax.numpy as jnp
from jax import lax
from jax.experimental import pallas as pl
from jax.experimental.pallas import tpu as pltpu
from jax.sharding import PartitionSpec as P

BF = jnp.bfloat16
F32 = jnp.float32
MESH = pl.DeviceIdType.MESH


def mm(a, b, dims=((1,), (0,))):
    return lax.dot_general(a, b, (dims, ((), ())), preferred_element_type=F32)


def cycle_index(k, n, x, y):
    return n * ((1 - k) * y + k * x) + (x + y) % n


def cycle_chip(k, n, i):
    r = i // n
    o = (i % n - r + n) % n
    return k * r + (1 - k) * o, k * o + (1 - k) * r


def moe_kernel(n, cap, x_ref, dy_ref, ids_ref, gates_ref, w1_hbm, w3_hbm, w2_hbm,
               y_ref, dx_ref, dgates_ref, acc1, acc3, acc2, xb, db, mb, ib, pown, psib, rin,
               w1_ref, w3_ref, w2_ref, xv, mv, iv, dv_, xs_ref, do_ref, o_ref, dxs_ref, du_ref, dw_ref, pk_ref, pt_ref, gc_ref, tri_ref,
               stage, pv, ov, land, oi, oh, dg_out, dg_in,
               ag_send, ag_recv, push_send, push_recv, part_recv, rs_send, rs_recv, dg_send, dg_recv,
               ld_x, ld_m, ld_i, ld_d, ld_w, st_loc, st_rem, ld_p, ld_r, ld_o):
    N = n * n
    H = N // 2
    row = lax.axis_index('row')
    col = lax.axis_index('col')
    cx = col // 2
    c = col % 2
    cy = row
    tok, d = x_ref.shape
    top = ids_ref.shape[0]
    el = w1_ref.shape[0]
    parts = ov.shape[1]
    part = tok // parts
    pos_k = (cycle_index(0, n, cx, cy), cycle_index(1, n, cx, cy))
    me = (1 - c) * pos_k[0] + c * pos_k[1]
    rank = cy * (2 * n) + 2 * cx + c
    first = rank * el
    nd = 2 * N
    chunks = max(1, tok // 128)
    lane = tok // chunks
    rs_unit = max(N // 2, 4)
    rs_extra = N - 3
    rs_done = 5 + 3 * (N - 1 - rs_unit) + N - 1 - rs_extra

    def device(i):
        px, py = cycle_chip(c, n, i)
        return {'row': py, 'col': 2 * px + c}

    nxt = device((me + 1) % N)
    prv = device((me + N - 1) % N)
    sib = {'row': row, 'col': 2 * cx + 1 - c}
    ring = (nxt, prv)

    def rcopy(src, dst, ss, rs, dev):
        return pltpu.make_async_remote_copy(src_ref=src, dst_ref=dst, send_sem=ss, recv_sem=rs, device_id=dev, device_id_type=MESH)

    def peer(p):
        return {'row': p // (2 * n), 'col': p % (2 * n)}

    barrier = pltpu.get_barrier_semaphore()
    for dev in (nxt, prv, sib):
        pl.semaphore_signal(barrier, inc=1, device_id=dev, device_id_type=MESH)
    own_ids = pltpu.make_async_copy(ids_ref, oi, ld_o)
    own_ids.start()
    pl.semaphore_wait(barrier, 3)

    own = (x_ref, gates_ref, dy_ref, oh)
    bufs = (xb, mb, db, ib)

    def ag_copy(q, kind, t, j, src=None):
        slot = bufs[kind].at[c, j]
        return rcopy(slot if src is None else src, slot, ag_send.at[q, t, kind], ag_recv.at[q, t, kind], ring[q])

    def push(kind, j, src=None):
        slot = bufs[kind].at[c, j]
        return rcopy(slot if src is None else src, slot, push_send.at[j, kind], push_recv.at[j, kind], sib)

    def push_arrival(kind, k, j):
        slot = bufs[kind].at[k, j]
        return rcopy(slot, slot, push_send.at[j, kind], push_recv.at[j, kind], sib)

    for kind in (0, 1, 3, 2):
        if kind == 3:
            own_ids.wait()
            oh[:top, :] = oi[:, :tok // 2].astype(F32).astype(BF)
            oh[top:, :] = oi[:, tok // 2:].astype(F32).astype(BF)
        ag_copy(0, kind, 0, me, own[kind]).start()
        ag_copy(1, kind, 0, me, own[kind]).start()
        push(kind, me, own[kind]).start()

    weights = ((w1_hbm, w1_ref), (w3_hbm, w3_ref), (w2_hbm, w2_ref))
    for i, (src, dst) in enumerate(weights):
        pltpu.make_async_copy(src, dst, ld_w.at[i]).start()

    def unit_blocks(u):
        o = (u + 1) // 2
        ka = jnp.where(u == 0, 0, (u + 1) % 2)
        kb = jnp.where(u == N - 1, 1, (u + 1) % 2)
        ia = (1 - ka) * pos_k[0] + ka * pos_k[1]
        ib = (1 - kb) * pos_k[0] + kb * pos_k[1]
        return ((ka, (ia - o + N) % N), (kb, (ib + o) % N))

    def block_loads(u, b, k, j, local):
        slot = u % 2
        cps = [pltpu.make_async_copy(x_ref if local else xb.at[k, j], xv.at[b], ld_x.at[b]),
               pltpu.make_async_copy(dy_ref if local else db.at[k, j], dv_.at[slot, b], ld_d.at[b])]
        cps.append(pltpu.make_async_copy(gates_ref if local else mb.at[k, j], mv.at[b], ld_m.at[b]))
        if not local:
            cps.append(pltpu.make_async_copy(ib.at[k, j], iv.at[b], ld_i.at[b]))
        return cps

    def start_loads(u):
        for b, (k, j) in enumerate(unit_blocks(u)):
            @pl.when(k != c)
            def _(k=k, j=j):
                for kind in (0, 1, 2, 3):
                    push_arrival(kind, k, j).wait_recv()

            @pl.when(jnp.logical_and(u == 0, k == c))
            def _(b=b, k=k, j=j):
                for cp in block_loads(u, b, k, j, True):
                    cp.start()
                iv[b] = oh[...]

            @pl.when(jnp.logical_or(u != 0, k != c))
            def _(b=b, k=k, j=j):
                for cp in block_loads(u, b, k, j, False):
                    cp.start()

    def wait_loads(u):
        for b, (k, j) in enumerate(unit_blocks(u)):
            for cp in block_loads(u, b, k, j, True):
                cp.wait()

            @pl.when(jnp.logical_or(u != 0, k != c))
            def _(b=b, k=k, j=j):
                pltpu.make_async_copy(ib.at[k, j], iv.at[b], ld_i.at[b]).wait()

    def ag_part(kinds, t):
        for kind in kinds:
            for q in range(2):
                j = (me - t + N) % N if q == 0 else (me + t) % N
                reach = H if (q == 1) == (kind == 2) else H - 1

                @pl.when(t <= reach)
                def _(kind=kind, q=q, j=j, reach=reach):
                    ag_copy(q, kind, t - 1, j).wait_recv()

                    @pl.when(t < reach)
                    def _():
                        ag_copy(q, kind, t, j).start()

                    push(kind, j).start()

    def rs_dest(q, s):
        return (me - 1 - s + 2 * N) % N if q == 0 else (me + 1 + s) % N

    def rows_of(h):
        return pl.ds(pl.multiple_of(h * part, part), part)

    def rs_loads(q, e):
        s, h = e // parts, e % parts
        dst = rs_dest(q, s)
        rows = rows_of(h)
        p0 = pltpu.make_async_copy(pown.at[dst, q, rows], pv.at[q, 0], ld_p.at[q, 0])
        p1 = pltpu.make_async_copy(psib.at[dst, q, rows], pv.at[q, 1], ld_p.at[q, 1])
        r = pltpu.make_async_copy(rin.at[q, jnp.maximum(s - 1, 0), rows], ov.at[q, h], ld_r.at[q])
        return p0, p1, r

    def rs_copy(q, e):
        s, h = e // parts, e % parts
        return rcopy(ov.at[q, h], rin.at[q, s, rows_of(h)], rs_send.at[q, h], rs_recv.at[q, s, h], ring[q])

    final = parts * N - 1

    def rs_last(q):
        return rcopy(ov.at[q, parts - 1], land.at[q], rs_send.at[q, parts - 1], rs_recv.at[q, N - 2, parts - 1], ring[q])

    def rs_start(q, e):
        s, h = e // parts, e % parts
        fresh = s <= H - 2
        if q == 0:
            fresh = jnp.logical_or(fresh, jnp.logical_or(s == H - 1, s == N - 1))

        @pl.when(jnp.logical_and(h == 0, fresh))
        def _():
            dst = rs_dest(q, s)
            rcopy(psib.at[dst], psib.at[dst], st_rem.at[0], part_recv.at[dst], sib).wait_recv()

        p0, p1, r = rs_loads(q, e)
        p0.start()
        p1.start()

        @pl.when(jnp.logical_and(e >= parts, e < final))
        def _():
            rs_copy(q, e - parts).wait_send()
            rs_copy(q, e - parts).wait_recv()
            r.start()

        @pl.when(e == final)
        def _():
            rs_last(q).wait()

    def rs_finish(e):
        h = e % parts
        loads = [rs_loads(q, e) for q in range(2)]
        for p0, p1, _ in loads:
            p0.wait()
            p1.wait()
        step = min(64, part)

        def add(base):
            def body(i, carry):
                rr = pl.ds(pl.multiple_of(i * step, step), step)
                for q in range(2):
                    total = pv[q, 0, rr, :] + pv[q, 1, rr, :]
                    if base == 'arrived':
                        total = ov[q, h, rr, :] + total
                    elif base == 'landed':
                        total = land[q, rr, :] + total
                    ov[q, h, rr, :] = total
                return carry
            lax.fori_loop(0, part // step, body, 0)

        @pl.when(e < parts)
        def _():
            add('none')

        @pl.when(jnp.logical_and(e >= parts, e < final))
        def _():
            for _, _, r in loads:
                r.wait()
            add('arrived')

        @pl.when(e == final)
        def _():
            add('landed')

        @pl.when(e < final - parts)
        def _():
            for q in range(2):
                rs_copy(q, e).start()

        @pl.when(e == final - parts)
        def _():
            for q in range(2):
                rs_last(q).start()

    def stage_loc(b, j):
        return pltpu.make_async_copy(stage.at[b], pown.at[j], st_loc.at[b])

    def stage_rem(b, j):
        return rcopy(stage.at[b], psib.at[j], st_rem.at[b], part_recv.at[j], sib)

    def source_rank(k, j):
        px, py = cycle_chip(k, n, j)
        return py * (2 * n) + 2 * px + k

    def dg_copy(u, b, p):
        return rcopy(dg_out.at[p], dg_in.at[rank], dg_send.at[u, b], dg_recv, peer(p))

    def stage_start(u):
        for b, (k, j) in enumerate(unit_blocks(u)):
            @pl.when(k == c)
            def _(b=b, j=j):
                stage_loc(b, j).start()

            @pl.when(k != c)
            def _(b=b, j=j):
                stage_rem(b, j).start()

            p = source_rank(k, j)

            @pl.when(p != rank)
            def _(b=b, p=p):
                dg_copy(u, b, p).start()

    def stage_wait(u, local):
        for b, (k, j) in enumerate(unit_blocks(u)):
            if local:
                @pl.when(k == c)
                def _(b=b, j=j):
                    stage_loc(b, j).wait()
            else:
                @pl.when(k != c)
                def _(b=b, j=j):
                    stage_rem(b, j).wait_send()

    start_loads(0)
    tri_ref[...] = (lax.broadcasted_iota(jnp.int32, (tok, tok), 0) <= lax.broadcasted_iota(jnp.int32, (tok, tok), 1)).astype(F32).astype(BF)
    for e in range(el):
        acc1[e] = jnp.zeros(acc1.shape[1:], F32)
        acc3[e] = jnp.zeros(acc3.shape[1:], F32)
        acc2[e] = jnp.zeros(acc2.shape[1:], F32)

    def gather_stage(u):
        rows = lax.broadcasted_iota(jnp.int32, (cap, tok), 0).astype(F32)
        lanes = lax.broadcasted_iota(jnp.int32, (tok, cap), 1).astype(F32)
        scale_all = []
        for b in range(2):
            halves = iv[b].astype(F32)
            ids = jnp.concatenate([halves[:top], halves[top:]], axis=1)
            gts = mv[b]
            masks, gws = [], []
            for e in range(el):
                hit = ids == (first + e).astype(F32)
                masks.append(jnp.sum(jnp.where(hit, 1.0, 0.0), axis=0, keepdims=True))
                gws.append(jnp.sum(jnp.where(hit, gts, 0.0), axis=0, keepdims=True))
            mask = jnp.concatenate(masks + [jnp.zeros((8 - el, tok), F32)], axis=0)
            cum = mm(mask.astype(BF), tri_ref[...])
            pos = jnp.where(mask > 0.0, cum - 1.0, -1.0)
            gw = jnp.concatenate(gws + [jnp.zeros((8 - el, tok), F32)], axis=0)
            cols = jnp.concatenate([pos, gw], axis=0).T
            gc_ref[b] = cols
            scales = []
            for e in range(el):
                hit = rows == pos[e:e + 1, :]
                pk_ref[b, e * cap:(e + 1) * cap, :] = jnp.where(hit, 1.0, 0.0).astype(BF)
                scales.append(jnp.sum(jnp.where(hit, gw[e:e + 1, :], 0.0), axis=1, keepdims=True))
                pt_ref[b, :, e * cap:(e + 1) * cap] = jnp.where(lanes == cols[:, e:e + 1], 1.0, 0.0).astype(BF)
            scale_all.append(jnp.concatenate(scales, axis=0))
        for b in range(2):
            p = pk_ref[b]
            xr = mm(p, xv[b]).astype(BF)
            dr = (scale_all[b] * mm(p, dv_[u % 2, b])).astype(BF)
            for e in range(el):
                xs_ref[e, b * cap:(b + 1) * cap, :] = xr[e * cap:(e + 1) * cap]
                do_ref[e, b * cap:(b + 1) * cap, :] = dr[e * cap:(e + 1) * cap]

    def expert_a(e):
        xs = xs_ref[e]
        uu = mm(xs, w1_ref[e]).astype(BF).astype(F32)
        vv = mm(xs, w3_ref[e]).astype(BF).astype(F32)
        sg = jax.nn.sigmoid(uu)
        a = (uu * sg * vv).astype(BF)
        o_ref[e] = mm(a, w2_ref[e]).astype(BF)
        do = do_ref[e]
        da = mm(do, w2_ref[e], ((1,), (1,)))
        du_ref[e] = (da * vv * sg * (1.0 + uu * (1.0 - sg))).astype(BF)
        dw_ref[e] = (da * uu * sg).astype(BF)
        acc2[e] += mm(a, do, ((0,), (0,)))

    def expert_b(e):
        xs = xs_ref[e]
        du = du_ref[e]
        dw = dw_ref[e]
        dxs = (mm(du, w1_ref[e], ((1,), (1,))) + mm(dw, w3_ref[e], ((1,), (1,)))).astype(BF)
        for b in range(2):
            dxs_ref[b, e * cap:(e + 1) * cap, :] = dxs[b * cap:(b + 1) * cap, :]
        acc1[e] += mm(xs, du, ((0,), (0,)))
        acc3[e] += mm(xs, dw, ((0,), (0,)))

    def scatter_stage(u):
        for b, (k, j) in enumerate(unit_blocks(u)):
            dyf = dv_[u % 2, b].astype(F32)
            yacc = None
            dgs = []
            for e in range(el):
                so = mm(pt_ref[b, :, e * cap:(e + 1) * cap], o_ref[e, b * cap:(b + 1) * cap, :])
                dgs.append(jnp.sum(dyf * so, axis=1, keepdims=True))
                term = gc_ref[b, :, 8 + e:9 + e] * so
                yacc = term if yacc is None else yacc + term
            stage[b, 0] = yacc
            stage[b, 1] = mm(pt_ref[b], dxs_ref[b])
            dg = jnp.concatenate(dgs + [jnp.zeros((tok, 8 - el), F32)], axis=1).T
            pieces = [dg[e:e + 1, i * lane:(i + 1) * lane] for e in range(el) for i in range(chunks)]
            if len(pieces) < 8:
                pieces.append(jnp.zeros((8 - len(pieces), lane), F32))
            dg = jnp.concatenate(pieces, axis=0)
            p = source_rank(k, j)
            dg_out[p] = dg

    def unit(u, carry):
        late = u >= rs_extra
        ahead_of = jnp.where(late, u - rs_extra, 0)

        def tick(i):
            if i != 2:
                ahead = 3 * u + min(i, 2) - 4
                t = ahead // 4 + 2
                due = jnp.logical_and(ahead >= 0, t <= H)

                @pl.when(jnp.logical_and(due, ahead % 4 == 0))
                def _():
                    ag_part((0, 1, 3), t)

                @pl.when(jnp.logical_and(due, ahead % 4 == 2))
                def _():
                    ag_part((2,), t)

            ev = 1 + 3 * (u - rs_unit) + ahead_of + min(i, 2)
            if i == 3:
                ev = ev + jnp.where(late, 1, 0)
            live = late if i == 2 else u >= 0

            @pl.when(jnp.logical_and(live, ev >= 1))
            def _():
                rs_finish(ev - 1)

            @pl.when(jnp.logical_and(live, ev >= 0))
            def _():
                rs_start(0, ev)
                rs_start(1, ev)

        wait_loads(u)

        @pl.when(u == 0)
        def _():
            for i, (src, dst) in enumerate(weights):
                pltpu.make_async_copy(src, dst, ld_w.at[i]).wait()

        gather_stage(u)
        expert_a(0)

        @pl.when(u >= 1)
        def _():
            stage_wait(u - 1, True)

        tick(0)
        expert_a(1)
        expert_b(0)
        tick(1)

        @pl.when(jnp.logical_and(u >= 1, u < N - 1))
        def _():
            start_loads(u + 1)

        expert_b(1)
        tick(2)

        @pl.when(u >= 1)
        def _():
            stage_wait(u - 1, False)

        scatter_stage(u)
        stage_start(u)
        tick(3)

        @pl.when(u == 0)
        def _():
            ag_part((0, 1, 3, 2), 1)
            start_loads(1)

        return carry

    lax.fori_loop(0, N, unit, 0)
    stage_wait(N - 1, True)
    def drain_sends():
        for kind in (0, 1, 2, 3):
            for q in range(2):
                def drain(t, carry, kind=kind, q=q):
                    ag_copy(q, kind, t, me).wait_send()
                    return carry
                lax.fori_loop(0, H if (q == 1) == (kind == 2) else H - 1, drain, 0)

            def drain_push(j, carry, kind=kind):
                push(kind, j).wait_send()
                return carry
            lax.fori_loop(0, N, drain_push, 0)

        def drain_dg(u, carry):
            for b in range(2):
                @pl.when(jnp.logical_or(u > 0, c != b))
                def _(b=b):
                    dg_copy(u, b, rank).wait_send()
            return carry
        lax.fori_loop(0, N, drain_dg, 0)
        stage_wait(N - 1, False)

    def finish_dgates():
        dg_in[rank] = dg_out[rank]
        rcopy(dg_in.at[pl.ds(0, nd - 1)], dg_in.at[pl.ds(0, nd - 1)], dg_send.at[0, 0], dg_recv, sib).wait_recv()
        for i in range(chunks):
            lanes = slice(i * lane, (i + 1) * lane)
            ids = oi[:, lanes].astype(F32)

            def pick(p, total, ids=ids, i=i):
                for e in range(el):
                    r = e * chunks + i
                    total = total + jnp.where(ids == (p * el + e).astype(F32), dg_in[p, r:r + 1, :], 0.0)
                return total

            dgates_ref[:, lanes] = lax.fori_loop(0, nd, pick, jnp.zeros((top, lane), F32))

    def tail(e, carry):
        rs_start(0, e)
        rs_start(1, e)
        rs_finish(e)

        @pl.when(e == rs_done + 2)
        def _():
            drain_sends()

        @pl.when(e == parts * (N - 2))
        def _():
            finish_dgates()

        @pl.when(e >= parts * (N - 1))
        def _():
            rows = rows_of(e % parts)
            for q, out in ((0, y_ref), (1, dx_ref)):
                out[rows, :] = ov[q, e % parts].astype(BF)
        return carry

    rs_finish(rs_done - 1)
    lax.fori_loop(rs_done, parts * N, tail, 0)


def store_pieces(shape):
    if len(shape) < 3:
        return [()]
    half = shape[1] // 2
    return [(i, pl.ds(r, half)) for i in range(shape[0]) for r in (0, half)]


def store_kernel(*refs):
    k = len(refs) // 2
    sems = refs[2 * k]
    copies = []
    for i in range(k):
        for piece in store_pieces(refs[i].shape):
            src, dst = (refs[i].at[piece], refs[k + i].at[piece]) if piece else (refs[i], refs[k + i])
            copies.append(pltpu.make_async_copy(src, dst, sems.at[len(copies)]))
    for cp in copies:
        cp.start()
    for cp in copies:
        cp.wait()


def store_call(arrays):
    vm = pl.BlockSpec(memory_space=pltpu.VMEM)
    return pl.pallas_call(
        store_kernel,
        in_specs=[vm] * len(arrays),
        out_specs=[pl.BlockSpec(memory_space=pl.ANY)] * len(arrays),
        out_shape=[pltpu.HBM(a.shape, a.dtype) for a in arrays],
        scratch_shapes=[pltpu.SemaphoreType.DMA((sum(len(store_pieces(a.shape)) for a in arrays),))],
        cost_estimate=pl.CostEstimate(flops=1, bytes_accessed=sum(a.size * a.dtype.itemsize for a in arrays), transcendentals=0),
        compiler_params=pltpu.CompilerParams(vmem_limit_bytes=16 * 1024 * 1024),
    )(*[pltpu.with_memory_space_constraint(a, pltpu.VMEM) for a in arrays])


def moe_call(n, cap, ids, gates, x, dy, w1, w3, w2):
    N = n * n
    tok, d = x.shape
    el, _, f = w1.shape
    parts = 4
    part = tok // parts
    meta = ids.shape
    halved = (2 * ids.shape[0], tok // 2)
    any_spec = pl.BlockSpec(memory_space=pl.ANY)
    vm = pl.BlockSpec(memory_space=pltpu.VMEM)
    flops = 13 * 2 * 2 * N * el * cap * d * f
    shape = jax.ShapeDtypeStruct
    dma = pltpu.SemaphoreType.DMA
    outs = pl.pallas_call(
        functools.partial(moe_kernel, n, cap),
        in_specs=[any_spec] * 7,
        out_specs=[vm] * 6 + [any_spec] * 7,
        out_shape=[
            pltpu.VMEM((tok, d), BF),
            pltpu.VMEM((tok, d), BF),
            pltpu.VMEM(ids.shape, F32),
            pltpu.VMEM((el, d, f), F32),
            pltpu.VMEM((el, d, f), F32),
            pltpu.VMEM((el, f, d), F32),
            shape((2, N, tok, d), BF),
            shape((2, N, tok, d), BF),
            shape((2, N) + meta, F32),
            shape((2, N) + halved, BF),
            shape((N, 2, tok, d), F32),
            shape((N, 2, tok, d), F32),
            shape((2, N - 1, tok, d), F32),
        ],
        scratch_shapes=[
            pltpu.VMEM((el, d, f), BF),
            pltpu.VMEM((el, d, f), BF),
            pltpu.VMEM((el, f, d), BF),
            pltpu.VMEM((2, tok, d), BF),
            pltpu.VMEM((2,) + meta, F32),
            pltpu.VMEM((2,) + halved, BF),
            pltpu.VMEM((2, 2, tok, d), BF),
            pltpu.VMEM((el, 2 * cap, d), BF),
            pltpu.VMEM((el, 2 * cap, d), BF),
            pltpu.VMEM((el, 2 * cap, d), BF),
            pltpu.VMEM((2, el * cap, d), BF),
            pltpu.VMEM((el, 2 * cap, f), BF),
            pltpu.VMEM((el, 2 * cap, f), BF),
            pltpu.VMEM((2, el * cap, tok), BF),
            pltpu.VMEM((2, tok, el * cap), BF),
            pltpu.VMEM((2, tok, 16), F32),
            pltpu.VMEM((tok, tok), BF),
            pltpu.VMEM((2, 2, tok, d), F32),
            pltpu.VMEM((2, 2, part, d), F32),
            pltpu.VMEM((2, parts, part, d), F32),
            pltpu.VMEM((2, part, d), F32),
            pltpu.VMEM(ids.shape, jnp.int32),
            pltpu.VMEM(halved, BF),
            pltpu.VMEM((2 * N, 8, tok // max(1, tok // 128)), F32),
            pltpu.VMEM((2 * N, 8, tok // max(1, tok // 128)), F32),
            dma((2, N // 2, 4)),
            dma((2, N // 2, 4)),
            dma((N, 4)),
            dma((N, 4)),
            dma((N,)),
            dma((2, parts)),
            dma((2, N, parts)),
            dma((N, 2)),
            dma(()),
            dma((2,)),
            dma((2,)),
            dma((2,)),
            dma((2,)),
            dma((3,)),
            dma((2,)),
            dma((2,)),
            dma((2, 2)),
            dma((2,)),
            dma(()),
        ],
        cost_estimate=pl.CostEstimate(flops=flops, bytes_accessed=2 * N * tok * d * 12, transcendentals=0),
        compiler_params=pltpu.CompilerParams(vmem_limit_bytes=46 * 1024 * 1024, collective_id=0, has_side_effects=True),
    )(x, dy, ids, gates, w1, w3, w2)
    return outs[:6]


def solution(mesh):
    nd = mesh.shape['row'] * mesh.shape['col']
    n = mesh.shape['row']
    grp = ('row', 'col')
    tspec = P(('dp', 'row', 'col'), None)
    wspec = P(grp, None, None)
    gspec = P(('dp', 'row', 'col'), None, None)

    def local(x, ridx, gates, w1, w3, w2, dy):
        tok, d = x.shape
        top = ridx.shape[1]
        el = w1.shape[0]
        ne = el * nd
        assert ne <= 256, 'ids exceed bfloat16'
        cap = min(tok, (4 * tok * top + ne - 1) // ne)
        y, dx, dgt, gw1, gw3, gw2 = store_call(moe_call(n, cap, ridx.T, gates.T, x, dy, w1, w3, w2))
        return y, dx, dgt.T, gw1, gw3, gw2

    return jax.shard_map(local, mesh=mesh, in_specs=(tspec, tspec, tspec, wspec, wspec, wspec, tspec), out_specs=(tspec, tspec, tspec, gspec, gspec, gspec), check_vma=False)
```

```python
import functools

import jax
import jax.numpy as jnp
from jax import lax
from jax.experimental import pallas as pl
from jax.experimental.pallas import tpu as pltpu
from jax.sharding import PartitionSpec as P

BF = jnp.bfloat16
F32 = jnp.float32
MESH = pl.DeviceIdType.MESH


def mm(a, b, dims=((1,), (0,))):
    return lax.dot_general(a, b, (dims, ((), ())), preferred_element_type=F32)


def cycle_index(k, n, x, y):
    return n * ((1 - k) * y + k * x) + (x + y) % n


def cycle_chip(k, n, i):
    r = i // n
    o = (i % n - r + n) % n
    return k * r + (1 - k) * o, k * o + (1 - k) * r


def moe_kernel(n, cap, x_ref, dy_ref, ids_ref, gates_ref, w1_hbm, w3_hbm, w2_hbm,
               y_ref, dx_ref, dgates_ref, acc1, acc3, acc2, xb, db, mb, ib, pown, psib, rin,
               w1_ref, w3_ref, w2_ref, xv, mv, iv, dv_, xs_ref, do_ref, o_ref, dxs_ref, du_ref, dw_ref, pk_ref, pt_ref, gc_ref, tri_ref,
               stage, pv, ov, land, oi, oh, dg_out, dg_in,
               ag_send, ag_recv, push_send, push_recv, part_recv, rs_send, rs_recv, dg_send, dg_recv,
               ld_x, ld_m, ld_i, ld_d, ld_w, st_loc, st_rem, ld_p, ld_r, ld_o):
    N = n * n
    H = N // 2
    row = lax.axis_index('row')
    col = lax.axis_index('col')
    cx = col // 2
    c = col % 2
    cy = row
    tok, d = x_ref.shape
    top = ids_ref.shape[0]
    el = w1_ref.shape[0]
    parts = ov.shape[1]
    part = tok // parts
    pos_k = (cycle_index(0, n, cx, cy), cycle_index(1, n, cx, cy))
    me = (1 - c) * pos_k[0] + c * pos_k[1]
    rank = cy * (2 * n) + 2 * cx + c
    first = rank * el
    nd = 2 * N
    chunks = max(1, tok // 128)
    lane = tok // chunks
    rs_unit = max(N // 2, 4)
    rs_extra = N - 3
    rs_done = 5 + 3 * (N - 1 - rs_unit) + N - 1 - rs_extra

    def device(i):
        px, py = cycle_chip(c, n, i)
        return {'row': py, 'col': 2 * px + c}

    nxt = device((me + 1) % N)
    prv = device((me + N - 1) % N)
    sib = {'row': row, 'col': 2 * cx + 1 - c}
    ring = (nxt, prv)

    def rcopy(src, dst, ss, rs, dev):
        return pltpu.make_async_remote_copy(src_ref=src, dst_ref=dst, send_sem=ss, recv_sem=rs, device_id=dev, device_id_type=MESH)

    def peer(p):
        return {'row': p // (2 * n), 'col': p % (2 * n)}

    barrier = pltpu.get_barrier_semaphore()
    for dev in (nxt, prv, sib):
        pl.semaphore_signal(barrier, inc=1, device_id=dev, device_id_type=MESH)
    own_ids = pltpu.make_async_copy(ids_ref, oi, ld_o)
    own_ids.start()
    pl.semaphore_wait(barrier, 3)

    own = (x_ref, gates_ref, dy_ref, oh)
    bufs = (xb, mb, db, ib)

    def ag_copy(q, kind, t, j, src=None):
        slot = bufs[kind].at[c, j]
        return rcopy(slot if src is None else src, slot, ag_send.at[q, t, kind], ag_recv.at[q, t, kind], ring[q])

    def push(kind, j, src=None):
        slot = bufs[kind].at[c, j]
        return rcopy(slot if src is None else src, slot, push_send.at[j, kind], push_recv.at[j, kind], sib)

    def push_arrival(kind, k, j):
        slot = bufs[kind].at[k, j]
        return rcopy(slot, slot, push_send.at[j, kind], push_recv.at[j, kind], sib)

    for kind in (0, 1, 3, 2):
        if kind == 3:
            own_ids.wait()
            oh[:top, :] = oi[:, :tok // 2].astype(F32).astype(BF)
            oh[top:, :] = oi[:, tok // 2:].astype(F32).astype(BF)
        ag_copy(0, kind, 0, me, own[kind]).start()
        ag_copy(1, kind, 0, me, own[kind]).start()
        push(kind, me, own[kind]).start()

    weights = ((w1_hbm, w1_ref), (w3_hbm, w3_ref), (w2_hbm, w2_ref))
    for i, (src, dst) in enumerate(weights):
        pltpu.make_async_copy(src, dst, ld_w.at[i]).start()

    def unit_blocks(u):
        o = (u + 1) // 2
        ka = jnp.where(u == 0, 0, (u + 1) % 2)
        kb = jnp.where(u == N - 1, 1, (u + 1) % 2)
        ia = (1 - ka) * pos_k[0] + ka * pos_k[1]
        ib = (1 - kb) * pos_k[0] + kb * pos_k[1]
        return ((ka, (ia - o + N) % N), (kb, (ib + o) % N))

    def block_loads(u, b, k, j, local):
        slot = u % 2
        cps = [pltpu.make_async_copy(x_ref if local else xb.at[k, j], xv.at[b], ld_x.at[b]),
               pltpu.make_async_copy(dy_ref if local else db.at[k, j], dv_.at[slot, b], ld_d.at[b])]
        cps.append(pltpu.make_async_copy(gates_ref if local else mb.at[k, j], mv.at[b], ld_m.at[b]))
        if not local:
            cps.append(pltpu.make_async_copy(ib.at[k, j], iv.at[b], ld_i.at[b]))
        return cps

    def start_loads(u):
        for b, (k, j) in enumerate(unit_blocks(u)):
            @pl.when(k != c)
            def _(k=k, j=j):
                for kind in (0, 1, 2, 3):
                    push_arrival(kind, k, j).wait_recv()

            @pl.when(jnp.logical_and(u == 0, k == c))
            def _(b=b, k=k, j=j):
                for cp in block_loads(u, b, k, j, True):
                    cp.start()
                iv[b] = oh[...]

            @pl.when(jnp.logical_or(u != 0, k != c))
            def _(b=b, k=k, j=j):
                for cp in block_loads(u, b, k, j, False):
                    cp.start()

    def wait_loads(u):
        for b, (k, j) in enumerate(unit_blocks(u)):
            for cp in block_loads(u, b, k, j, True):
                cp.wait()

            @pl.when(jnp.logical_or(u != 0, k != c))
            def _(b=b, k=k, j=j):
                pltpu.make_async_copy(ib.at[k, j], iv.at[b], ld_i.at[b]).wait()

    def ag_part(kinds, t):
        for kind in kinds:
            for q in range(2):
                j = (me - t + N) % N if q == 0 else (me + t) % N
                reach = H if (q == 1) == (kind == 2) else H - 1

                @pl.when(t <= reach)
                def _(kind=kind, q=q, j=j, reach=reach):
                    ag_copy(q, kind, t - 1, j).wait_recv()

                    @pl.when(t < reach)
                    def _():
                        ag_copy(q, kind, t, j).start()

                    push(kind, j).start()

    def rs_dest(q, s):
        return (me - 1 - s + 2 * N) % N if q == 0 else (me + 1 + s) % N

    def rows_of(h):
        return pl.ds(pl.multiple_of(h * part, part), part)

    def rs_loads(q, e):
        s, h = e // parts, e % parts
        dst = rs_dest(q, s)
        rows = rows_of(h)
        p0 = pltpu.make_async_copy(pown.at[dst, q, rows], pv.at[q, 0], ld_p.at[q, 0])
        p1 = pltpu.make_async_copy(psib.at[dst, q, rows], pv.at[q, 1], ld_p.at[q, 1])
        r = pltpu.make_async_copy(rin.at[q, jnp.maximum(s - 1, 0), rows], ov.at[q, h], ld_r.at[q])
        return p0, p1, r

    def rs_copy(q, e):
        s, h = e // parts, e % parts
        return rcopy(ov.at[q, h], rin.at[q, s, rows_of(h)], rs_send.at[q, h], rs_recv.at[q, s, h], ring[q])

    final = parts * N - 1

    def rs_last(q):
        return rcopy(ov.at[q, parts - 1], land.at[q], rs_send.at[q, parts - 1], rs_recv.at[q, N - 2, parts - 1], ring[q])

    def rs_start(q, e):
        s, h = e // parts, e % parts
        fresh = s <= H - 2
        if q == 0:
            fresh = jnp.logical_or(fresh, jnp.logical_or(s == H - 1, s == N - 1))

        @pl.when(jnp.logical_and(h == 0, fresh))
        def _():
            dst = rs_dest(q, s)
            rcopy(psib.at[dst], psib.at[dst], st_rem.at[0], part_recv.at[dst], sib).wait_recv()

        p0, p1, r = rs_loads(q, e)
        p0.start()
        p1.start()

        @pl.when(jnp.logical_and(e >= parts, e < final))
        def _():
            rs_copy(q, e - parts).wait_send()
            rs_copy(q, e - parts).wait_recv()
            r.start()

        @pl.when(e == final)
        def _():
            rs_last(q).wait()

    def rs_finish(e):
        h = e % parts
        loads = [rs_loads(q, e) for q in range(2)]
        for p0, p1, _ in loads:
            p0.wait()
            p1.wait()
        step = min(64, part)

        def add(base):
            def body(i, carry):
                rr = pl.ds(pl.multiple_of(i * step, step), step)
                for q in range(2):
                    total = pv[q, 0, rr, :] + pv[q, 1, rr, :]
                    if base == 'arrived':
                        total = ov[q, h, rr, :] + total
                    elif base == 'landed':
                        total = land[q, rr, :] + total
                    ov[q, h, rr, :] = total
                return carry
            lax.fori_loop(0, part // step, body, 0)

        @pl.when(e < parts)
        def _():
            add('none')

        @pl.when(jnp.logical_and(e >= parts, e < final))
        def _():
            for _, _, r in loads:
                r.wait()
            add('arrived')

        @pl.when(e == final)
        def _():
            add('landed')

        @pl.when(e < final - parts)
        def _():
            for q in range(2):
                rs_copy(q, e).start()

        @pl.when(e == final - parts)
        def _():
            for q in range(2):
                rs_last(q).start()

    def stage_loc(b, j):
        return pltpu.make_async_copy(stage.at[b], pown.at[j], st_loc.at[b])

    def stage_rem(b, j):
        return rcopy(stage.at[b], psib.at[j], st_rem.at[b], part_recv.at[j], sib)

    def source_rank(k, j):
        px, py = cycle_chip(k, n, j)
        return py * (2 * n) + 2 * px + k

    def dg_copy(u, b, p):
        return rcopy(dg_out.at[p], dg_in.at[rank], dg_send.at[u, b], dg_recv, peer(p))

    def stage_start(u):
        for b, (k, j) in enumerate(unit_blocks(u)):
            @pl.when(k == c)
            def _(b=b, j=j):
                stage_loc(b, j).start()

            @pl.when(k != c)
            def _(b=b, j=j):
                stage_rem(b, j).start()

            p = source_rank(k, j)

            @pl.when(p != rank)
            def _(b=b, p=p):
                dg_copy(u, b, p).start()

    def stage_wait(u, local):
        for b, (k, j) in enumerate(unit_blocks(u)):
            if local:
                @pl.when(k == c)
                def _(b=b, j=j):
                    stage_loc(b, j).wait()
            else:
                @pl.when(k != c)
                def _(b=b, j=j):
                    stage_rem(b, j).wait_send()

    start_loads(0)
    tri_ref[...] = (lax.broadcasted_iota(jnp.int32, (tok, tok), 0) <= lax.broadcasted_iota(jnp.int32, (tok, tok), 1)).astype(F32).astype(BF)
    for e in range(el):
        acc1[e] = jnp.zeros(acc1.shape[1:], F32)
        acc3[e] = jnp.zeros(acc3.shape[1:], F32)
        acc2[e] = jnp.zeros(acc2.shape[1:], F32)

    def gather_stage(u):
        rows = lax.broadcasted_iota(jnp.int32, (cap, tok), 0).astype(F32)
        lanes = lax.broadcasted_iota(jnp.int32, (tok, cap), 1).astype(F32)
        scale_all = []
        for b in range(2):
            halves = iv[b].astype(F32)
            ids = jnp.concatenate([halves[:top], halves[top:]], axis=1)
            gts = mv[b]
            masks, gws = [], []
            for e in range(el):
                hit = ids == (first + e).astype(F32)
                masks.append(jnp.sum(jnp.where(hit, 1.0, 0.0), axis=0, keepdims=True))
                gws.append(jnp.sum(jnp.where(hit, gts, 0.0), axis=0, keepdims=True))
            mask = jnp.concatenate(masks + [jnp.zeros((8 - el, tok), F32)], axis=0)
            cum = mm(mask.astype(BF), tri_ref[...])
            pos = jnp.where(mask > 0.0, cum - 1.0, -1.0)
            gw = jnp.concatenate(gws + [jnp.zeros((8 - el, tok), F32)], axis=0)
            cols = jnp.concatenate([pos, gw], axis=0).T
            gc_ref[b] = cols
            scales = []
            for e in range(el):
                hit = rows == pos[e:e + 1, :]
                pk_ref[b, e * cap:(e + 1) * cap, :] = jnp.where(hit, 1.0, 0.0).astype(BF)
                scales.append(jnp.sum(jnp.where(hit, gw[e:e + 1, :], 0.0), axis=1, keepdims=True))
                pt_ref[b, :, e * cap:(e + 1) * cap] = jnp.where(lanes == cols[:, e:e + 1], 1.0, 0.0).astype(BF)
            scale_all.append(jnp.concatenate(scales, axis=0))
        for b in range(2):
            p = pk_ref[b]
            xr = mm(p, xv[b]).astype(BF)
            dr = (scale_all[b] * mm(p, dv_[u % 2, b])).astype(BF)
            for e in range(el):
                xs_ref[e, b * cap:(b + 1) * cap, :] = xr[e * cap:(e + 1) * cap]
                do_ref[e, b * cap:(b + 1) * cap, :] = dr[e * cap:(e + 1) * cap]

    def expert_a(e):
        xs = xs_ref[e]
        uu = mm(xs, w1_ref[e]).astype(BF).astype(F32)
        vv = mm(xs, w3_ref[e]).astype(BF).astype(F32)
        sg = jax.nn.sigmoid(uu)
        a = (uu * sg * vv).astype(BF)
        o_ref[e] = mm(a, w2_ref[e]).astype(BF)
        do = do_ref[e]
        da = mm(do, w2_ref[e], ((1,), (1,)))
        du_ref[e] = (da * vv * sg * (1.0 + uu * (1.0 - sg))).astype(BF)
        dw_ref[e] = (da * uu * sg).astype(BF)
        acc2[e] += mm(a, do, ((0,), (0,)))

    def expert_b(e):
        xs = xs_ref[e]
        du = du_ref[e]
        dw = dw_ref[e]
        dxs = (mm(du, w1_ref[e], ((1,), (1,))) + mm(dw, w3_ref[e], ((1,), (1,)))).astype(BF)
        for b in range(2):
            dxs_ref[b, e * cap:(e + 1) * cap, :] = dxs[b * cap:(b + 1) * cap, :]
        acc1[e] += mm(xs, du, ((0,), (0,)))
        acc3[e] += mm(xs, dw, ((0,), (0,)))

    def scatter_stage(u):
        for b, (k, j) in enumerate(unit_blocks(u)):
            dyf = dv_[u % 2, b].astype(F32)
            yacc = None
            dgs = []
            for e in range(el):
                so = mm(pt_ref[b, :, e * cap:(e + 1) * cap], o_ref[e, b * cap:(b + 1) * cap, :])
                dgs.append(jnp.sum(dyf * so, axis=1, keepdims=True))
                term = gc_ref[b, :, 8 + e:9 + e] * so
                yacc = term if yacc is None else yacc + term
            stage[b, 0] = yacc
            stage[b, 1] = mm(pt_ref[b], dxs_ref[b])
            dg = jnp.concatenate(dgs + [jnp.zeros((tok, 8 - el), F32)], axis=1).T
            pieces = [dg[e:e + 1, i * lane:(i + 1) * lane] for e in range(el) for i in range(chunks)]
            if len(pieces) < 8:
                pieces.append(jnp.zeros((8 - len(pieces), lane), F32))
            dg = jnp.concatenate(pieces, axis=0)
            p = source_rank(k, j)
            dg_out[p] = dg

    def unit(u, carry):
        late = u >= rs_extra
        ahead_of = jnp.where(late, u - rs_extra, 0)

        def tick(i):
            if i != 2:
                ahead = 3 * u + min(i, 2) - 4
                t = ahead // 4 + 2
                due = jnp.logical_and(ahead >= 0, t <= H)

                @pl.when(jnp.logical_and(due, ahead % 4 == 0))
                def _():
                    ag_part((0, 1, 3), t)

                @pl.when(jnp.logical_and(due, ahead % 4 == 2))
                def _():
                    ag_part((2,), t)

            ev = 1 + 3 * (u - rs_unit) + ahead_of + min(i, 2)
            if i == 3:
                ev = ev + jnp.where(late, 1, 0)
            live = late if i == 2 else u >= 0

            @pl.when(jnp.logical_and(live, ev >= 1))
            def _():
                rs_finish(ev - 1)

            @pl.when(jnp.logical_and(live, ev >= 0))
            def _():
                rs_start(0, ev)
                rs_start(1, ev)

        wait_loads(u)

        @pl.when(u == 0)
        def _():
            for i, (src, dst) in enumerate(weights):
                pltpu.make_async_copy(src, dst, ld_w.at[i]).wait()

        gather_stage(u)
        expert_a(0)

        @pl.when(u >= 1)
        def _():
            stage_wait(u - 1, True)

        tick(0)
        expert_a(1)
        expert_b(0)
        tick(1)

        @pl.when(u == 0)
        def _():
            ag_part((0, 1, 3), 1)

        @pl.when(jnp.logical_and(u >= 1, u < N - 1))
        def _():
            start_loads(u + 1)

        expert_b(1)
        tick(2)

        @pl.when(u >= 1)
        def _():
            stage_wait(u - 1, False)

        scatter_stage(u)
        stage_start(u)
        tick(3)

        @pl.when(u == 0)
        def _():
            ag_part((2,), 1)
            start_loads(1)

        return carry

    lax.fori_loop(0, N, unit, 0)
    stage_wait(N - 1, True)
    def drain_sends():
        for kind in (0, 1, 2, 3):
            for q in range(2):
                def drain(t, carry, kind=kind, q=q):
                    ag_copy(q, kind, t, me).wait_send()
                    return carry
                lax.fori_loop(0, H if (q == 1) == (kind == 2) else H - 1, drain, 0)

            def drain_push(j, carry, kind=kind):
                push(kind, j).wait_send()
                return carry
            lax.fori_loop(0, N, drain_push, 0)

        def drain_dg(u, carry):
            for b in range(2):
                @pl.when(jnp.logical_or(u > 0, c != b))
                def _(b=b):
                    dg_copy(u, b, rank).wait_send()
            return carry
        lax.fori_loop(0, N, drain_dg, 0)
        stage_wait(N - 1, False)

    def finish_dgates():
        dg_in[rank] = dg_out[rank]
        rcopy(dg_in.at[pl.ds(0, nd - 1)], dg_in.at[pl.ds(0, nd - 1)], dg_send.at[0, 0], dg_recv, sib).wait_recv()
        for i in range(chunks):
            lanes = slice(i * lane, (i + 1) * lane)
            ids = oi[:, lanes].astype(F32)

            def pick(p, total, ids=ids, i=i):
                for e in range(el):
                    r = e * chunks + i
                    total = total + jnp.where(ids == (p * el + e).astype(F32), dg_in[p, r:r + 1, :], 0.0)
                return total

            dgates_ref[:, lanes] = lax.fori_loop(0, nd, pick, jnp.zeros((top, lane), F32))

    def tail(e, carry):
        rs_start(0, e)
        rs_start(1, e)
        rs_finish(e)

        @pl.when(e == rs_done + 2)
        def _():
            drain_sends()

        @pl.when(e == parts * (N - 2))
        def _():
            finish_dgates()

        @pl.when(e >= parts * (N - 1))
        def _():
            rows = rows_of(e % parts)
            for q, out in ((0, y_ref), (1, dx_ref)):
                out[rows, :] = ov[q, e % parts].astype(BF)
        return carry

    rs_finish(rs_done - 1)
    lax.fori_loop(rs_done, parts * N, tail, 0)


def store_pieces(shape):
    if len(shape) < 3:
        return [()]
    half = shape[1] // 2
    return [(i, pl.ds(r, half)) for i in range(shape[0]) for r in (0, half)]


def store_kernel(*refs):
    k = len(refs) // 2
    sems = refs[2 * k]
    copies = []
    for i in range(k):
        for piece in store_pieces(refs[i].shape):
            src, dst = (refs[i].at[piece], refs[k + i].at[piece]) if piece else (refs[i], refs[k + i])
            copies.append(pltpu.make_async_copy(src, dst, sems.at[len(copies)]))
    for cp in copies:
        cp.start()
    for cp in copies:
        cp.wait()


def store_call(arrays):
    vm = pl.BlockSpec(memory_space=pltpu.VMEM)
    return pl.pallas_call(
        store_kernel,
        in_specs=[vm] * len(arrays),
        out_specs=[pl.BlockSpec(memory_space=pl.ANY)] * len(arrays),
        out_shape=[pltpu.HBM(a.shape, a.dtype) for a in arrays],
        scratch_shapes=[pltpu.SemaphoreType.DMA((sum(len(store_pieces(a.shape)) for a in arrays),))],
        cost_estimate=pl.CostEstimate(flops=1, bytes_accessed=sum(a.size * a.dtype.itemsize for a in arrays), transcendentals=0),
        compiler_params=pltpu.CompilerParams(vmem_limit_bytes=16 * 1024 * 1024),
    )(*[pltpu.with_memory_space_constraint(a, pltpu.VMEM) for a in arrays])


def moe_call(n, cap, ids, gates, x, dy, w1, w3, w2):
    N = n * n
    tok, d = x.shape
    el, _, f = w1.shape
    parts = 4
    part = tok // parts
    meta = ids.shape
    halved = (2 * ids.shape[0], tok // 2)
    any_spec = pl.BlockSpec(memory_space=pl.ANY)
    vm = pl.BlockSpec(memory_space=pltpu.VMEM)
    flops = 13 * 2 * 2 * N * el * cap * d * f
    shape = jax.ShapeDtypeStruct
    dma = pltpu.SemaphoreType.DMA
    outs = pl.pallas_call(
        functools.partial(moe_kernel, n, cap),
        in_specs=[any_spec] * 7,
        out_specs=[vm] * 6 + [any_spec] * 7,
        out_shape=[
            pltpu.VMEM((tok, d), BF),
            pltpu.VMEM((tok, d), BF),
            pltpu.VMEM(ids.shape, F32),
            pltpu.VMEM((el, d, f), F32),
            pltpu.VMEM((el, d, f), F32),
            pltpu.VMEM((el, f, d), F32),
            shape((2, N, tok, d), BF),
            shape((2, N, tok, d), BF),
            shape((2, N) + meta, F32),
            shape((2, N) + halved, BF),
            shape((N, 2, tok, d), F32),
            shape((N, 2, tok, d), F32),
            shape((2, N - 1, tok, d), F32),
        ],
        scratch_shapes=[
            pltpu.VMEM((el, d, f), BF),
            pltpu.VMEM((el, d, f), BF),
            pltpu.VMEM((el, f, d), BF),
            pltpu.VMEM((2, tok, d), BF),
            pltpu.VMEM((2,) + meta, F32),
            pltpu.VMEM((2,) + halved, BF),
            pltpu.VMEM((2, 2, tok, d), BF),
            pltpu.VMEM((el, 2 * cap, d), BF),
            pltpu.VMEM((el, 2 * cap, d), BF),
            pltpu.VMEM((el, 2 * cap, d), BF),
            pltpu.VMEM((2, el * cap, d), BF),
            pltpu.VMEM((el, 2 * cap, f), BF),
            pltpu.VMEM((el, 2 * cap, f), BF),
            pltpu.VMEM((2, el * cap, tok), BF),
            pltpu.VMEM((2, tok, el * cap), BF),
            pltpu.VMEM((2, tok, 16), F32),
            pltpu.VMEM((tok, tok), BF),
            pltpu.VMEM((2, 2, tok, d), F32),
            pltpu.VMEM((2, 2, part, d), F32),
            pltpu.VMEM((2, parts, part, d), F32),
            pltpu.VMEM((2, part, d), F32),
            pltpu.VMEM(ids.shape, jnp.int32),
            pltpu.VMEM(halved, BF),
            pltpu.VMEM((2 * N, 8, tok // max(1, tok // 128)), F32),
            pltpu.VMEM((2 * N, 8, tok // max(1, tok // 128)), F32),
            dma((2, N // 2, 4)),
            dma((2, N // 2, 4)),
            dma((N, 4)),
            dma((N, 4)),
            dma((N,)),
            dma((2, parts)),
            dma((2, N, parts)),
            dma((N, 2)),
            dma(()),
            dma((2,)),
            dma((2,)),
            dma((2,)),
            dma((2,)),
            dma((3,)),
            dma((2,)),
            dma((2,)),
            dma((2, 2)),
            dma((2,)),
            dma(()),
        ],
        cost_estimate=pl.CostEstimate(flops=flops, bytes_accessed=2 * N * tok * d * 12, transcendentals=0),
        compiler_params=pltpu.CompilerParams(vmem_limit_bytes=46 * 1024 * 1024, collective_id=0, has_side_effects=True),
    )(x, dy, ids, gates, w1, w3, w2)
    return outs[:6]


def solution(mesh):
    nd = mesh.shape['row'] * mesh.shape['col']
    n = mesh.shape['row']
    grp = ('row', 'col')
    tspec = P(('dp', 'row', 'col'), None)
    wspec = P(grp, None, None)
    gspec = P(('dp', 'row', 'col'), None, None)

    def local(x, ridx, gates, w1, w3, w2, dy):
        tok, d = x.shape
        top = ridx.shape[1]
        el = w1.shape[0]
        ne = el * nd
        assert ne <= 256, 'ids exceed bfloat16'
        cap = min(tok, (4 * tok * top + ne - 1) // ne)
        y, dx, dgt, gw1, gw3, gw2 = store_call(moe_call(n, cap, ridx.T, gates.T, x, dy, w1, w3, w2))
        return y, dx, dgt.T, gw1, gw3, gw2

    return jax.shard_map(local, mesh=mesh, in_specs=(tspec, tspec, tspec, wspec, wspec, wspec, tspec), out_specs=(tspec, tspec, tspec, gspec, gspec, gspec), check_vma=False)
```
